256 devices in a mesh: dp: 256 (over z, y, x, core).
Axes of the slice: x: 4, y: 4, z: 8, core: 2. Of those that a mesh axis runs over, the one named last changes fastest.
Arguments:
- query_feat: bfloat16 [32768, 256], P('dp')
- item_feat: bfloat16 [32768, 256], P('dp')
- log_q: float32 [32768], P('dp')
- w_query_in: bfloat16 [256, 256], replicated
- w_query_out: bfloat16 [256, 128], replicated
- w_item_in: bfloat16 [256, 256], replicated
- w_item_out: bfloat16 [256, 128], replicated
Outputs:
- output 1: float32 [1], replicated
- output 2: float32 [256, 256], replicated
- output 3: float32 [256, 128], replicated
- output 4: float32 [256, 256], replicated
- output 5: float32 [256, 128], replicated
All inputs are finite; a program needn't handle non-finite values.
Results may differ from the reference program's by a relative error of at most 0.00618852.
Values are sent between devices in bfloat16 or wider.
A program may use at most 768 MiB of HBM per device.

```python
import jax
import jax.numpy as jnp
from jax import lax

GROUP_DEVICES = 256
ROWS_DEV = 128
FEAT_DIM = 256
HIDDEN_DIM = 256
EMBED_DIM = 128
GLOBAL_ROWS = GROUP_DEVICES * ROWS_DEV
POOL_SIZE = GLOBAL_ROWS // 4
BLOCK_ROWS = min(GLOBAL_ROWS, 256)
TEMPERATURE = 0.05
NORM_EPS = 1e-6


def setup_inputs(seed: int = 0) -> dict:
    base_key = jax.random.key(seed)
    keys_all = jax.random.split(base_key, 9)
    query_feat = jax.random.normal(keys_all[0], (GLOBAL_ROWS, FEAT_DIM), jnp.float32).astype(jnp.bfloat16)
    item_pool = jax.random.normal(keys_all[1], (POOL_SIZE, FEAT_DIM), jnp.float32)
    pick_a = jax.random.randint(keys_all[2], (GLOBAL_ROWS,), 0, POOL_SIZE)
    pick_b = jax.random.randint(keys_all[3], (GLOBAL_ROWS,), 0, POOL_SIZE)
    item_ids = (pick_a * pick_b) // POOL_SIZE
    item_feat = jnp.take(item_pool, item_ids, axis=0).astype(jnp.bfloat16)
    counts = jax.ops.segment_sum(jnp.ones((GLOBAL_ROWS,), jnp.float32), item_ids, num_segments=POOL_SIZE)
    log_q = jnp.log(jnp.take(counts, item_ids) / GLOBAL_ROWS) + 0.3 * jax.random.normal(keys_all[4], (GLOBAL_ROWS,), jnp.float32)
    w_query_in = (jax.random.normal(keys_all[5], (FEAT_DIM, HIDDEN_DIM), jnp.float32) * FEAT_DIM ** -0.5).astype(jnp.bfloat16)
    w_query_out = (jax.random.normal(keys_all[6], (HIDDEN_DIM, EMBED_DIM), jnp.float32) * HIDDEN_DIM ** -0.5).astype(jnp.bfloat16)
    w_item_in = (jax.random.normal(keys_all[7], (FEAT_DIM, HIDDEN_DIM), jnp.float32) * FEAT_DIM ** -0.5).astype(jnp.bfloat16)
    w_item_out = (jax.random.normal(keys_all[8], (HIDDEN_DIM, EMBED_DIM), jnp.float32) * HIDDEN_DIM ** -0.5).astype(jnp.bfloat16)
    return {'query_feat': query_feat, 'item_feat': item_feat, 'log_q': log_q, 'w_query_in': w_query_in, 'w_query_out': w_query_out, 'w_item_in': w_item_in, 'w_item_out': w_item_out}


def tower_forward(feat_rows, w_in, w_out):
    pre_act = jnp.dot(feat_rows, w_in, preferred_element_type=jnp.float32)
    hidden = jnp.maximum(pre_act, 0.0).astype(jnp.bfloat16)
    embed = jnp.dot(hidden, w_out, preferred_element_type=jnp.float32)
    inv_norm = lax.rsqrt(jnp.sum(embed * embed, axis=-1, keepdims=True) + NORM_EPS)
    return pre_act, hidden, inv_norm, embed * inv_norm


def tower_backward(feat_rows, w_out, pre_act, hidden, inv_norm, unit_vec, d_unit):
    d_embed = inv_norm * (d_unit - unit_vec * jnp.sum(unit_vec * d_unit, axis=-1, keepdims=True))
    d_embed_bf = d_embed.astype(jnp.bfloat16)
    grad_out = jnp.dot(hidden.T, d_embed_bf, preferred_element_type=jnp.float32)
    d_hidden = jnp.dot(d_embed_bf, w_out.T, preferred_element_type=jnp.float32)
    d_pre = jnp.where(pre_act > 0, d_hidden, 0.0).astype(jnp.bfloat16)
    grad_in = jnp.dot(feat_rows.T, d_pre, preferred_element_type=jnp.float32)
    return grad_in, grad_out


def softmax_grads(query_bf, items_bf, log_q):
    num_blocks = GLOBAL_ROWS // BLOCK_ROWS
    grad_scale = 1.0 / (TEMPERATURE * GLOBAL_ROWS)
    col_ids = jnp.arange(GLOBAL_ROWS)[None, :]
    query_blocks = query_bf.reshape(num_blocks, BLOCK_ROWS, EMBED_DIM)

    def block_step(d_item_acc, inputs):
        block_index, query_blk = inputs
        logits = jnp.dot(query_blk, items_bf.T, preferred_element_type=jnp.float32) / TEMPERATURE - log_q[None, :]
        row_ids = block_index * BLOCK_ROWS + jnp.arange(BLOCK_ROWS)[:, None]
        is_pos = row_ids == col_ids
        row_max = jnp.max(logits, axis=1, keepdims=True)
        log_norm = row_max + jnp.log(jnp.sum(jnp.exp(logits - row_max), axis=1, keepdims=True))
        pos_logit = jnp.sum(jnp.where(is_pos, logits, 0.0), axis=1, keepdims=True)
        prob_rows = jnp.exp(logits - log_norm)
        grad_logits = jnp.where(is_pos, prob_rows - 1.0, prob_rows).astype(jnp.bfloat16)
        d_query_blk = jnp.dot(grad_logits, items_bf, preferred_element_type=jnp.float32) * grad_scale
        d_item_acc = d_item_acc + jnp.dot(grad_logits.T, query_blk, preferred_element_type=jnp.float32)
        return d_item_acc, (jnp.sum(log_norm - pos_logit), d_query_blk)

    acc_init = jnp.zeros((GLOBAL_ROWS, EMBED_DIM), jnp.float32)
    d_item_acc, (loss_parts, d_query_blocks) = lax.scan(block_step, acc_init, (jnp.arange(num_blocks), query_blocks))
    return jnp.sum(loss_parts), d_query_blocks.reshape(GLOBAL_ROWS, EMBED_DIM), d_item_acc * grad_scale


def reference(query_feat, item_feat, log_q, w_query_in, w_query_out, w_item_in, w_item_out):
    q_pre, q_hidden, q_inv, q_unit = tower_forward(query_feat, w_query_in, w_query_out)
    v_pre, v_hidden, v_inv, v_unit = tower_forward(item_feat, w_item_in, w_item_out)
    loss_sum, d_query, d_item = softmax_grads(q_unit.astype(jnp.bfloat16), v_unit.astype(jnp.bfloat16), log_q)
    grad_query_in, grad_query_out = tower_backward(query_feat, w_query_out, q_pre, q_hidden, q_inv, q_unit, d_query)
    grad_item_in, grad_item_out = tower_backward(item_feat, w_item_out, v_pre, v_hidden, v_inv, v_unit, d_item)
    loss = jnp.reshape(loss_sum / GLOBAL_ROWS, (1,))
    return (loss, grad_query_in, grad_query_out, grad_item_in, grad_item_out)
```

```python
import functools

import jax
import jax.numpy as jnp
from jax import lax
from jax.experimental import pallas as pl
from jax.experimental.pallas import tpu as pltpu
from jax.sharding import PartitionSpec as P

f32, bf16 = jnp.float32, jnp.bfloat16
MESH = pl.DeviceIdType.MESH
TEMP = 0.05
EPS = 1e-6
LOG2E = 1.4426950408889634
LN2 = 0.6931471805599453
NT = (((1,), (1,)), ((), ()))
TN = (((0,), (0,)), ((), ()))
NN = (((1,), (0,)), ((), ()))


def dot(a, b, dims=NN):
    return lax.dot_general(a, b, dims, preferred_element_type=f32)


def kernel(NZ, NXY, qf, vf, lq, wqi, wqo, wvi, wvo,
           gqi_o, gqo_o, gvi_o, gvo_o, loss_o,
           u_all, v_all, vt, lq_all, bcol, e_all, g_all, csum, stats, invl,
           up, ui, uh, ua, vp, vi, vh, va,
           su, ru, pv_out, pv_in, sv, rv, gl, gpair, gx_s, gx_r, gz_r, fin, loss_p, loss_x,
           s_u, r_u, s_v, r_v, s_lq, r_lq, s_st, r_st, s_pv, r_pv, s_sv, r_sv, s_su, r_su,
           s_gp, r_gp, s_gx, r_gx, s_gz, r_gz, s_ag, r_ag, s_rl, r_rl, s_lp, r_lp, s_lx, r_lx, s_vr):
    R, D = 128, 128
    NQ = NZ * R
    NI = 2 * NXY * R
    B = NZ * NXY * 2 * R
    CH = 768 // NXY
    me = lax.axis_index("dp")
    c = lax.rem(me, 2)
    j = lax.rem(lax.div(me, 2), NXY)
    z = lax.div(me, 2 * NXY)

    def dev(zz, jj, cc):
        return ((zz * NXY + jj) * 2 + cc,)

    zpeers = [lax.rem(z + k, NZ) for k in range(1, NZ)]
    xpeers = [lax.rem(j + k, NXY) for k in range(1, NXY)]
    oc = 1 - c
    slot = c * NXY + j

    def send(src, dst, ss, rs, to):
        pltpu.make_async_remote_copy(src_ref=src, dst_ref=dst, send_sem=ss, recv_sem=rs,
                                     device_id=to, device_id_type=MESH).start()

    def wait(ref, sem):
        pltpu.make_async_copy(ref, ref, sem).wait()

    bar = pltpu.get_barrier_semaphore()
    npeer = 0
    for zz in zpeers:
        pl.semaphore_signal(bar, inc=1, device_id=dev(zz, j, c), device_id_type=MESH); npeer += 1
    for jj in xpeers:
        for cc in (c, oc):
            pl.semaphore_signal(bar, inc=1, device_id=dev(z, jj, cc), device_id_type=MESH); npeer += 1
    pl.semaphore_signal(bar, inc=1, device_id=dev(z, j, oc), device_id_type=MESH); npeer += 1

    def tower(x, wi, wo, unit, inv, hid, act):
        a = dot(x[...], wi[...])
        h = jnp.maximum(a, 0.0).astype(bf16)
        e = dot(h, wo[...])
        r = lax.rsqrt(jnp.sum(e * e, axis=-1, keepdims=True) + EPS)
        u = e * r
        unit[...] = u
        inv[...] = jnp.broadcast_to(r, (R, 128))
        hid[...] = h
        act[...] = a
        return u.astype(bf16)

    u_bf = tower(qf, wqi, wqo, up, ui, uh, ua)
    v_bf = tower(vf, wvi, wvo, vp, vi, vh, va)
    u_all[pl.ds(z * R, R), :] = u_bf
    v_all[pl.ds(slot * R, R), :] = v_bf
    lq_all[slot] = lq[...]
    pos = jnp.sum(u_bf.astype(f32) * v_bf.astype(f32), axis=0, keepdims=True) * (1.0 / TEMP) - lq[...]
    stats[z, :, pl.ds(NQ + 128, 128)] = pos

    pl.semaphore_wait(bar, npeer)
    mine_v = v_all.at[pl.ds(slot * R, R), :]
    mine_u = u_all.at[pl.ds(z * R, R), :]
    for jj in xpeers:
        for cc in (c, oc):
            send(lq_all.at[slot], lq_all.at[slot], s_lq, r_lq, dev(z, jj, cc))
    send(lq_all.at[slot], lq_all.at[slot], s_lq, r_lq, dev(z, j, oc))
    for zz in zpeers:
        send(mine_u, mine_u, s_u, r_u.at[z], dev(zz, j, c))
    for jj in xpeers:
        send(mine_v, mine_v, s_v, r_v.at[slot], dev(z, jj, c))
    send(mine_v, mine_v, s_vr, r_v.at[slot], dev(z, j, oc))

    wait(lq_all.at[pl.ds(0, 2 * NXY - 1)], r_lq)
    m2 = jnp.max(-lq_all[...], axis=(0, 1, 2), keepdims=True)[0] * LOG2E
    m2 = jnp.broadcast_to(m2, (1, 128))
    stats[z, :, pl.ds(NQ, 128)] = m2

    def bias(k, _):
        row = lq_all[k] * LOG2E + m2
        bcol[pl.ds(k * R, R), :] = jnp.transpose(jnp.broadcast_to(row, (128, 128)))
        return 0
    lax.fori_loop(0, 2 * NXY, bias, 0)

    for k, jj in enumerate(xpeers):
        sl = c * NXY + jj
        ref = v_all.at[pl.ds(sl * R, R), :]
        wait(ref, r_v.at[sl])
        send(ref, ref, s_vr, r_v.at[sl], dev(z, j, oc))
    for zz in zpeers:
        wait(u_all.at[pl.ds(zz * R, R), :], r_u.at[zz])
    for jj in range(NXY):
        sl = oc * NXY + jj
        wait(v_all.at[pl.ds(sl * R, R), :], r_v.at[sl])

    csum[...] = jnp.zeros_like(csum)
    QC = min(256, NQ)

    def pass1(g, _):
        rows = pl.ds(g * 256, 256)
        vb = v_all[rows, :]
        bc = bcol[rows, :]
        for qc in range(NQ // QC):
            cols = slice(qc * QC, (qc + 1) * QC)
            s = dot(vb, u_all[cols, :], NT)
            e = jnp.exp2(s * (LOG2E / TEMP) - jnp.concatenate([bc] * (QC // 128), axis=1))
            e_all[rows, cols] = e
            csum[:, cols] += jnp.sum(e.reshape(32, 8, QC), axis=0)
        vt[:, rows] = jnp.transpose(vb.astype(f32)).astype(bf16)
        return 0
    lax.fori_loop(0, NI // 256, pass1, 0)

    stats[z, :, pl.ds(0, NQ)] = jnp.sum(csum[...], axis=0, keepdims=True)
    for zz in zpeers:
        send(stats.at[z], stats.at[z], s_st, r_st, dev(zz, j, c))
    wait(stats.at[pl.ds(0, NZ - 1)], r_st)
    ms = [stats[k, :, NQ:NQ + 128] for k in range(NZ)]
    mx = functools.reduce(jnp.maximum, ms)
    tot = jnp.zeros((1, NQ), f32)
    for k in range(NZ):
        w = jnp.exp2(ms[k] - mx)
        tot = tot + stats[k, :, 0:NQ] * jnp.concatenate([w] * NZ, axis=1)
    mine_w = jnp.exp2(m2 - mx)
    invl[...] = jnp.concatenate([mine_w] * NZ, axis=1) / tot
    lse = (jnp.log2(tot) + jnp.concatenate([mx] * NZ, axis=1)) * LN2
    lrow = jnp.zeros((1, 128), f32)
    for k in range(NZ):
        lrow = lrow + (lse[:, k * 128:(k + 1) * 128] - stats[k, :, NQ + 128:NQ + 256])
    loss_p[c] = lrow
    send(loss_p.at[c], loss_p.at[c], s_lp, r_lp, dev(z, j, oc))

    def g_block(g):
        rows = pl.ds(g * 256, 256)
        il = invl[...]
        g_all[rows, :] = (e_all[rows, :] * il).astype(bf16)

        @pl.when(lax.div(slot, 2) == g)
        def _():
            rr = pl.ds(slot * R, R)
            qq = pl.ds(pl.multiple_of(z * R, 128), R)
            eye = lax.broadcasted_iota(jnp.int32, (R, R), 0) == lax.broadcasted_iota(jnp.int32, (R, R), 1)
            p = e_all[rr, qq] * invl[:, qq]
            g_all[rr, qq] = jnp.where(eye, p - 1.0, p).astype(bf16)
        return dot(g_all[rows, :], u_all[...])

    def first_half(k, _):
        g = oc * (NXY // 2) + k
        d = g_block(g)
        for t in range(2):
            jj = 2 * k + t
            pv_out[jj] = d[t * 128:(t + 1) * 128, :]
            send(pv_out.at[jj], pv_in.at[jj], s_pv, r_pv.at[jj], dev(z, j, oc))
        return 0
    lax.fori_loop(0, NXY // 2, first_half, 0)

    def second_half(k, _):
        g = c * (NXY // 2) + k
        d = g_block(g)
        for t in range(2):
            jj = 2 * k + t
            wait(pv_in.at[jj], r_pv.at[jj])
            sv[jj] = d[t * 128:(t + 1) * 128, :] + pv_in[jj]

            @pl.when(jj != j)
            def _():
                send(sv.at[jj], rv.at[j], s_sv, r_sv, dev(z, jj, c))
        return 0
    lax.fori_loop(0, NXY // 2, second_half, 0)
    rv[j] = sv[j]

    def du_part(n, _):
        cols = pl.ds(pl.multiple_of(n * QC, 128), QC)
        d = dot(vt[...], g_all[:, cols])
        for t in range(QC // 128):
            zz = n * (QC // 128) + t
            su[zz] = d[:, t * 128:(t + 1) * 128]

            @pl.when(zz != z)
            def _():
                send(su.at[zz], ru.at[z], s_su, r_su, dev(zz, j, c))
        return 0
    lax.fori_loop(0, NQ // QC, du_part, 0)
    ru[z] = su[z]

    wait(loss_p.at[oc], r_lp)
    loss_x[j] = loss_p[0] + loss_p[1]
    for jj in xpeers:
        send(loss_x.at[j], loss_x.at[j], s_lx, r_lx, dev(z, jj, c))

    def backward(du, x, wo, unit, inv, hid, act, t):
        u, r = unit[...], inv[...]
        de = (r * (du - u * jnp.sum(u * du, axis=-1, keepdims=True))).astype(bf16)
        go = dot(hid[...], de, TN)
        dh = dot(de, wo[...], NT)
        da = jnp.where(act[...] > 0, dh, 0.0).astype(bf16)
        gi = dot(x[...], da, TN)
        gl[t, 0:256, :] = gi[:, 0:128]
        gl[t, 256:512, :] = gi[:, 128:256]
        gl[t, 512:768, :] = go

    scale = 1.0 / (TEMP * B)
    wait(ru.at[pl.ds(0, NZ - 1)], r_su)
    acc = ru[0]
    for k in range(1, NZ):
        acc = acc + ru[k]
    backward(jnp.transpose(acc) * scale, qf, wqo, up, ui, uh, ua, 0)

    wait(rv.at[pl.ds(0, NXY - 1)], r_sv)
    acc = rv[0]
    for k in range(1, NXY):
        acc = acc + rv[k]
    backward(acc * scale, vf, wvo, vp, vi, vh, va, 1)

    send(gl.at[oc], gpair, s_gp, r_gp, dev(z, j, oc))
    wait(gpair, r_gp)
    gx_s[...] = (gl[c] + gpair[...]).reshape(NXY, CH, 128)
    for jj in xpeers:
        send(gx_s.at[jj], gx_r.at[j], s_gx, r_gx, dev(z, jj, c))
    gx_r[j] = gx_s[j]
    wait(gx_r.at[pl.ds(0, NXY - 1)], r_gx)
    acc = gx_r[0]
    for k in range(1, NXY):
        acc = acc + gx_r[k]
    gz_r[z] = acc
    for zz in zpeers:
        send(gz_r.at[z], gz_r.at[z], s_gz, r_gz, dev(zz, j, c))
    wait(gz_r.at[pl.ds(0, NZ - 1)], r_gz)
    acc = gz_r[0]
    for k in range(1, NZ):
        acc = acc + gz_r[k]
    fin[c, j] = acc
    for jj in xpeers:
        send(fin.at[c, j], fin.at[c, j], s_ag, r_ag.at[j], dev(z, jj, c))
    send(fin.at[c, j], fin.at[c, j], s_rl, r_rl.at[j], dev(z, j, oc))
    for jj in xpeers:
        wait(fin.at[c, jj], r_ag.at[jj])
        send(fin.at[c, jj], fin.at[c, jj], s_rl, r_rl.at[jj], dev(z, j, oc))
    wait(loss_x.at[pl.ds(0, NXY - 1)], r_lx)
    ls = loss_x[0]
    for k in range(1, NXY):
        ls = ls + loss_x[k]
    loss_o[...] = jnp.broadcast_to(jnp.sum(ls, axis=-1, keepdims=True) * (1.0 / B), (1, 128))
    for jj in range(NXY):
        wait(fin.at[oc, jj], r_rl.at[jj])
    for t, (gi, go) in enumerate(((gqi_o, gqo_o), (gvi_o, gvo_o))):
        full = fin[t].reshape(768, 128)
        gi[:, 0:128] = full[0:256]
        gi[:, 128:256] = full[256:512]
        go[...] = full[512:768]

    for k in range(2 * NXY - 1):
        pass
    wait(lq_all.at[pl.ds(0, 2 * NXY - 1)], s_lq)
    wait(u_all.at[pl.ds(0, (NZ - 1) * R), :], s_u)
    wait(v_all.at[pl.ds(0, (NXY - 1) * R), :], s_v)
    wait(v_all.at[pl.ds(0, NXY * R), :], s_vr)
    wait(stats.at[pl.ds(0, NZ - 1)], s_st)
    wait(loss_p.at[0], s_lp)
    wait(pv_out, s_pv)
    wait(sv.at[pl.ds(0, NXY - 1)], s_sv)
    wait(su.at[pl.ds(0, NZ - 1)], s_su)
    wait(loss_x.at[pl.ds(0, NXY - 1)], s_lx)
    wait(gpair, s_gp)
    wait(gx_s.at[pl.ds(0, NXY - 1)], s_gx)
    wait(gz_r.at[pl.ds(0, NZ - 1)], s_gz)
    wait(gx_s.at[pl.ds(0, NXY - 1)], s_ag)
    wait(gx_s, s_rl)


def build(NZ, NXY):
    def step(query_feat, item_feat, log_q, w_query_in, w_query_out, w_item_in, w_item_out):
        R = 128
        NQ, NI, CH = NZ * R, 2 * NXY * R, 768 // NXY
        V = pltpu.VMEM
        vm = pl.BlockSpec(memory_space=pltpu.VMEM)
        S = pltpu.SemaphoreType.DMA
        out = pl.pallas_call(
            functools.partial(kernel, NZ, NXY),
            name="two_tower",
            out_shape=[jax.ShapeDtypeStruct((256, 256), f32), jax.ShapeDtypeStruct((256, 128), f32),
                       jax.ShapeDtypeStruct((256, 256), f32), jax.ShapeDtypeStruct((256, 128), f32),
                       jax.ShapeDtypeStruct((1, 128), f32)],
            in_specs=[vm] * 7,
            out_specs=[vm] * 5,
            scratch_shapes=[
                V((NQ, 128), bf16), V((NI, 128), bf16), V((128, NI), bf16), V((2 * NXY, 1, 128), f32),
                V((NI, 128), f32), V((NI, NQ), f32), V((NI, NQ), bf16), V((8, NQ), f32),
                V((NZ, 1, NQ + 256), f32), V((1, NQ), f32),
                V((R, 128), f32), V((R, 128), f32), V((R, 256), bf16), V((R, 256), f32),
                V((R, 128), f32), V((R, 128), f32), V((R, 256), bf16), V((R, 256), f32),
                V((NZ, 128, 128), f32), V((NZ, 128, 128), f32),
                V((NXY, 128, 128), f32), V((NXY, 128, 128), f32), V((NXY, 128, 128), f32), V((NXY, 128, 128), f32),
                V((2, 768, 128), f32), V((768, 128), f32), V((NXY, CH, 128), f32), V((NXY, CH, 128), f32),
                V((NZ, CH, 128), f32), V((2, NXY, CH, 128), f32), V((2, 1, 128), f32), V((NXY, 1, 128), f32),
                S, S((NZ,)), S, S((2 * NXY,)), S, S, S, S, S, S((NXY,)), S, S, S, S,
                S, S, S, S, S, S, S, S((NXY,)), S, S((NXY,)), S, S, S, S, S,
            ],
            compiler_params=pltpu.CompilerParams(collective_id=0, has_side_effects=True, vmem_limit_bytes=60 * 2**20),
        )(query_feat, item_feat, log_q.reshape(1, 128), w_query_in, w_query_out, w_item_in, w_item_out)
        gqi, gqo, gvi, gvo, loss = out
        return loss[0, 0:1], gqi, gqo, gvi, gvo
    return step


def solution(mesh):
    n = mesh.shape["dp"]
    NZ, NXY = (8, 16) if n == 256 else (2, 4)
    return jax.shard_map(build(NZ, NXY), mesh=mesh,
                         in_specs=(P("dp", None), P("dp", None), P("dp"), P(), P(), P(), P()),
                         out_specs=(P(), P(), P(), P(), P()), check_vma=False)
```

```python
import functools

import jax
import jax.numpy as jnp
from jax import lax
from jax.experimental import pallas as pl
from jax.experimental.pallas import tpu as pltpu
from jax.sharding import PartitionSpec as P

f32, bf16 = jnp.float32, jnp.bfloat16
MESH = pl.DeviceIdType.MESH
TEMP = 0.05
EPS = 1e-6
LOG2E = 1.4426950408889634
LN2 = 0.6931471805599453
NT = (((1,), (1,)), ((), ()))
TN = (((0,), (0,)), ((), ()))
NN = (((1,), (0,)), ((), ()))
R = 128
GR = 256


class Scope:
    def __init__(self):
        self.cur = None

    def __call__(self, name):
        if self.cur is not None:
            self.cur.__exit__(None, None, None)
        self.cur = None
        if name:
            self.cur = jax.named_scope(name)
            self.cur.__enter__()


def dot(a, b, dims=NN):
    return lax.dot_general(a, b, dims, preferred_element_type=f32)


def ring(n):
    return sorted(range(n), key=lambda k: (min(k, n - k), k))


def torus(ny, nx):
    def dist(o):
        return min(o[0], ny - o[0]) + min(o[1], nx - o[1])
    return sorted(((a, b) for a in range(ny) for b in range(nx)), key=lambda o: (dist(o), o))


def kernel(NZ, NY, NX, qf_h, vf_h, lq_h, wqi_h, wqo_h, wvi_h, wvo_h, fin, loss_o,
           qf, vf, lq, wqi, wqo, wvi, wvo, s_in,
           u_all, v_all, vt, lq_all, bcol, e_all, g_all, csum, stats, invl, invt,
           up, ui, uh, ua, vp, vi, vh, va,
           su, ru, pv_out, pv_in, sv, rv, gl, gpair, gx_s, gx_r, gz_r, loss_p, loss_x,
           s_u, r_u, s_v, r_v, s_lq, r_lq, s_st, r_st, s_pv, r_pv, s_sv, r_sv, s_su, r_su,
           s_gp, r_gp, s_gx, r_gx, s_gz, r_gz, s_ag, r_ag, s_rl, r_rl, s_lp, r_lp, s_lx, r_lx, s_vr):
    sc = Scope()
    NXY = NY * NX
    NQ = NZ * R
    NI = 2 * NXY * R
    B = NZ * NI
    CH = 384 // NXY
    LV = NZ // 2
    SL = NXY // LV
    QC = 2 * R
    IR = 2 * SL * R
    NG = IR // GR
    zoff, xoff = ring(NZ), torus(NY, NX)
    me = lax.axis_index("dp")
    c = lax.rem(me, 2)
    j = lax.rem(lax.div(me, 2), NXY)
    y, x = lax.div(j, NX), lax.rem(j, NX)
    z = lax.div(me, 2 * NXY)
    oc = 1 - c

    def dev(zz, jj, cc):
        return ((zz * NXY + jj) * 2 + cc,)

    def zs(k, sign):
        o = zoff[k]
        return lax.rem(z + (o if sign > 0 else NZ - o), NZ)

    def xs(k, sign):
        a, b = xoff[k]
        yy = lax.rem(y + (a if sign > 0 else NY - a), NY)
        xx = lax.rem(x + (b if sign > 0 else NX - b), NX)
        return yy * NX + xx

    def slot(k, core):
        return (k // SL) * 2 * SL + core * SL + k % SL

    def send(src, dst, ss, rs, to):
        pltpu.make_async_remote_copy(src_ref=src, dst_ref=dst, send_sem=ss, recv_sem=rs,
                                     device_id=to, device_id_type=MESH).start()

    def wait(ref, sem):
        pltpu.make_async_copy(ref, ref, sem).wait()

    def vrows(s):
        return v_all.at[pl.ds(s * R, R), :]

    sc("barsig")
    bar = pltpu.get_barrier_semaphore()
    peers = [dev(zs(k, 1), j, c) for k in range(1, NZ)]
    peers += [dev(z, xs(k, 1), cc) for k in range(1, NXY) for cc in (c, oc)]
    peers += [dev(z, j, oc)]
    for p in peers:
        pl.semaphore_signal(bar, inc=1, device_id=p, device_id_type=MESH)
    loads = [pltpu.make_async_copy(a, b, s_in.at[i]) for i, (a, b) in enumerate(
        ((qf_h, qf), (wqi_h, wqi), (wqo_h, wqo), (vf_h, vf), (wvi_h, wvi), (wvo_h, wvo), (lq_h, lq)))]
    for cp in loads:
        cp.start()
    for cp in loads:
        cp.wait()

    sc("tower")

    def tower(xr, wi, wo, unit, inv, hid, act):
        a = dot(xr[...], wi[...])
        h = jnp.maximum(a, 0.0).astype(bf16)
        e = dot(h, wo[...])
        r = lax.rsqrt(jnp.sum(e * e, axis=-1, keepdims=True) + EPS)
        u = e * r
        unit[...] = u
        inv[...] = jnp.broadcast_to(r, (R, 128))
        hid[...] = h
        act[...] = a
        return u.astype(bf16)

    u_bf = tower(qf, wqi, wqo, up, ui, uh, ua)
    v_bf = tower(vf, wvi, wvo, vp, vi, vh, va)
    u_all[0:R, :] = u_bf
    v_all[0:R, :] = v_bf
    lq_all[0] = lq[...]
    pos = jnp.sum(u_bf.astype(f32) * v_bf.astype(f32), axis=0, keepdims=True) * (1.0 / TEMP) - lq[...]
    stats[z, :, pl.ds(NQ + 128, 128)] = pos
    csum[...] = jnp.zeros_like(csum)

    sc("barwait")
    pl.semaphore_wait(bar, len(peers))
    sc("sends")
    mine_u, mine_v = u_all.at[pl.ds(0, R), :], vrows(0)
    for k in range(1, NXY):
        for core, cc in ((0, c), (1, oc)):
            send(lq_all.at[0], lq_all.at[slot(k, core)], s_lq, r_lq, dev(z, xs(k, 1), cc))
    send(lq_all.at[0], lq_all.at[slot(0, 1)], s_lq, r_lq, dev(z, j, oc))
    send(mine_v, vrows(slot(0, 1)), s_vr, r_v.at[slot(0, 1)], dev(z, j, oc))
    for k in range(1, NXY):
        if k < NZ:
            send(mine_u, u_all.at[pl.ds(k * R, R), :], s_u, r_u.at[k], dev(zs(k, 1), j, c))
        send(mine_v, vrows(slot(k, 0)), s_v, r_v.at[slot(k, 0)], dev(z, xs(k, 1), c))

    sc("lqwait")
    wait(lq_all.at[pl.ds(0, 2 * NXY - 1)], r_lq)
    sc("bias")
    nl = -lq_all[...].reshape(2 * NXY, 128)
    m2 = jnp.max(jnp.max(nl, axis=0, keepdims=True), axis=1, keepdims=True) * LOG2E
    m2 = jnp.broadcast_to(m2, (1, 128))
    stats[z, :, pl.ds(NQ, 128)] = m2
    bt = jnp.transpose(m2 - nl * LOG2E)
    for s in range(2 * NXY):
        bcol[s * R:(s + 1) * R, :] = jnp.broadcast_to(bt[:, s:s + 1], (R, 128))

    def block(rows, cols):
        s = dot(v_all[rows, :], u_all[cols, :], NT)
        b = bcol[rows, :]
        e = jnp.exp2(s * (LOG2E / TEMP) - jnp.concatenate([b, b], axis=1))
        e_all[rows, cols] = e
        csum[:, cols] += jnp.sum(e.reshape(GR // 8, 8, QC), axis=0)

    def grp(g):
        return pl.ds(pl.multiple_of(g * GR, GR), GR)

    def qcols(l):
        return slice(l * QC, (l + 1) * QC)

    def new_items(l, g):
        for l2 in range(l + 1):
            block(grp(g), qcols(l2))
        vt[:, grp(g)] = jnp.transpose(v_all[grp(g), :].astype(f32)).astype(bf16)

    def loop(lo, n, f):
        lax.fori_loop(0, n, lambda i, u: (f(lo + i), u)[1], 0)

    for l in range(LV):
        sc(f"uwait{l}")
        for k in (2 * l, 2 * l + 1):
            if k:
                wait(u_all.at[pl.ds(k * R, R), :], r_u.at[k])
        sc(f"vwait{l}")
        for k in range(l * SL, (l + 1) * SL):
            if k:
                s = slot(k, 0)
                wait(vrows(s), r_v.at[s])
                send(vrows(s), vrows(slot(k, 1)), s_vr, r_v.at[slot(k, 1)], dev(z, j, oc))
        sc(f"pass1_{l}a")
        if l:
            loop(0, l * NG, lambda g: block(grp(g), qcols(l)))
        sc(f"pass1_{l}b")
        loop(l * NG, NG // 2, functools.partial(new_items, l))
        sc(f"vwait{l}p")
        for k in range(l * SL, (l + 1) * SL):
            s = slot(k, 1)
            wait(vrows(s), r_v.at[s])
        sc(f"pass1_{l}c")
        loop(l * NG + NG // 2, NG // 2, functools.partial(new_items, l))

    sc("stats_send")
    tot = jnp.sum(csum[...], axis=0, keepdims=True)
    for k in range(NZ):
        stats[z, :, pl.ds(pl.multiple_of(zs(k, -1) * R, R), R)] = tot[:, k * R:(k + 1) * R]
    for k in range(1, NZ):
        send(stats.at[z], stats.at[z], s_st, r_st, dev(zs(k, 1), j, c))
    sc("stats_wait")
    wait(stats.at[pl.ds(0, NZ - 1)], r_st)
    sc("stats_comp")
    ms = [stats[k, :, NQ:NQ + 128] for k in range(NZ)]
    mx = functools.reduce(jnp.maximum, ms)
    tot = jnp.zeros((1, NQ), f32)
    for k in range(NZ):
        tot = tot + stats[k, :, 0:NQ] * jnp.concatenate([jnp.exp2(ms[k] - mx)] * NZ, axis=1)
    invt[...] = jnp.concatenate([jnp.exp2(m2 - mx)] * NZ, axis=1) / tot
    for k in range(NZ):
        invl[:, k * R:(k + 1) * R] = invt[:, pl.ds(pl.multiple_of(zs(k, -1) * R, R), R)]
    lse = (jnp.log2(tot) + jnp.concatenate([mx] * NZ, axis=1)) * LN2
    lrow = jnp.zeros((1, 128), f32)
    for k in range(NZ):
        lrow = lrow + (lse[:, k * R:(k + 1) * R] - stats[k, :, NQ + 128:NQ + 256])
    loss_p[c] = lrow
    send(loss_p.at[c], loss_p.at[c], s_lp, r_lp, dev(z, j, oc))

    def norm(rows, c0, c1):
        cols = slice(c0 * QC, c1 * QC)
        g_all[rows, cols] = (e_all[rows, cols] * invl[:, cols]).astype(bf16)

    def dv(g):
        return dot(g_all[g * GR:(g + 1) * GR, :], u_all[...])

    pend = []

    def flush():
        for k in pend:
            wait(pv_in.at[k], r_pv.at[k])
            sv[k] = sv[k] + pv_in[k]
            if k:
                send(sv.at[k], rv.at[k], s_sv, r_sv, dev(z, xs(k, -1), c))
        pend.clear()

    def dv_level(l, c0, c1):
        sc(f"dv{l}")
        for t in range(SL // 2):
            for core in (1, 0):
                g = l * NG + core * (NG // 2) + t
                if c1 > c0:
                    norm(slice(g * GR, (g + 1) * GR), c0, c1)
                d = dv(g)
                ks = (l * SL + 2 * t, l * SL + 2 * t + 1)
                for i, k in enumerate(ks):
                    if core:
                        pv_out[k] = d[i * R:(i + 1) * R, :]
                        send(pv_out.at[k], pv_in.at[k], s_pv, r_pv.at[k], dev(z, j, oc))
                    else:
                        sv[k] = d[i * R:(i + 1) * R, :]
            flush()
            pend.extend(ks)

    def du_level(l, nrows):
        sc(f"du{l}")
        loop(0, nrows // GR, lambda g: norm(grp(g), l, l + 1))
        if l == 0:
            eye = lax.broadcasted_iota(jnp.int32, (R, R), 0) == lax.broadcasted_iota(jnp.int32, (R, R), 1)
            p = e_all[0:R, 0:R] * invl[:, 0:R]
            g_all[0:R, 0:R] = jnp.where(eye, p - 1.0, p).astype(bf16)
        d = dot(vt[...], g_all[:, qcols(l)])
        for i in range(2):
            k = 2 * l + i
            su[k] = d[:, i * R:(i + 1) * R]
            if k:
                send(su.at[k], ru.at[k], s_su, r_su, dev(zs(k, -1), j, c))

    dv_level(LV - 1, 0, LV)
    half = (LV + 1) // 2
    for l in range(LV - 1, half - 1, -1):
        du_level(l, (LV - 1) * IR)
    if LV > 2:
        dv_level(LV - 2, 0, half)
    rest = LV - 2 if LV > 2 else LV - 1
    for l in range(half - 1, -1, -1):
        du_level(l, rest * IR)
    for l in range(rest - 1, -1, -1):
        dv_level(l, 0, 0)
    sc("flush")
    flush()

    sc("loss")
    wait(loss_p.at[oc], r_lp)
    loss_x[j] = loss_p[0] + loss_p[1]
    for k in range(1, NXY):
        send(loss_x.at[j], loss_x.at[j], s_lx, r_lx, dev(z, xs(k, 1), c))

    def backward(du, xr, wo, unit, inv, hid, act, t):
        u, r = unit[...], inv[...]
        de = (r * (du - u * jnp.sum(u * du, axis=-1, keepdims=True))).astype(bf16)
        go = dot(hid[...], de, TN)
        dh = dot(de, wo[...], NT)
        da = jnp.where(act[...] > 0, dh, 0.0).astype(bf16)
        gi = dot(xr[...], da, TN)
        gl[t, 0:256, :] = gi[:, 0:128]
        gl[t, 256:512, :] = gi[:, 128:256]
        gl[t, 512:768, :] = go
        send(gl.at[t, pl.ds(pl.multiple_of(oc * 384, 8), 384), :], gpair.at[t], s_gp.at[t], r_gp.at[t], dev(z, j, oc))

    def pair_sum(t):
        sc(f"gp_wait{t}")
        wait(gpair.at[t], r_gp.at[t])
        gx_s[t] = (gl[t, pl.ds(pl.multiple_of(c * 384, 8), 384), :] + gpair[t]).reshape(NXY, CH, 128)
        for k in range(1, NXY):
            to = xs(k, 1)
            send(gx_s.at[t, to], gx_r.at[t, j], s_gx.at[t], r_gx.at[t], dev(z, to, c))
        gx_r[t, j] = gx_s[t, j]

    def plane_sum(t):
        sc(f"gx_wait{t}")
        wait(gx_r.at[t, pl.ds(0, NXY - 1)], r_gx.at[t])
        acc = gx_r[t, 0]
        for k in range(1, NXY):
            acc = acc + gx_r[t, k]
        gz_r[t, z] = acc
        for k in range(1, NZ):
            send(gz_r.at[t, z], gz_r.at[t, z], s_gz.at[t], r_gz.at[t], dev(zs(k, 1), j, c))

    def ring_sum(t):
        sc(f"gz_wait{t}")
        wait(gz_r.at[t, pl.ds(0, NZ - 1)], r_gz.at[t])
        acc = gz_r[t, 0]
        for k in range(1, NZ):
            acc = acc + gz_r[t, k]
        fin[t, c, j] = acc
        for k in range(1, NXY):
            send(fin.at[t, c, j], fin.at[t, c, j], s_ag.at[t], r_ag.at[t, k], dev(z, xs(k, 1), c))
        send(fin.at[t, c, j], fin.at[t, c, j], s_rl.at[t], r_rl.at[t, 0], dev(z, j, oc))

    def relay(t):
        sc(f"ag_wait{t}")
        for k in range(1, NXY):
            ref = fin.at[t, c, xs(k, -1)]
            wait(ref, r_ag.at[t, k])
            send(ref, ref, s_rl.at[t], r_rl.at[t, k], dev(z, j, oc))

    scale = 1.0 / (TEMP * B)
    sc("ru_wait")
    wait(ru.at[pl.ds(0, NZ - 1)], r_su)
    sc("bwd_q")
    acc = su[0]
    for k in range(1, NZ):
        acc = acc + ru[k]
    backward(jnp.transpose(acc) * scale, qf, wqo, up, ui, uh, ua, 0)
    pair_sum(0)
    sc("rv_wait")
    wait(rv.at[pl.ds(0, NXY - 1)], r_sv)
    sc("bwd_v")
    acc = sv[0]
    for k in range(1, NXY):
        acc = acc + rv[k]
    backward(acc * scale, vf, wvo, vp, vi, vh, va, 1)
    pair_sum(1)
    plane_sum(0)
    plane_sum(1)
    ring_sum(0)
    ring_sum(1)
    relay(0)
    relay(1)
    sc("loss2")
    wait(loss_x.at[pl.ds(0, NXY - 1)], r_lx)
    ls = loss_x[0]
    for k in range(1, NXY):
        ls = ls + loss_x[k]
    loss_o[...] = jnp.broadcast_to(jnp.sum(ls, axis=-1, keepdims=True) * (1.0 / B), (1, 128))
    sc("rl_wait")
    for t in range(2):
        for k in range(NXY):
            wait(fin.at[t, oc, xs(k, -1)], r_rl.at[t, k])

    sc("sendwait")
    wait(lq_all.at[pl.ds(0, 2 * NXY - 1)], s_lq)
    wait(u_all.at[pl.ds(0, (NZ - 1) * R), :], s_u)
    wait(v_all.at[pl.ds(0, (NXY - 1) * R), :], s_v)
    wait(v_all.at[pl.ds(0, NXY * R), :], s_vr)
    wait(stats.at[pl.ds(0, NZ - 1)], s_st)
    wait(loss_p.at[0], s_lp)
    wait(pv_out, s_pv)
    wait(sv.at[pl.ds(0, NXY - 1)], s_sv)
    wait(su.at[pl.ds(0, NZ - 1)], s_su)
    wait(loss_x.at[pl.ds(0, NXY - 1)], s_lx)
    for t in range(2):
        wait(gpair.at[t], s_gp.at[t])
        wait(gx_s.at[t, pl.ds(0, NXY - 1)], s_gx.at[t])
        wait(gz_r.at[t, pl.ds(0, NZ - 1)], s_gz.at[t])
        wait(gx_s.at[t, pl.ds(0, NXY - 1)], s_ag.at[t])
        wait(gx_s.at[t], s_rl.at[t])
    sc(None)


def emit(fin, loss, gqi, gqo, gvi, gvo, loss_o):
    for t, (gi, go) in enumerate(((gqi, gqo), (gvi, gvo))):
        gi[:, 0:128] = fin[t, 0:256]
        gi[:, 128:256] = fin[t, 256:512]
        go[...] = fin[t, 512:768]
    loss_o[...] = loss[...]


def build(NZ, NY, NX):
    def step(query_feat, item_feat, log_q, w_query_in, w_query_out, w_item_in, w_item_out):
        NXY = NY * NX
        NQ, NI, CH = NZ * R, 2 * NXY * R, 384 // NXY
        V, S = pltpu.VMEM, pltpu.SemaphoreType.DMA
        vm, hbm = pl.BlockSpec(memory_space=pltpu.VMEM), pl.BlockSpec(memory_space=pl.ANY)
        sd = jax.ShapeDtypeStruct
        tower = [V((R, 128), f32), V((R, 128), f32), V((R, 256), bf16), V((R, 256), f32)]
        fin, loss = pl.pallas_call(
            functools.partial(kernel, NZ, NY, NX),
            name="two_tower",
            out_shape=[sd((2, 2, NXY, CH, 128), f32), sd((1, 128), f32)],
            in_specs=[hbm] * 7,
            out_specs=[vm] * 2,
            scratch_shapes=[
                V((R, 256), bf16), V((R, 256), bf16), V((1, 128), f32),
                V((256, 256), bf16), V((256, 128), bf16), V((256, 256), bf16), V((256, 128), bf16), S((7,)),
                V((NQ, 128), bf16), V((NI, 128), bf16), V((128, NI), bf16), V((2 * NXY, 1, 128), f32),
                V((NI, 128), f32), V((NI, NQ), f32), V((NI, NQ), bf16), V((8, NQ), f32),
                V((NZ, 1, NQ + 256), f32), V((1, NQ), f32), V((1, NQ), f32),
                *tower, *tower,
                V((NZ, 128, 128), f32), V((NZ, 128, 128), f32),
                V((NXY, 128, 128), f32), V((NXY, 128, 128), f32), V((NXY, 128, 128), f32), V((NXY, 128, 128), f32),
                V((2, 768, 128), f32), V((2, 384, 128), f32), V((2, NXY, CH, 128), f32), V((2, NXY, CH, 128), f32),
                V((2, NZ, CH, 128), f32), V((2, 1, 128), f32), V((NXY, 1, 128), f32),
                S, S((NZ,)), S, S((2 * NXY,)), S, S, S, S, S, S((NXY,)), S, S, S, S,
                S((2,)), S((2,)), S((2,)), S((2,)), S((2,)), S((2,)), S((2,)), S((2, NXY)), S((2,)), S((2, NXY)),
                S, S, S, S, S,
            ],
            compiler_params=pltpu.CompilerParams(collective_id=0, has_side_effects=True, vmem_limit_bytes=60 * 2**20),
        )(query_feat, item_feat, log_q.reshape(1, 128), w_query_in, w_query_out, w_item_in, w_item_out)
        gqi, gqo, gvi, gvo, out = pl.pallas_call(
            emit,
            name="emit",
            out_shape=[sd((256, 256), f32), sd((256, 128), f32), sd((256, 256), f32), sd((256, 128), f32), sd((1, 128), f32)],
            in_specs=[vm] * 2,
            out_specs=[vm] * 5,
        )(fin.reshape(2, 768, 128), loss)
        return out[0, 0:1], gqi, gqo, gvi, gvo
    return step


def solution(mesh):
    n = mesh.shape["dp"]
    dims = (8, 4, 4) if n == 256 else (4, 2, 2)
    return jax.shard_map(build(*dims), mesh=mesh,
                         in_specs=(P("dp", None), P("dp", None), P("dp"), P(), P(), P(), P()),
                         out_specs=(P(), P(), P(), P(), P()), check_vma=False)
```

```python
import functools

import jax
import jax.numpy as jnp
from jax import lax
from jax.experimental import pallas as pl
from jax.experimental.pallas import tpu as pltpu
from jax.sharding import PartitionSpec as P

f32, bf16 = jnp.float32, jnp.bfloat16
MESH = pl.DeviceIdType.MESH
TEMP = 0.05
EPS = 1e-6
LOG2E = 1.4426950408889634
LN2 = 0.6931471805599453
NT = (((1,), (1,)), ((), ()))
TN = (((0,), (0,)), ((), ()))
NN = (((1,), (0,)), ((), ()))
R = 128
GR = 256
H = R // 2


class Scope:
    def __init__(self):
        self.cur = None

    def __call__(self, name):
        if self.cur is not None:
            self.cur.__exit__(None, None, None)
        self.cur = None
        if name:
            self.cur = jax.named_scope(name)
            self.cur.__enter__()


def dot(a, b, dims=NN):
    return lax.dot_general(a, b, dims, preferred_element_type=f32)


def ring(n):
    return sorted(range(n), key=lambda k: (min(k, n - k), k))


def torus(ny, nx):
    def dist(o):
        return min(o[0], ny - o[0]) + min(o[1], nx - o[1])
    return sorted(((a, b) for a in range(ny) for b in range(nx)), key=lambda o: (dist(o), o))


def kernel(NZ, NY, NX, qf_h, vf_h, lq_h, wqi_h, wqo_h, wvi_h, wvo_h, fin, loss_o,
           qf, vf, lq, wqi, wqo, wvi, wvo, s_in,
           u_all, v_all, vt, lq_all, mslot, wslot, cnt, bcol, sbuf, e_all, g_all, csum, stats, invl, invt,
           up, ui, uh, ua, vp, vi, vh, va,
           su, ru, hop_in, pv_out, pv_in, sv, rx, ry, tx, ty, r2x, r2y, t_cnt, gl, gpair, gx_s, gx_r, gz_r, loss_p, loss_x,
           s_u, r_u, s_v, r_v, s_lq, s_st, r_st, s_pv, r_pv, s_p1, s_p2, r_x, r_y, r_2x, r_2y, s_su, r_su, r_hop,
           s_gp, r_gp, s_gx, r_gx, s_gz, r_gz, s_ag, r_ag, s_rl, r_rl, s_lp, r_lp, s_lx, r_lx, s_vr):
    sc = Scope()
    NXY = NY * NX
    NQ = NZ * R
    NI = 2 * NXY * R
    B = NZ * NI
    CH = 384 // NXY
    LV = NZ // 2
    SL = NXY // LV
    QC = 2 * R
    IR = 2 * SL * R
    NG = IR // GR
    zoff, xoff = ring(NZ), torus(NY, NX)
    me = lax.axis_index("dp")
    c = lax.rem(me, 2)
    j = lax.rem(lax.div(me, 2), NXY)
    y, x = lax.div(j, NX), lax.rem(j, NX)
    z = lax.div(me, 2 * NXY)
    oc = 1 - c

    def dev(zz, jj, cc):
        return ((zz * NXY + jj) * 2 + cc,)

    def zs(k, sign):
        o = zoff[k]
        return lax.rem(z + (o if sign > 0 else NZ - o), NZ)

    def xs(k, sign):
        a, b = xoff[k]
        yy = lax.rem(y + (a if sign > 0 else NY - a), NY)
        xx = lax.rem(x + (b if sign > 0 else NX - b), NX)
        return yy * NX + xx

    def slot(k, core):
        return (k // SL) * 2 * SL + core * SL + k % SL

    def send(src, dst, ss, rs, to):
        pltpu.make_async_remote_copy(src_ref=src, dst_ref=dst, send_sem=ss, recv_sem=rs,
                                     device_id=to, device_id_type=MESH).start()

    def wait(ref, sem):
        pltpu.make_async_copy(ref, ref, sem).wait()

    def vrows(s):
        return v_all.at[pl.ds(s * R, R), :]

    sc("barsig")
    bar = pltpu.get_barrier_semaphore()
    peers = [dev(zs(k, 1), j, c) for k in range(1, NZ)]
    peers += [dev(z, xs(k, 1), c) for k in range(1, NXY)]
    peers += [dev(z, j, oc)]
    for p in peers:
        pl.semaphore_signal(bar, inc=1, device_id=p, device_id_type=MESH)
    loads = [pltpu.make_async_copy(a, b, s_in.at[i]) for i, (a, b) in enumerate(
        ((qf_h, qf), (wqi_h, wqi), (wqo_h, wqo), (vf_h, vf), (wvi_h, wvi), (wvo_h, wvo), (lq_h, lq)))]
    for cp in loads:
        cp.start()
    for cp in loads:
        cp.wait()

    sc("tower")

    def tower(xr, wi, wo, unit, inv, hid, act):
        a = dot(xr[...], wi[...])
        h = jnp.maximum(a, 0.0).astype(bf16)
        e = dot(h, wo[...])
        r = lax.rsqrt(jnp.sum(e * e, axis=-1, keepdims=True) + EPS)
        u = e * r
        unit[...] = u
        inv[...] = jnp.broadcast_to(r, (R, 128))
        hid[...] = h
        act[...] = a
        return u.astype(bf16)

    u_bf = tower(qf, wqi, wqo, up, ui, uh, ua)
    v_bf = tower(vf, wvi, wvo, vp, vi, vh, va)
    u_all[0:R, :] = u_bf
    v_all[0:R, :] = v_bf
    lq_all[0] = lq[...]
    pos = jnp.sum(u_bf.astype(f32) * v_bf.astype(f32), axis=0, keepdims=True) * (1.0 / TEMP) - lq[...]
    stats[z, :, pl.ds(NQ + 128, 128)] = pos

    sc("barwait")
    pl.semaphore_wait(bar, len(peers))
    sc("sends")
    mine_u = u_all.at[pl.ds(0, R), :]

    def send_item(s, s2, ss, to):
        send(lq_all.at[s], lq_all.at[s2], s_lq, r_v.at[s2], to)
        send(vrows(s), vrows(s2), ss, r_v.at[s2], to)

    send_item(0, slot(0, 1), s_vr, dev(z, j, oc))
    for k in range(1, NXY):
        if k < NZ:
            send(mine_u, u_all.at[pl.ds(k * R, R), :], s_u, r_u.at[k], dev(zs(k, 1), j, c))
        send_item(0, slot(k, 0), s_v, dev(z, xs(k, 1), c))

    def grp(g):
        return slice(g * GR, (g + 1) * GR)

    def dyn(g):
        return pl.ds(pl.multiple_of(g * GR, GR), GR)

    def qcols(l):
        return slice(l * QC, (l + 1) * QC)

    def loop(lo, n, f):
        lax.fori_loop(0, n, lambda i, u: (f(lo + i), u)[1], 0)

    def bias(s0):
        q = lq_all[s0:s0 + SL].reshape(SL, 128)
        big = jnp.max(-q, axis=1, keepdims=True)
        b = (big + q) * LOG2E
        bt = jnp.transpose(jnp.concatenate([b] * (8 // SL), axis=0))
        for i in range(SL):
            mslot[s0 + i] = jnp.broadcast_to(big[i:i + 1, :], (1, 128))
            bcol[(s0 + i) * R:(s0 + i + 1) * R, :] = jnp.broadcast_to(bt[:, i:i + 1], (R, 128))

    def expo(n, g, l):
        rows, cols = grp(g), qcols(l)
        bb = bcol[rows, :]
        e = jnp.exp2(sbuf[n % 2] * (LOG2E / TEMP) - jnp.concatenate([bb, bb], axis=1))
        e_all[rows, cols] = e
        csum[2 * g:2 * g + 2, :, cols] = jnp.sum(e.reshape(2, R // 8, 8, QC), axis=1)

    def groups(l, core):
        return [l * NG + core * (NG // 2) + t for t in range(NG // 2)]

    done = []
    for l in range(LV + 1):
        sc(f"wait{l}")
        fresh = []
        if l < LV:
            for k in range(l * SL, (l + 1) * SL):
                if k:
                    wait(cnt, r_v.at[slot(k, 0)])
                    send_item(slot(k, 0), slot(k, 1), s_vr, dev(z, j, oc))
            for k in (2 * l, 2 * l + 1):
                if k:
                    wait(u_all.at[pl.ds(k * R, R), :], r_u.at[k])
            fresh += groups(l, 0)
        if l:
            for k in range((l - 1) * SL, l * SL):
                wait(cnt, r_v.at[slot(k, 1)])
            fresh += groups(l - 1, 1)
        sc(f"pass1_{l}")
        if l < LV:
            bias(slot(l * SL, 0))
        if l:
            bias(slot((l - 1) * SL, 1))
        tasks = [(g, l2) for g in fresh for l2 in range(min(l, LV - 1) + 1)]
        if l < LV:
            old = [g for g in range(LV * NG) if g in done]
            tasks = [(g, l) for g in old] + tasks
        done += fresh
        for g in fresh:
            vt[:, grp(g)] = jnp.transpose(v_all[grp(g), :].astype(f32)).astype(bf16)
        for n, (g, l2) in enumerate(tasks):
            sbuf[n % 2] = dot(v_all[grp(g), :], u_all[qcols(l2), :], NT)
            if n:
                expo(n - 1, *tasks[n - 1])
        expo(len(tasks) - 1, *tasks[-1])

    sc("stats_send")
    big = jnp.max(mslot[...], axis=0)
    stats[z, :, pl.ds(NQ, 128)] = big
    wslot[...] = jnp.exp2((mslot[...] - big) * LOG2E)
    for k in range(NZ):
        acc = csum[0, :, k * R:(k + 1) * R] * wslot[0]
        for s in range(1, 2 * NXY):
            acc = acc + csum[s, :, k * R:(k + 1) * R] * wslot[s]
        stats[z, :, pl.ds(pl.multiple_of(zs(k, -1) * R, R), R)] = jnp.sum(acc, axis=0, keepdims=True)
    for k in range(1, NZ):
        send(stats.at[z], stats.at[z], s_st, r_st, dev(zs(k, 1), j, c))
    sc("stats_wait")
    wait(stats.at[pl.ds(0, NZ - 1)], r_st)
    sc("stats_comp")
    ms = [stats[k, :, NQ:NQ + 128] for k in range(NZ)]
    mx = functools.reduce(jnp.maximum, ms)
    tot = jnp.zeros((1, NQ), f32)
    for k in range(NZ):
        tot = tot + stats[k, :, 0:NQ] * jnp.concatenate([jnp.exp2((ms[k] - mx) * LOG2E)] * NZ, axis=1)
    invt[...] = jnp.concatenate([jnp.exp2((big - mx) * LOG2E)] * NZ, axis=1) / tot
    for k in range(NZ):
        invl[:, k * R:(k + 1) * R] = invt[:, pl.ds(pl.multiple_of(zs(k, -1) * R, R), R)]
    lse = jnp.log2(tot) * LN2 + jnp.concatenate([mx] * NZ, axis=1)
    lrow = jnp.zeros((1, 128), f32)
    for k in range(NZ):
        lrow = lrow + (lse[:, k * R:(k + 1) * R] - stats[k, :, NQ + 128:NQ + 256])
    loss_p[c] = lrow
    send(loss_p.at[c], loss_p.at[c], s_lp, r_lp, dev(z, j, oc))

    def norm(g, c0, c1):
        cols = slice(c0 * QC, c1 * QC)
        out = []
        for i in range(2):
            rows = slice(g * GR + i * R, g * GR + (i + 1) * R)
            p = e_all[rows, cols] * (invl[:, cols] * jnp.concatenate([wslot[2 * g + i]] * (2 * (c1 - c0)), axis=1))
            if g == 0 and i == 0 and c0 == 0:
                col = lax.broadcasted_iota(jnp.int32, p.shape, 1)
                p = jnp.where(lax.broadcasted_iota(jnp.int32, p.shape, 0) == col, p - 1.0, p)
            p = p.astype(bf16)
            g_all[rows, cols] = p
            out.append(p)
        return jnp.concatenate(out, axis=0)

    pend = []
    sv_of = {}
    for k, (a, b) in enumerate(xoff):
        sv_of[a, b] = k

    def flush(keep):
        while len(pend) > keep:
            for k in pend.pop(0):
                a, b = xoff[k]
                wait(pv_in.at[k], r_pv.at[k])
                sv[k] = sv[k] + pv_in[k]
                if b:
                    send(sv.at[k, pl.ds(0, H)], rx.at[a, b - 1], s_p1, r_x.at[a], dev(z, xs(sv_of[0, b], -1), c))
                if a:
                    send(sv.at[k, pl.ds(H, H)], ry.at[b, a - 1], s_p1, r_y.at[b], dev(z, xs(sv_of[a, 0], -1), c))

    def dv_level(l, c0, c1):
        sc(f"dv{l}")
        ks = list(range(l * SL, (l + 1) * SL))
        for g in range(l * NG, (l + 1) * NG):
            if c1 > c0:
                norm(g, c0, c1)
        d = dot(g_all[l * IR:(l + 1) * IR, :], u_all[...])
        for i, k in enumerate(ks):
            pv_out[k] = d[(SL + i) * R:(SL + i + 1) * R, :]
            send(pv_out.at[k], pv_in.at[k], s_pv, r_pv.at[k], dev(z, j, oc))
            sv[k] = d[i * R:(i + 1) * R, :]
        flush(0)
        pend.append(ks)

    def du_levels(l0, l1, fresh):
        sc(f"du{l0}")
        d = None
        for lk in range(LV):
            if lk < fresh:
                gv = jnp.concatenate([norm(g, l0, l1) for g in range(lk * NG, (lk + 1) * NG)], axis=0)
            else:
                gv = g_all[lk * IR:(lk + 1) * IR, l0 * QC:l1 * QC]
            p = dot(vt[:, lk * IR:(lk + 1) * IR], gv)
            d = p if d is None else d + p
        for k in range(2 * l0, 2 * l1):
            su[k] = d[:, (k - 2 * l0) * R:(k - 2 * l0 + 1) * R]
        for k in range(2 * l0, 2 * l1):
            if k and k not in late:
                send_u(k, near.get(k, zoff[k]))

    near, late = {}, {}
    if NZ >= 99:
        for o, via in ((3, 2), (NZ - 3, NZ - 2)):
            near[zoff.index(o)] = (o - via) % NZ
            late[zoff.index(via)] = zoff.index(o)

    def send_u(k, hop):
        to = lax.rem(z + (NZ - hop), NZ)
        sem = r_hop.at[k] if k in near else r_su
        dst = hop_in.at[k] if k in near else ru.at[k]
        send(su.at[k], dst, s_su, sem, dev(to, j, c))

    def send_late(k):
        sc("late")
        wait(hop_in.at[late[k]], r_hop.at[late[k]])
        su[k] = su[k] + hop_in[late[k]]
        send_u(k, zoff[k])

    if LV == 4:
        du_levels(3, 4, 4)
        dv_level(3, 0, 3)
        dv_level(2, 0, 3)
        du_levels(2, 3, 2)
        dv_level(1, 0, 2)
        dv_level(0, 0, 2)
        du_levels(1, 2, 0)
        flush(0)
        du_levels(0, 1, 0)
    else:
        du_levels(1, 2, 2)
        dv_level(1, 0, 1)
        dv_level(0, 0, 1)
        du_levels(0, 1, 0)
        flush(0)

    def leg2(n, own, r1, sem1, t1, r2, sem2, far):
        for o in ring(n)[::-1]:
            wait(r1.at[o], sem1.at[o])
            acc = own(o)
            for i in range(r1.shape[1]):
                acc = acc + r1[o, i]
            t1[o] = acc
            if o:
                send(t1.at[o], r2.at[o - 1], s_p2, sem2, far(o))

    sc("leg2")
    leg2(NY, lambda a: sv[sv_of[a, 0], 0:H], rx, r_x, tx, r2x, r_2x, lambda a: dev(z, xs(sv_of[a, 0], -1), c))
    leg2(NX, lambda b: sv[sv_of[0, b], H:R], ry, r_y, ty, r2y, r_2y, lambda b: dev(z, xs(sv_of[0, b], -1), c))

    sc("loss")
    wait(loss_p.at[oc], r_lp)
    loss_x[j] = loss_p[0] + loss_p[1]
    for k in range(1, NXY):
        send(loss_x.at[j], loss_x.at[j], s_lx, r_lx, dev(z, xs(k, 1), c))

    def backward(du, xr, wo, unit, inv, hid, act, t):
        u, r = unit[...], inv[...]
        de = (r * (du - u * jnp.sum(u * du, axis=-1, keepdims=True))).astype(bf16)
        go = dot(hid[...], de, TN)
        dh = dot(de, wo[...], NT)
        da = jnp.where(act[...] > 0, dh, 0.0).astype(bf16)
        gi = dot(xr[...], da, TN)
        gl[t, 0:256, :] = gi[:, 0:128]
        gl[t, 256:512, :] = gi[:, 128:256]
        gl[t, 512:768, :] = go
        send(gl.at[t, pl.ds(pl.multiple_of(oc * 384, 8), 384), :], gpair.at[t], s_gp.at[t], r_gp.at[t], dev(z, j, oc))

    def pair_sum(t):
        sc(f"gp_wait{t}")
        wait(gpair.at[t], r_gp.at[t])
        gx_s[t] = (gl[t, pl.ds(pl.multiple_of(c * 384, 8), 384), :] + gpair[t]).reshape(NXY, CH, 128)
        for k in range(1, NXY):
            to = xs(k, 1)
            send(gx_s.at[t, to], gx_r.at[t, j], s_gx.at[t], r_gx.at[t], dev(z, to, c))
        gx_r[t, j] = gx_s[t, j]

    def plane_sum(t):
        sc(f"gx_wait{t}")
        wait(gx_r.at[t, pl.ds(0, NXY - 1)], r_gx.at[t])
        acc = gx_r[t, 0]
        for k in range(1, NXY):
            acc = acc + gx_r[t, k]
        gz_r[t, z] = acc
        for k in range(1, NZ):
            send(gz_r.at[t, z], gz_r.at[t, z], s_gz.at[t], r_gz.at[t], dev(zs(k, 1), j, c))

    def ring_sum(t):
        sc(f"gz_wait{t}")
        wait(gz_r.at[t, pl.ds(0, NZ - 1)], r_gz.at[t])
        acc = gz_r[t, 0]
        for k in range(1, NZ):
            acc = acc + gz_r[t, k]
        fin[t, c, j] = acc
        for k in range(1, NXY):
            send(fin.at[t, c, j], fin.at[t, c, j], s_ag.at[t], r_ag.at[t, k], dev(z, xs(k, 1), c))
        send(fin.at[t, c, j], fin.at[t, c, j], s_rl.at[t], r_rl.at[t, 0], dev(z, j, oc))

    def relay(t):
        sc(f"ag_wait{t}")
        for k in range(1, NXY):
            ref = fin.at[t, c, xs(k, -1)]
            wait(ref, r_ag.at[t, k])
            send(ref, ref, s_rl.at[t], r_rl.at[t, k], dev(z, j, oc))

    scale = 1.0 / (TEMP * B)
    sc("rv_wait")
    wait(r2x, r_2x)
    wait(r2y, r_2y)
    sc("bwd_v")
    top, bot = tx[0], ty[0]
    for i in range(NY - 1):
        top = top + r2x[i]
    for i in range(NX - 1):
        bot = bot + r2y[i]
    backward(jnp.concatenate([top, bot], axis=0) * scale, vf, wvo, vp, vi, vh, va, 1)
    pair_sum(1)
    sc("ru_wait")
    wait(ru.at[pl.ds(0, NZ - 1 - len(near))], r_su)
    sc("bwd_q")
    acc = su[0]
    for k in range(1, NZ):
        if k not in near:
            acc = acc + ru[k]
    backward(jnp.transpose(acc) * scale, qf, wqo, up, ui, uh, ua, 0)
    pair_sum(0)
    plane_sum(1)
    plane_sum(0)
    ring_sum(1)
    ring_sum(0)
    relay(1)
    relay(0)
    sc("loss2")
    wait(loss_x.at[pl.ds(0, NXY - 1)], r_lx)
    ls = loss_x[0]
    for k in range(1, NXY):
        ls = ls + loss_x[k]
    loss_o[...] = jnp.broadcast_to(jnp.sum(ls, axis=-1, keepdims=True) * (1.0 / B), (1, 128))
    sc("rl_wait")
    for t in range(2):
        for k in range(NXY):
            wait(fin.at[t, oc, xs(k, -1)], r_rl.at[t, k])

    sc("sendwait")
    wait(lq_all.at[pl.ds(0, 2 * NXY - 1)], s_lq)
    wait(u_all.at[pl.ds(0, (NZ - 1) * R), :], s_u)
    wait(v_all.at[pl.ds(0, (NXY - 1) * R), :], s_v)
    wait(v_all.at[pl.ds(0, NXY * R), :], s_vr)
    wait(stats.at[pl.ds(0, NZ - 1)], s_st)
    wait(loss_p.at[0], s_lp)
    wait(pv_out, s_pv)
    wait(sv.at[pl.ds(0, (NY * (NX - 1) + NX * (NY - 1)) // 2)], s_p1)
    wait(t_cnt, s_p2)
    wait(su.at[pl.ds(0, NZ - 1)], s_su)
    wait(loss_x.at[pl.ds(0, NXY - 1)], s_lx)
    for t in range(2):
        wait(gpair.at[t], s_gp.at[t])
        wait(gx_s.at[t, pl.ds(0, NXY - 1)], s_gx.at[t])
        wait(gz_r.at[t, pl.ds(0, NZ - 1)], s_gz.at[t])
        wait(gx_s.at[t, pl.ds(0, NXY - 1)], s_ag.at[t])
        wait(gx_s.at[t], s_rl.at[t])
    sc(None)


def emit(fin, loss, gqi, gqo, gvi, gvo, loss_o):
    for t, (gi, go) in enumerate(((gqi, gqo), (gvi, gvo))):
        gi[:, 0:128] = fin[t, 0:256]
        gi[:, 128:256] = fin[t, 256:512]
        go[...] = fin[t, 512:768]
    loss_o[...] = loss[...]


def build(NZ, NY, NX):
    def step(query_feat, item_feat, log_q, w_query_in, w_query_out, w_item_in, w_item_out):
        NXY = NY * NX
        NQ, NI, CH = NZ * R, 2 * NXY * R, 384 // NXY
        V, S = pltpu.VMEM, pltpu.SemaphoreType.DMA
        vm, hbm = pl.BlockSpec(memory_space=pltpu.VMEM), pl.BlockSpec(memory_space=pl.ANY)
        sd = jax.ShapeDtypeStruct
        tower = [V((R, 128), f32), V((R, 128), f32), V((R, 256), bf16), V((R, 256), f32)]
        fin, loss = pl.pallas_call(
            functools.partial(kernel, NZ, NY, NX),
            name="two_tower",
            out_shape=[sd((2, 2, NXY, CH, 128), f32), sd((1, 128), f32)],
            in_specs=[hbm] * 7,
            out_specs=[vm] * 2,
            scratch_shapes=[
                V((R, 256), bf16), V((R, 256), bf16), V((1, 128), f32),
                V((256, 256), bf16), V((256, 128), bf16), V((256, 256), bf16), V((256, 128), bf16), S((7,)),
                V((NQ, 128), bf16), V((NI, 128), bf16), V((128, NI), bf16), V((2 * NXY, 1, 128), f32), V((2 * NXY, 1, 128), f32), V((2 * NXY, 1, 128), f32), V((65, 1, 128), f32),
                V((NI, 128), f32), V((2, GR, 2 * R), f32), V((NI, NQ), f32), V((NI, NQ), bf16), V((2 * NXY, 8, NQ), f32),
                V((NZ, 1, NQ + 256), f32), V((1, NQ), f32), V((1, NQ), f32),
                *tower, *tower,
                V((NZ, 128, 128), f32), V((NZ, 128, 128), f32), V((NZ, 128, 128), f32),
                V((NXY, 128, 128), f32), V((NXY, 128, 128), f32), V((NXY, 128, 128), f32),
                V((NY, NX - 1, H, 128), f32), V((NX, NY - 1, H, 128), f32), V((NY, H, 128), f32), V((NX, H, 128), f32),
                V((NY - 1, H, 128), f32), V((NX - 1, H, 128), f32), V((NY + NX - 2, H, 128), f32),
                V((2, 768, 128), f32), V((2, 384, 128), f32), V((2, NXY, CH, 128), f32), V((2, NXY, CH, 128), f32),
                V((2, NZ, CH, 128), f32), V((2, 1, 128), f32), V((NXY, 1, 128), f32),
                S, S((NZ,)), S, S((2 * NXY,)), S, S, S, S, S((NXY,)), S, S, S((NY,)), S((NX,)), S, S, S, S, S((NZ,)),
                S((2,)), S((2,)), S((2,)), S((2,)), S((2,)), S((2,)), S((2,)), S((2, NXY)), S((2,)), S((2, NXY)),
                S, S, S, S, S,
            ],
            compiler_params=pltpu.CompilerParams(collective_id=0, has_side_effects=True, vmem_limit_bytes=60 * 2**20),
        )(query_feat, item_feat, log_q.reshape(1, 128), w_query_in, w_query_out, w_item_in, w_item_out)
        gqi, gqo, gvi, gvo, out = pl.pallas_call(
            emit,
            name="emit",
            out_shape=[sd((256, 256), f32), sd((256, 128), f32), sd((256, 256), f32), sd((256, 128), f32), sd((1, 128), f32)],
            in_specs=[vm] * 2,
            out_specs=[vm] * 5,
        )(fin.reshape(2, 768, 128), loss)
        return out[0, 0:1], gqi, gqo, gvi, gvo
    return step


def solution(mesh):
    n = mesh.shape["dp"]
    dims = (8, 4, 4) if n == 256 else (4, 2, 2)
    return jax.shard_map(build(*dims), mesh=mesh,
                         in_specs=(P("dp", None), P("dp", None), P("dp"), P(), P(), P(), P()),
                         out_specs=(P(), P(), P(), P(), P()), check_vma=False)
```

```python
import functools

import jax
import jax.numpy as jnp
from jax import lax
from jax.experimental import pallas as pl
from jax.experimental.pallas import tpu as pltpu
from jax.sharding import PartitionSpec as P

f32, bf16 = jnp.float32, jnp.bfloat16
MESH = pl.DeviceIdType.MESH
TEMP = 0.05
EPS = 1e-6
LOG2E = 1.4426950408889634
LN2 = 0.6931471805599453
NT = (((1,), (1,)), ((), ()))
TN = (((0,), (0,)), ((), ()))
NN = (((1,), (0,)), ((), ()))
R = 128
GR = 256
H = R // 2


class Scope:
    def __init__(self):
        self.cur = None

    def __call__(self, name):
        if self.cur is not None:
            self.cur.__exit__(None, None, None)
        self.cur = None
        if name:
            self.cur = jax.named_scope(name)
            self.cur.__enter__()


def dot(a, b, dims=NN):
    return lax.dot_general(a, b, dims, preferred_element_type=f32)


def arrange(near, level):
    rest = near[level:]
    return near[:level] + rest[level:][::-1] + rest[:level]


def ring(n):
    return sorted(range(n), key=lambda k: (min(k, n - k), k))


def torus(ny, nx):
    def dist(o):
        return min(o[0], ny - o[0]) + min(o[1], nx - o[1])
    return sorted(((a, b) for a in range(ny) for b in range(nx)), key=lambda o: (dist(o), o[0] * o[1] != 0, o))


def kernel(NZ, NY, NX, qf_h, vf_h, lq_h, wqi_h, wqo_h, wvi_h, wvo_h, fin, loss_o,
           qf, vf, lq, wqi, wqo, wvi, wvo, s_in,
           u_all, v_all, vt, lq_all, mslot, wslot, cnt, bcol, sbuf, e_all, g_all, csum, stats, invl, invt,
           up, ui, uh, ua, vp, vi, vh, va,
           su, ru, pv_out, pv_in, sv, rx, ry, tx, ty, r2x, r2y, t_cnt, gl, gpair, gx_s, gx_r, gz_r, loss_p, loss_x,
           s_u, r_u, s_v, r_v, s_lq, s_st, r_st, s_pv, r_pv, s_p1, s_p2, r_x, r_y, r_2x, r_2y, s_su, r_su,
           s_gp, r_gp, s_gx, r_gx, s_gz, r_gz, s_ag, r_ag, s_rl, r_rl, s_lp, r_lp, s_lx, r_lx, s_vr):
    sc = Scope()
    NXY = NY * NX
    NQ = NZ * R
    NI = 2 * NXY * R
    B = NZ * NI
    CH = 384 // NXY
    LV = NZ // 2
    SL = NXY // LV
    QC = 2 * R
    IR = 2 * SL * R
    NG = IR // GR
    zoff, xoff = arrange(ring(NZ), 2), arrange(torus(NY, NX), SL)
    zfar = [zoff.index(o) for o in ring(NZ)[:0:-1]]
    xfar = [xoff.index(o) for o in torus(NY, NX)[:0:-1]]
    me = lax.axis_index("dp")
    c = lax.rem(me, 2)
    j = lax.rem(lax.div(me, 2), NXY)
    y, x = lax.div(j, NX), lax.rem(j, NX)
    z = lax.div(me, 2 * NXY)
    oc = 1 - c

    def dev(zz, jj, cc):
        return ((zz * NXY + jj) * 2 + cc,)

    def zs(k, sign):
        o = zoff[k]
        return lax.rem(z + (o if sign > 0 else NZ - o), NZ)

    def xs(k, sign):
        a, b = xoff[k]
        yy = lax.rem(y + (a if sign > 0 else NY - a), NY)
        xx = lax.rem(x + (b if sign > 0 else NX - b), NX)
        return yy * NX + xx

    def slot(k, core):
        return (k // SL) * 2 * SL + core * SL + k % SL

    def send(src, dst, ss, rs, to):
        pltpu.make_async_remote_copy(src_ref=src, dst_ref=dst, send_sem=ss, recv_sem=rs,
                                     device_id=to, device_id_type=MESH).start()

    def wait(ref, sem):
        pltpu.make_async_copy(ref, ref, sem).wait()

    def vrows(s):
        return v_all.at[pl.ds(s * R, R), :]

    sc("barsig")
    bar = pltpu.get_barrier_semaphore()
    peers = [dev(zs(k, 1), j, c) for k in range(1, NZ)]
    peers += [dev(z, xs(k, 1), c) for k in range(1, NXY)]
    peers += [dev(z, j, oc)]
    for p in peers:
        pl.semaphore_signal(bar, inc=1, device_id=p, device_id_type=MESH)
    loads = [pltpu.make_async_copy(a, b, s_in.at[i]) for i, (a, b) in enumerate(
        ((qf_h, qf), (wqi_h, wqi), (wqo_h, wqo), (vf_h, vf), (wvi_h, wvi), (wvo_h, wvo), (lq_h, lq)))]
    for cp in loads:
        cp.start()
    for cp in loads:
        cp.wait()

    sc("tower")

    def tower(xr, wi, wo, unit, inv, hid, act):
        a = dot(xr[...], wi[...])
        h = jnp.maximum(a, 0.0).astype(bf16)
        e = dot(h, wo[...])
        r = lax.rsqrt(jnp.sum(e * e, axis=-1, keepdims=True) + EPS)
        u = e * r
        unit[...] = u
        inv[...] = jnp.broadcast_to(r, (R, 128))
        hid[...] = h
        act[...] = a
        return u.astype(bf16)

    u_bf = tower(qf, wqi, wqo, up, ui, uh, ua)
    v_bf = tower(vf, wvi, wvo, vp, vi, vh, va)
    u_all[0:R, :] = u_bf
    v_all[0:R, :] = v_bf
    lq_all[0] = lq[...]
    pos = jnp.sum(u_bf.astype(f32) * v_bf.astype(f32), axis=0, keepdims=True) * (1.0 / TEMP) - lq[...]
    stats[z, :, pl.ds(NQ + 128, 128)] = pos

    sc("barwait")
    pl.semaphore_wait(bar, len(peers))
    sc("sends")
    mine_u = u_all.at[pl.ds(0, R), :]

    def send_item(s, s2, ss, to):
        send(lq_all.at[s], lq_all.at[s2], s_lq, r_v.at[s2], to)
        send(vrows(s), vrows(s2), ss, r_v.at[s2], to)

    send_item(0, slot(0, 1), s_vr, dev(z, j, oc))
    for k in range(1, NXY):
        if k < NZ:
            send(mine_u, u_all.at[pl.ds(k * R, R), :], s_u, r_u.at[k], dev(zs(k, 1), j, c))
        send_item(0, slot(k, 0), s_v, dev(z, xs(k, 1), c))

    def grp(g):
        return slice(g * GR, (g + 1) * GR)

    def dyn(g):
        return pl.ds(pl.multiple_of(g * GR, GR), GR)

    def qcols(l):
        return slice(l * QC, (l + 1) * QC)

    def loop(lo, n, f):
        lax.fori_loop(0, n, lambda i, u: (f(lo + i), u)[1], 0)

    def bias(s0):
        q = lq_all[s0:s0 + SL].reshape(SL, 128)
        big = jnp.max(-q, axis=1, keepdims=True)
        b = (big + q) * LOG2E
        bt = jnp.transpose(jnp.concatenate([b] * (8 // SL), axis=0))
        for i in range(SL):
            mslot[s0 + i] = jnp.broadcast_to(big[i:i + 1, :], (1, 128))
            bcol[(s0 + i) * R:(s0 + i + 1) * R, :] = jnp.broadcast_to(bt[:, i:i + 1], (R, 128))

    def expo(n, g, l):
        rows, cols = grp(g), qcols(l)
        bb = bcol[rows, :]
        e = jnp.exp2(sbuf[n % 2] * (LOG2E / TEMP) - jnp.concatenate([bb, bb], axis=1))
        e_all[rows, cols] = e
        csum[2 * g:2 * g + 2, :, cols] = jnp.sum(e.reshape(2, R // 8, 8, QC), axis=1)

    def groups(l, core):
        return [l * NG + core * (NG // 2) + t for t in range(NG // 2)]

    done = []
    for l in range(LV + 1):
        sc(f"wait{l}")
        fresh = []
        if l < LV:
            for k in range(l * SL, (l + 1) * SL):
                if k:
                    wait(cnt, r_v.at[slot(k, 0)])
                    send_item(slot(k, 0), slot(k, 1), s_vr, dev(z, j, oc))
            for k in (2 * l, 2 * l + 1):
                if k:
                    wait(u_all.at[pl.ds(k * R, R), :], r_u.at[k])
            fresh += groups(l, 0)
        if l:
            for k in range((l - 1) * SL, l * SL):
                wait(cnt, r_v.at[slot(k, 1)])
            fresh += groups(l - 1, 1)
        sc(f"pass1_{l}")
        if l < LV:
            bias(slot(l * SL, 0))
        if l:
            bias(slot((l - 1) * SL, 1))
        tasks = [(g, l2) for g in fresh for l2 in range(min(l, LV - 1) + 1)]
        if l < LV:
            old = [g for g in range(LV * NG) if g in done]
            tasks = [(g, l) for g in old] + tasks
        done += fresh
        for g in fresh:
            vt[:, grp(g)] = jnp.transpose(v_all[grp(g), :].astype(f32)).astype(bf16)
        for n, (g, l2) in enumerate(tasks):
            sbuf[n % 2] = dot(v_all[grp(g), :], u_all[qcols(l2), :], NT)
            if n:
                expo(n - 1, *tasks[n - 1])
        expo(len(tasks) - 1, *tasks[-1])

    sc("stats_send")
    big = jnp.max(mslot[...], axis=0)
    stats[z, :, pl.ds(NQ, 128)] = big
    wslot[...] = jnp.exp2((mslot[...] - big) * LOG2E)
    for k in range(NZ):
        acc = csum[0, :, k * R:(k + 1) * R] * wslot[0]
        for s in range(1, 2 * NXY):
            acc = acc + csum[s, :, k * R:(k + 1) * R] * wslot[s]
        stats[z, :, pl.ds(pl.multiple_of(zs(k, -1) * R, R), R)] = jnp.sum(acc, axis=0, keepdims=True)
    for k in zfar:
        send(stats.at[z], stats.at[z], s_st, r_st, dev(zs(k, 1), j, c))
    sc("stats_wait")
    wait(stats.at[pl.ds(0, NZ - 1)], r_st)
    sc("stats_comp")
    ms = [stats[k, :, NQ:NQ + 128] for k in range(NZ)]
    mx = functools.reduce(jnp.maximum, ms)
    tot = jnp.zeros((1, NQ), f32)
    for k in range(NZ):
        tot = tot + stats[k, :, 0:NQ] * jnp.concatenate([jnp.exp2((ms[k] - mx) * LOG2E)] * NZ, axis=1)
    invt[...] = jnp.concatenate([jnp.exp2((big - mx) * LOG2E)] * NZ, axis=1) / tot
    for k in range(NZ):
        invl[:, k * R:(k + 1) * R] = invt[:, pl.ds(pl.multiple_of(zs(k, -1) * R, R), R)]
    lse = jnp.log2(tot) * LN2 + jnp.concatenate([mx] * NZ, axis=1)
    lrow = jnp.zeros((1, 128), f32)
    for k in range(NZ):
        lrow = lrow + (lse[:, k * R:(k + 1) * R] - stats[k, :, NQ + 128:NQ + 256])
    loss_p[c] = lrow
    send(loss_p.at[c], loss_p.at[c], s_lp, r_lp, dev(z, j, oc))

    def norm(g, c0, c1):
        cols = slice(c0 * QC, c1 * QC)
        out = []
        for i in range(2):
            rows = slice(g * GR + i * R, g * GR + (i + 1) * R)
            p = e_all[rows, cols] * (invl[:, cols] * jnp.concatenate([wslot[2 * g + i]] * (2 * (c1 - c0)), axis=1))
            if g == 0 and i == 0 and c0 == 0:
                col = lax.broadcasted_iota(jnp.int32, p.shape, 1)
                p = jnp.where(lax.broadcasted_iota(jnp.int32, p.shape, 0) == col, p - 1.0, p)
            p = p.astype(bf16)
            g_all[rows, cols] = p
            out.append(p)
        return jnp.concatenate(out, axis=0)

    pend = []
    sv_of = {}
    for k, (a, b) in enumerate(xoff):
        sv_of[a, b] = k

    def flush(keep):
        while len(pend) > keep:
            for k in pend.pop(0):
                a, b = xoff[k]
                wait(pv_in.at[k], r_pv.at[k])
                sv[k] = sv[k] + pv_in[k]
                if b:
                    send(sv.at[k, pl.ds(0, H)], rx.at[a, b - 1], s_p1, r_x.at[a], dev(z, xs(sv_of[0, b], -1), c))
                if a:
                    send(sv.at[k, pl.ds(H, H)], ry.at[b, a - 1], s_p1, r_y.at[b], dev(z, xs(sv_of[a, 0], -1), c))

    normed = set()

    def ready(g, l):
        if (g, l) not in normed:
            normed.add((g, l))
            norm(g, l, l + 1)

    def dv_half(ls, core):
        sc(f"dv{ls[0]}{core}")
        ds = []
        for l in ls:
            gs = groups(l, core)
            for g in gs:
                for l2 in range(LV):
                    ready(g, l2)
            ds.append(dot(g_all[gs[0] * GR:(gs[-1] + 1) * GR, :], u_all[...]))
        keep = pv_out if core else sv
        for l, d in zip(ls, ds):
            for i in range(SL):
                keep[l * SL + i] = d[i * R:(i + 1) * R, :]
        for l in ls:
            ks = list(range(l * SL, (l + 1) * SL))
            if core:
                for k in ks:
                    send(pv_out.at[k], pv_in.at[k], s_pv, r_pv.at[k], dev(z, j, oc))
            else:
                pend.append(ks)
        if not core:
            sc(f"flush{ls[0]}")
            flush(0)

    def du_levels(ls):
        sc(f"du{ls[0]}")
        for l in ls:
            parts = []
            for lk in range(LV):
                for g in range(lk * NG, (lk + 1) * NG):
                    ready(g, l)
                rows = slice(lk * IR, (lk + 1) * IR)
                parts.append(dot(vt[:, rows], g_all[rows, qcols(l)]))
            d = functools.reduce(jnp.add, parts)
            for i in range(2):
                su[2 * l + i] = d[:, i * R:(i + 1) * R]
        for l in ls:
            for k in (2 * l, 2 * l + 1):
                if k:
                    send(su.at[k], ru.at[k], s_su, r_su, dev(zs(k, -1), j, c))

    if LV == 4:
        dv_half([1, 2], 1)
        du_levels([1, 2])
        dv_half([1, 2], 0)
        dv_half([3, 0], 1)
        du_levels([3, 0])
        dv_half([3, 0], 0)
    else:
        dv_half([0, 1], 1)
        du_levels([1, 0])
        dv_half([0, 1], 0)

    def leg2(o, own, r1, sem1, t1, r2, sem2, far):
        wait(r1.at[o], sem1.at[o])
        acc = own
        for i in range(r1.shape[1]):
            acc = acc + r1[o, i]
        t1[o] = acc
        if o:
            send(t1.at[o], r2.at[o - 1], s_p2, sem2, far)

    sc("leg2")
    for o in ring(max(NY, NX))[::-1]:
        if o < NY:
            leg2(o, sv[sv_of[o, 0], 0:H], rx, r_x, tx, r2x, r_2x, dev(z, xs(sv_of[o, 0], -1), c))
        if o < NX:
            leg2(o, sv[sv_of[0, o], H:R], ry, r_y, ty, r2y, r_2y, dev(z, xs(sv_of[0, o], -1), c))

    sc("loss")
    wait(loss_p.at[oc], r_lp)
    loss_x[j] = loss_p[0] + loss_p[1]
    for k in range(1, NXY):
        send(loss_x.at[j], loss_x.at[j], s_lx, r_lx, dev(z, xs(k, 1), c))

    def backward(du, xr, wo, unit, inv, hid, act, t):
        u, r = unit[...], inv[...]
        de = (r * (du - u * jnp.sum(u * du, axis=-1, keepdims=True))).astype(bf16)
        go = dot(hid[...], de, TN)
        dh = dot(de, wo[...], NT)
        da = jnp.where(act[...] > 0, dh, 0.0).astype(bf16)
        gi = dot(xr[...], da, TN)
        gl[t, 0:256, :] = gi[:, 0:128]
        gl[t, 256:512, :] = gi[:, 128:256]
        gl[t, 512:768, :] = go
        send(gl.at[t, pl.ds(pl.multiple_of(oc * 384, 8), 384), :], gpair.at[t], s_gp.at[t], r_gp.at[t], dev(z, j, oc))

    def pair_sum(t):
        sc(f"gp_wait{t}")
        wait(gpair.at[t], r_gp.at[t])
        gx_s[t] = (gl[t, pl.ds(pl.multiple_of(c * 384, 8), 384), :] + gpair[t]).reshape(NXY, CH, 128)
        for k in xfar:
            to = xs(k, 1)
            send(gx_s.at[t, to], gx_r.at[t, j], s_gx.at[t], r_gx.at[t], dev(z, to, c))
        gx_r[t, j] = gx_s[t, j]

    def plane_sum(t):
        sc(f"gx_wait{t}")
        wait(gx_r.at[t, pl.ds(0, NXY - 1)], r_gx.at[t])
        acc = gx_r[t, 0]
        for k in range(1, NXY):
            acc = acc + gx_r[t, k]
        gz_r[t, z] = acc
        for k in zfar:
            send(gz_r.at[t, z], gz_r.at[t, z], s_gz.at[t], r_gz.at[t], dev(zs(k, 1), j, c))

    def ring_sum(t):
        sc(f"gz_wait{t}")
        wait(gz_r.at[t, pl.ds(0, NZ - 1)], r_gz.at[t])
        acc = gz_r[t, 0]
        for k in range(1, NZ):
            acc = acc + gz_r[t, k]
        fin[t, c, j] = acc
        for k in xfar:
            send(fin.at[t, c, j], fin.at[t, c, j], s_ag.at[t], r_ag.at[t, k], dev(z, xs(k, 1), c))
        send(fin.at[t, c, j], fin.at[t, c, j], s_rl.at[t], r_rl.at[t, 0], dev(z, j, oc))

    def relay(t):
        sc(f"ag_wait{t}")
        for k in xfar:
            ref = fin.at[t, c, xs(k, -1)]
            wait(ref, r_ag.at[t, k])
            send(ref, ref, s_rl.at[t], r_rl.at[t, k], dev(z, j, oc))

    scale = 1.0 / (TEMP * B)
    sc("rv_wait")
    wait(r2x, r_2x)
    wait(r2y, r_2y)
    sc("bwd_v")
    top, bot = tx[0], ty[0]
    for i in range(NY - 1):
        top = top + r2x[i]
    for i in range(NX - 1):
        bot = bot + r2y[i]
    backward(jnp.concatenate([top, bot], axis=0) * scale, vf, wvo, vp, vi, vh, va, 1)
    pair_sum(1)
    sc("ru_wait")
    wait(ru.at[pl.ds(0, NZ - 1)], r_su)
    sc("bwd_q")
    acc = su[0]
    for k in range(1, NZ):
        acc = acc + ru[k]
    backward(jnp.transpose(acc) * scale, qf, wqo, up, ui, uh, ua, 0)
    pair_sum(0)
    plane_sum(1)
    plane_sum(0)
    ring_sum(1)
    ring_sum(0)
    relay(1)
    relay(0)
    sc("loss2")
    wait(loss_x.at[pl.ds(0, NXY - 1)], r_lx)
    ls = loss_x[0]
    for k in range(1, NXY):
        ls = ls + loss_x[k]
    loss_o[...] = jnp.broadcast_to(jnp.sum(ls, axis=-1, keepdims=True) * (1.0 / B), (1, 128))
    sc("rl_wait")
    for t in range(2):
        for k in range(NXY):
            wait(fin.at[t, oc, xs(k, -1)], r_rl.at[t, k])

    sc("sendwait")
    wait(lq_all.at[pl.ds(0, 2 * NXY - 1)], s_lq)
    wait(u_all.at[pl.ds(0, (NZ - 1) * R), :], s_u)
    wait(v_all.at[pl.ds(0, (NXY - 1) * R), :], s_v)
    wait(v_all.at[pl.ds(0, NXY * R), :], s_vr)
    wait(stats.at[pl.ds(0, NZ - 1)], s_st)
    wait(loss_p.at[0], s_lp)
    wait(pv_out, s_pv)
    wait(sv.at[pl.ds(0, (NY * (NX - 1) + NX * (NY - 1)) // 2)], s_p1)
    wait(t_cnt, s_p2)
    wait(su.at[pl.ds(0, NZ - 1)], s_su)
    wait(loss_x.at[pl.ds(0, NXY - 1)], s_lx)
    for t in range(2):
        wait(gpair.at[t], s_gp.at[t])
        wait(gx_s.at[t, pl.ds(0, NXY - 1)], s_gx.at[t])
        wait(gz_r.at[t, pl.ds(0, NZ - 1)], s_gz.at[t])
        wait(gx_s.at[t, pl.ds(0, NXY - 1)], s_ag.at[t])
        wait(gx_s.at[t], s_rl.at[t])
    sc(None)


def emit(fin, loss, gqi, gqo, gvi, gvo, loss_o):
    for t, (gi, go) in enumerate(((gqi, gqo), (gvi, gvo))):
        gi[:, 0:128] = fin[t, 0:256]
        gi[:, 128:256] = fin[t, 256:512]
        go[...] = fin[t, 512:768]
    loss_o[...] = loss[...]


def build(NZ, NY, NX):
    def step(query_feat, item_feat, log_q, w_query_in, w_query_out, w_item_in, w_item_out):
        NXY = NY * NX
        NQ, NI, CH = NZ * R, 2 * NXY * R, 384 // NXY
        V, S = pltpu.VMEM, pltpu.SemaphoreType.DMA
        vm, hbm = pl.BlockSpec(memory_space=pltpu.VMEM), pl.BlockSpec(memory_space=pl.ANY)
        sd = jax.ShapeDtypeStruct
        tower = [V((R, 128), f32), V((R, 128), f32), V((R, 256), bf16), V((R, 256), f32)]
        fin, loss = pl.pallas_call(
            functools.partial(kernel, NZ, NY, NX),
            name="two_tower",
            out_shape=[sd((2, 2, NXY, CH, 128), f32), sd((1, 128), f32)],
            in_specs=[hbm] * 7,
            out_specs=[vm] * 2,
            scratch_shapes=[
                V((R, 256), bf16), V((R, 256), bf16), V((1, 128), f32),
                V((256, 256), bf16), V((256, 128), bf16), V((256, 256), bf16), V((256, 128), bf16), S((7,)),
                V((NQ, 128), bf16), V((NI, 128), bf16), V((128, NI), bf16), V((2 * NXY, 1, 128), f32), V((2 * NXY, 1, 128), f32), V((2 * NXY, 1, 128), f32), V((65, 1, 128), f32),
                V((NI, 128), f32), V((2, GR, 2 * R), f32), V((NI, NQ), f32), V((NI, NQ), bf16), V((2 * NXY, 8, NQ), f32),
                V((NZ, 1, NQ + 256), f32), V((1, NQ), f32), V((1, NQ), f32),
                *tower, *tower,
                V((NZ, 128, 128), f32), V((NZ, 128, 128), f32),
                V((NXY, 128, 128), f32), V((NXY, 128, 128), f32), V((NXY, 128, 128), f32),
                V((NY, NX - 1, H, 128), f32), V((NX, NY - 1, H, 128), f32), V((NY, H, 128), f32), V((NX, H, 128), f32),
                V((NY - 1, H, 128), f32), V((NX - 1, H, 128), f32), V((NY + NX - 2, H, 128), f32),
                V((2, 768, 128), f32), V((2, 384, 128), f32), V((2, NXY, CH, 128), f32), V((2, NXY, CH, 128), f32),
                V((2, NZ, CH, 128), f32), V((2, 1, 128), f32), V((NXY, 1, 128), f32),
                S, S((NZ,)), S, S((2 * NXY,)), S, S, S, S, S((NXY,)), S, S, S((NY,)), S((NX,)), S, S, S, S,
                S((2,)), S((2,)), S((2,)), S((2,)), S((2,)), S((2,)), S((2,)), S((2, NXY)), S((2,)), S((2, NXY)),
                S, S, S, S, S,
            ],
            compiler_params=pltpu.CompilerParams(collective_id=0, has_side_effects=True, vmem_limit_bytes=60 * 2**20),
        )(query_feat, item_feat, log_q.reshape(1, 128), w_query_in, w_query_out, w_item_in, w_item_out)
        gqi, gqo, gvi, gvo, out = pl.pallas_call(
            emit,
            name="emit",
            out_shape=[sd((256, 256), f32), sd((256, 128), f32), sd((256, 256), f32), sd((256, 128), f32), sd((1, 128), f32)],
            in_specs=[vm] * 2,
            out_specs=[vm] * 5,
        )(fin.reshape(2, 768, 128), loss)
        return out[0, 0:1], gqi, gqo, gvi, gvo
    return step


def solution(mesh):
    n = mesh.shape["dp"]
    dims = (8, 4, 4) if n == 256 else (4, 2, 2)
    return jax.shard_map(build(*dims), mesh=mesh,
                         in_specs=(P("dp", None), P("dp", None), P("dp"), P(), P(), P(), P()),
                         out_specs=(P(), P(), P(), P(), P()), check_vma=False)
```

```python
import functools

import jax
import jax.numpy as jnp
from jax import lax
from jax.experimental import pallas as pl
from jax.experimental.pallas import tpu as pltpu
from jax.sharding import PartitionSpec as P

f32, bf16 = jnp.float32, jnp.bfloat16
MESH = pl.DeviceIdType.MESH
TEMP = 0.05
EPS = 1e-6
LOG2E = 1.4426950408889634
LN2 = 0.6931471805599453
NT = (((1,), (1,)), ((), ()))
TN = (((0,), (0,)), ((), ()))
NN = (((1,), (0,)), ((), ()))
R = 128
GR = 256
H = R // 2


class Scope:
    def __init__(self):
        self.cur = None

    def __call__(self, name):
        if self.cur is not None:
            self.cur.__exit__(None, None, None)
        self.cur = None
        if name:
            self.cur = jax.named_scope(name)
            self.cur.__enter__()


def dot(a, b, dims=NN):
    return lax.dot_general(a, b, dims, preferred_element_type=f32)


def arrange(near, level):
    rest = near[level:]
    return near[:level] + rest[level:][::-1] + rest[:level]


def ring(n):
    return sorted(range(n), key=lambda k: (min(k, n - k), k))


def torus(ny, nx):
    def dist(o):
        return min(o[0], ny - o[0]) + min(o[1], nx - o[1])
    return sorted(((a, b) for a in range(ny) for b in range(nx)), key=lambda o: (dist(o), o[0] * o[1] != 0, o))


def kernel(NZ, NY, NX, qf_h, vf_h, lq_h, wqi_h, wqo_h, wvi_h, wvo_h, fin, loss_o,
           qf, vf, lq, wqi, wqo, wvi, wvo, s_in,
           u_all, v_all, vt, lq_all, mslot, wslot, cnt, bcol, sbuf, e_all, g_all, csum, stats, invl, invt,
           up, ui, uh, ua, vp, vi, vh, va,
           su, ru, hop_in, pv_out, pv_in, sv, rx, ry, tx, ty, r2x, r2y, t_cnt, gl, gpair, gx_s, gx_r, gz_r, loss_p, loss_x,
           s_u, r_u, s_v, r_v, s_lq, s_st, r_st, s_pv, r_pv, s_p1, s_p2, r_x, r_y, r_2x, r_2y, s_su, r_su, r_hop,
           s_gp, r_gp, s_gx, r_gx, s_gz, r_gz, s_ag, r_ag, s_rl, r_rl, s_lp, r_lp, s_lx, r_lx, s_vr):
    sc = Scope()
    NXY = NY * NX
    NQ = NZ * R
    NI = 2 * NXY * R
    B = NZ * NI
    CH = 384 // NXY
    LV = NZ // 2
    SL = NXY // LV
    QC = 2 * R
    IR = 2 * SL * R
    NG = IR // GR
    zoff, xoff = arrange(ring(NZ), 2), arrange(torus(NY, NX), SL)
    zfar = [zoff.index(o) for o in ring(NZ)[:0:-1]]
    xfar = [xoff.index(o) for o in torus(NY, NX)[:0:-1]]
    me = lax.axis_index("dp")
    c = lax.rem(me, 2)
    j = lax.rem(lax.div(me, 2), NXY)
    y, x = lax.div(j, NX), lax.rem(j, NX)
    z = lax.div(me, 2 * NXY)
    oc = 1 - c

    def dev(zz, jj, cc):
        return ((zz * NXY + jj) * 2 + cc,)

    def zs(k, sign):
        o = zoff[k]
        return lax.rem(z + (o if sign > 0 else NZ - o), NZ)

    def xs(k, sign):
        a, b = xoff[k]
        yy = lax.rem(y + (a if sign > 0 else NY - a), NY)
        xx = lax.rem(x + (b if sign > 0 else NX - b), NX)
        return yy * NX + xx

    def slot(k, core):
        return (k // SL) * 2 * SL + core * SL + k % SL

    def send(src, dst, ss, rs, to):
        pltpu.make_async_remote_copy(src_ref=src, dst_ref=dst, send_sem=ss, recv_sem=rs,
                                     device_id=to, device_id_type=MESH).start()

    def wait(ref, sem):
        pltpu.make_async_copy(ref, ref, sem).wait()

    def vrows(s):
        return v_all.at[pl.ds(s * R, R), :]

    sc("barsig")
    bar = pltpu.get_barrier_semaphore()
    peers = [dev(zs(k, 1), j, c) for k in range(1, NZ)]
    peers += [dev(z, xs(k, 1), c) for k in range(1, NXY)]
    peers += [dev(z, j, oc)]
    for p in peers:
        pl.semaphore_signal(bar, inc=1, device_id=p, device_id_type=MESH)
    loads = [pltpu.make_async_copy(a, b, s_in.at[i]) for i, (a, b) in enumerate(
        ((vf_h, vf), (wvi_h, wvi), (wvo_h, wvo), (lq_h, lq), (qf_h, qf), (wqi_h, wqi), (wqo_h, wqo)))]
    for cp in loads:
        cp.start()

    def tower(xr, wi, wo, unit, inv, hid, act, cps):
        cps[0].wait()
        cps[1].wait()
        a = dot(xr[...], wi[...])
        h = jnp.maximum(a, 0.0).astype(bf16)
        cps[2].wait()
        e = dot(h, wo[...])
        r = lax.rsqrt(jnp.sum(e * e, axis=-1, keepdims=True) + EPS)
        u = e * r
        unit[...] = u
        inv[...] = jnp.broadcast_to(r, (R, 128))
        hid[...] = h
        act[...] = a
        return u.astype(bf16)

    def send_item(s, s2, ss, to):
        send(lq_all.at[s], lq_all.at[s2], s_lq, r_v.at[s2], to)
        send(vrows(s), vrows(s2), ss, r_v.at[s2], to)

    sc("tower_v")
    v_bf = tower(vf, wvi, wvo, vp, vi, vh, va, loads[0:3])
    v_all[0:R, :] = v_bf
    loads[3].wait()
    lq_all[0] = lq[...]
    sc("barwait")
    pl.semaphore_wait(bar, len(peers))
    sc("sends_v")
    for k in range(1, NXY):
        send_item(0, slot(k, 0), s_v, dev(z, xs(k, 1), c))
    send_item(0, slot(0, 1), s_vr, dev(z, j, oc))
    sc("tower_q")
    u_bf = tower(qf, wqi, wqo, up, ui, uh, ua, loads[4:7])
    u_all[0:R, :] = u_bf
    for k in range(1, NZ):
        send(u_all.at[pl.ds(0, R), :], u_all.at[pl.ds(k * R, R), :], s_u, r_u.at[k], dev(zs(k, 1), j, c))
    pos = jnp.sum(u_bf.astype(f32) * v_bf.astype(f32), axis=0, keepdims=True) * (1.0 / TEMP) - lq[...]
    stats[z, :, pl.ds(NQ + 128, 128)] = pos

    def grp(g):
        return slice(g * GR, (g + 1) * GR)

    def dyn(g):
        return pl.ds(pl.multiple_of(g * GR, GR), GR)

    def qcols(l):
        return slice(l * QC, (l + 1) * QC)

    def loop(lo, n, f):
        lax.fori_loop(0, n, lambda i, u: (f(lo + i), u)[1], 0)

    def bias(s0):
        q = lq_all[s0:s0 + SL].reshape(SL, 128)
        big = jnp.max(-q, axis=1, keepdims=True)
        b = (big + q) * LOG2E
        bt = jnp.transpose(jnp.concatenate([b] * (8 // SL), axis=0))
        for i in range(SL):
            mslot[s0 + i] = jnp.broadcast_to(big[i:i + 1, :], (1, 128))
            bcol[(s0 + i) * R:(s0 + i + 1) * R, :] = jnp.broadcast_to(bt[:, i:i + 1], (R, 128))

    def expo(n, g, l):
        rows, cols = grp(g), qcols(l)
        bb = bcol[rows, :]
        e = jnp.exp2(sbuf[n % 2] * (LOG2E / TEMP) - jnp.concatenate([bb, bb], axis=1))
        e_all[rows, cols] = e
        csum[2 * g:2 * g + 2, :, cols] = jnp.sum(e.reshape(2, R // 8, 8, QC), axis=1)

    def groups(l, core):
        return [l * NG + core * (NG // 2) + t for t in range(NG // 2)]

    done = []
    for l in range(LV + 1):
        sc(f"wait{l}")
        fresh = []
        if l < LV:
            for k in range(l * SL, (l + 1) * SL):
                if k:
                    wait(cnt, r_v.at[slot(k, 0)])
                    send_item(slot(k, 0), slot(k, 1), s_vr, dev(z, j, oc))
            for k in (2 * l, 2 * l + 1):
                if k:
                    wait(u_all.at[pl.ds(k * R, R), :], r_u.at[k])
            fresh += groups(l, 0)
        if l:
            for k in range((l - 1) * SL, l * SL):
                wait(cnt, r_v.at[slot(k, 1)])
            fresh += groups(l - 1, 1)
        sc(f"pass1_{l}")
        if l < LV:
            bias(slot(l * SL, 0))
        if l:
            bias(slot((l - 1) * SL, 1))
        tasks = [(g, l2) for g in fresh for l2 in range(min(l, LV - 1) + 1)]
        if l < LV:
            old = [g for g in range(LV * NG) if g in done]
            tasks = [(g, l) for g in old] + tasks
        done += fresh
        for n, (g, l2) in enumerate(tasks):
            sbuf[n % 2] = dot(v_all[grp(g), :], u_all[qcols(l2), :], NT)
            if n:
                expo(n - 1, *tasks[n - 1])
        expo(len(tasks) - 1, *tasks[-1])

    sc("stats_send")
    big = jnp.max(mslot[...], axis=0)
    stats[z, :, pl.ds(NQ, 128)] = big
    wslot[...] = jnp.exp2((mslot[...] - big) * LOG2E)
    for k in range(NZ):
        acc = csum[0, :, k * R:(k + 1) * R] * wslot[0]
        for s in range(1, 2 * NXY):
            acc = acc + csum[s, :, k * R:(k + 1) * R] * wslot[s]
        stats[z, :, pl.ds(pl.multiple_of(zs(k, -1) * R, R), R)] = jnp.sum(acc, axis=0, keepdims=True)
    for k in zfar:
        send(stats.at[z], stats.at[z], s_st, r_st, dev(zs(k, 1), j, c))
    sc("transpose")
    for g in range(LV * NG):
        vt[:, grp(g)] = jnp.transpose(v_all[grp(g), :].astype(f32)).astype(bf16)
    sc("stats_wait")
    wait(stats.at[pl.ds(0, NZ - 1)], r_st)
    sc("stats_comp")
    ms = [stats[k, :, NQ:NQ + 128] for k in range(NZ)]
    mx = functools.reduce(jnp.maximum, ms)
    tot = jnp.zeros((1, NQ), f32)
    for k in range(NZ):
        tot = tot + stats[k, :, 0:NQ] * jnp.concatenate([jnp.exp2((ms[k] - mx) * LOG2E)] * NZ, axis=1)
    invt[...] = jnp.concatenate([jnp.exp2((big - mx) * LOG2E)] * NZ, axis=1) / tot
    for k in range(NZ):
        invl[:, k * R:(k + 1) * R] = invt[:, pl.ds(pl.multiple_of(zs(k, -1) * R, R), R)]
    lse = jnp.log2(tot) * LN2 + jnp.concatenate([mx] * NZ, axis=1)
    lrow = jnp.zeros((1, 128), f32)
    for k in range(NZ):
        lrow = lrow + (lse[:, k * R:(k + 1) * R] - stats[k, :, NQ + 128:NQ + 256])
    loss_p[c] = lrow
    send(loss_p.at[c], loss_p.at[c], s_lp, r_lp, dev(z, j, oc))

    def norm(g, c0, c1):
        cols = slice(c0 * QC, c1 * QC)
        out = []
        for i in range(2):
            rows = slice(g * GR + i * R, g * GR + (i + 1) * R)
            p = e_all[rows, cols] * (invl[:, cols] * jnp.concatenate([wslot[2 * g + i]] * (2 * (c1 - c0)), axis=1))
            if g == 0 and i == 0 and c0 == 0:
                col = lax.broadcasted_iota(jnp.int32, p.shape, 1)
                p = jnp.where(lax.broadcasted_iota(jnp.int32, p.shape, 0) == col, p - 1.0, p)
            p = p.astype(bf16)
            g_all[rows, cols] = p
            out.append(p)
        return jnp.concatenate(out, axis=0)

    pend = []
    sv_of = {}
    for k, (a, b) in enumerate(xoff):
        sv_of[a, b] = k

    def flush(keep):
        while len(pend) > keep:
            for k in pend.pop(0):
                a, b = xoff[k]
                wait(pv_in.at[k], r_pv.at[k])
                sv[k] = sv[k] + pv_in[k]
                if b:
                    send(sv.at[k, pl.ds(0, H)], rx.at[a, b - 1], s_p1, r_x.at[a], dev(z, xs(sv_of[0, b], -1), c))
                if a:
                    send(sv.at[k, pl.ds(H, H)], ry.at[b, a - 1], s_p1, r_y.at[b], dev(z, xs(sv_of[a, 0], -1), c))

    normed = set()

    def ready(g, l):
        if (g, l) not in normed:
            normed.add((g, l))
            norm(g, l, l + 1)

    def dv_half(ls, core):
        sc(f"dv{ls[0]}{core}")
        ds = []
        for l in ls:
            gs = groups(l, core)
            for g in gs:
                for l2 in range(LV):
                    ready(g, l2)
            rows = [(gs[0] * GR, (gs[-1] + 1) * GR)] if len(ls) > 1 else [(g * GR, (g + 1) * GR) for g in gs]
            ds += [(l, r0 - gs[0] * GR, dot(g_all[r0:r1, :], u_all[...])) for r0, r1 in rows]
        keep = pv_out if core else sv
        for l, r0, d in ds:
            for i in range(d.shape[0] // R):
                keep[l * SL + r0 // R + i] = d[i * R:(i + 1) * R, :]
        for l in ls:
            ks = list(range(l * SL, (l + 1) * SL))
            if core:
                for k in ks:
                    send(pv_out.at[k], pv_in.at[k], s_pv, r_pv.at[k], dev(z, j, oc))
            else:
                pend.append(ks)
        if not core:
            sc(f"flush{ls[0]}")
            flush(0)

    def du_levels(ls):
        sc(f"du{ls[0]}")
        for l in ls:
            parts = []
            for lk in range(LV):
                for g in range(lk * NG, (lk + 1) * NG):
                    ready(g, l)
                rows = slice(lk * IR, (lk + 1) * IR)
                parts.append(dot(vt[:, rows], g_all[rows, qcols(l)]))
            d = functools.reduce(jnp.add, parts)
            for i in range(2):
                su[2 * l + i] = d[:, i * R:(i + 1) * R]
        ks = [k for l in ls for k in (2 * l, 2 * l + 1)]
        for k in ks:
            if k in hop:
                send(su.at[k], hop_in.at[k], s_su, r_hop.at[k], dev(lax.rem(z + NZ - hop[k], NZ), j, c))
        for k in ks:
            if k and k not in hop and k not in late:
                send(su.at[k], ru.at[k], s_su, r_su, dev(zs(k, -1), j, c))

    hop, late = {}, {}
    if NZ >= 8:
        for o, via in ((3, 2), (NZ - 3, NZ - 2)):
            hop[zoff.index(o)] = (o - via) % NZ
            late[zoff.index(via)] = zoff.index(o)

    def send_late():
        sc("late")
        for k, k2 in late.items():
            wait(hop_in.at[k2], r_hop.at[k2])
            su[k] = su[k] + hop_in[k2]
            send(su.at[k], ru.at[k], s_su, r_su, dev(zs(k, -1), j, c))

    if LV == 4:
        dv_half([1, 2], 1)
        du_levels([1, 2])
        dv_half([1, 2], 0)
        dv_half([3, 0], 1)
        du_levels([3, 0])
        dv_half([3, 0], 0)
        send_late()
    else:
        dv_half([0, 1], 1)
        du_levels([1, 0])
        dv_half([0, 1], 0)

    def leg2(o, own, r1, sem1, t1, r2, sem2, far):
        wait(r1.at[o], sem1.at[o])
        acc = own
        for i in range(r1.shape[1]):
            acc = acc + r1[o, i]
        t1[o] = acc
        if o:
            send(t1.at[o], r2.at[o - 1], s_p2, sem2, far)

    sc("leg2")
    for o in ring(max(NY, NX))[::-1]:
        if o < NY:
            leg2(o, sv[sv_of[o, 0], 0:H], rx, r_x, tx, r2x, r_2x, dev(z, xs(sv_of[o, 0], -1), c))
        if o < NX:
            leg2(o, sv[sv_of[0, o], H:R], ry, r_y, ty, r2y, r_2y, dev(z, xs(sv_of[0, o], -1), c))

    sc("loss")
    wait(loss_p.at[oc], r_lp)
    loss_x[j] = loss_p[0] + loss_p[1]
    for k in range(1, NXY):
        send(loss_x.at[j], loss_x.at[j], s_lx, r_lx, dev(z, xs(k, 1), c))

    def backward(du, xr, wo, unit, inv, hid, act, t):
        u, r = unit[...], inv[...]
        de = (r * (du - u * jnp.sum(u * du, axis=-1, keepdims=True))).astype(bf16)
        go = dot(hid[...], de, TN)
        dh = dot(de, wo[...], NT)
        da = jnp.where(act[...] > 0, dh, 0.0).astype(bf16)
        gi = dot(xr[...], da, TN)
        gl[t, 0:256, :] = gi[:, 0:128]
        gl[t, 256:512, :] = gi[:, 128:256]
        gl[t, 512:768, :] = go
        send(gl.at[t, pl.ds(pl.multiple_of(oc * 384, 8), 384), :], gpair.at[t], s_gp.at[t], r_gp.at[t], dev(z, j, oc))

    def pair_sum(t):
        sc(f"gp_wait{t}")
        wait(gpair.at[t], r_gp.at[t])
        gx_s[t] = (gl[t, pl.ds(pl.multiple_of(c * 384, 8), 384), :] + gpair[t]).reshape(NXY, CH, 128)
        for k in xfar:
            to = xs(k, 1)
            send(gx_s.at[t, to], gx_r.at[t, j], s_gx.at[t], r_gx.at[t], dev(z, to, c))
        gx_r[t, j] = gx_s[t, j]

    def plane_sum(t):
        sc(f"gx_wait{t}")
        wait(gx_r.at[t, pl.ds(0, NXY - 1)], r_gx.at[t])
        acc = gx_r[t, 0]
        for k in range(1, NXY):
            acc = acc + gx_r[t, k]
        gz_r[t, z] = acc
        for k in zfar:
            send(gz_r.at[t, z], gz_r.at[t, z], s_gz.at[t], r_gz.at[t], dev(zs(k, 1), j, c))

    def ring_sum(t):
        sc(f"gz_wait{t}")
        wait(gz_r.at[t, pl.ds(0, NZ - 1)], r_gz.at[t])
        acc = gz_r[t, 0]
        for k in range(1, NZ):
            acc = acc + gz_r[t, k]
        fin[t, c, j] = acc
        for k in xfar:
            send(fin.at[t, c, j], fin.at[t, c, j], s_ag.at[t], r_ag.at[t, k], dev(z, xs(k, 1), c))
        send(fin.at[t, c, j], fin.at[t, c, j], s_rl.at[t], r_rl.at[t, 0], dev(z, j, oc))

    def relay(t):
        sc(f"ag_wait{t}")
        for k in xfar:
            ref = fin.at[t, c, xs(k, -1)]
            wait(ref, r_ag.at[t, k])
            send(ref, ref, s_rl.at[t], r_rl.at[t, k], dev(z, j, oc))

    scale = 1.0 / (TEMP * B)
    sc("rv_wait")
    wait(r2x, r_2x)
    wait(r2y, r_2y)
    sc("bwd_v")
    top, bot = tx[0], ty[0]
    for i in range(NY - 1):
        top = top + r2x[i]
    for i in range(NX - 1):
        bot = bot + r2y[i]
    backward(jnp.concatenate([top, bot], axis=0) * scale, vf, wvo, vp, vi, vh, va, 1)
    pair_sum(1)
    sc("ru_wait")
    wait(ru.at[pl.ds(0, NZ - 1 - len(hop))], r_su)
    sc("bwd_q")
    acc = su[0]
    for k in range(1, NZ):
        if k not in hop:
            acc = acc + ru[k]
    backward(jnp.transpose(acc) * scale, qf, wqo, up, ui, uh, ua, 0)
    pair_sum(0)
    plane_sum(1)
    plane_sum(0)
    ring_sum(1)
    ring_sum(0)
    relay(1)
    relay(0)
    sc("loss2")
    wait(loss_x.at[pl.ds(0, NXY - 1)], r_lx)
    ls = loss_x[0]
    for k in range(1, NXY):
        ls = ls + loss_x[k]
    loss_o[...] = jnp.broadcast_to(jnp.sum(ls, axis=-1, keepdims=True) * (1.0 / B), (1, 128))
    sc("rl_wait")
    for t in range(2):
        for k in range(NXY):
            wait(fin.at[t, oc, xs(k, -1)], r_rl.at[t, k])

    sc("sendwait")
    wait(lq_all.at[pl.ds(0, 2 * NXY - 1)], s_lq)
    wait(u_all.at[pl.ds(0, (NZ - 1) * R), :], s_u)
    wait(v_all.at[pl.ds(0, (NXY - 1) * R), :], s_v)
    wait(v_all.at[pl.ds(0, NXY * R), :], s_vr)
    wait(stats.at[pl.ds(0, NZ - 1)], s_st)
    wait(loss_p.at[0], s_lp)
    wait(pv_out, s_pv)
    wait(sv.at[pl.ds(0, (NY * (NX - 1) + NX * (NY - 1)) // 2)], s_p1)
    wait(t_cnt, s_p2)
    wait(su.at[pl.ds(0, NZ - 1)], s_su)
    wait(loss_x.at[pl.ds(0, NXY - 1)], s_lx)
    for t in range(2):
        wait(gpair.at[t], s_gp.at[t])
        wait(gx_s.at[t, pl.ds(0, NXY - 1)], s_gx.at[t])
        wait(gz_r.at[t, pl.ds(0, NZ - 1)], s_gz.at[t])
        wait(gx_s.at[t, pl.ds(0, NXY - 1)], s_ag.at[t])
        wait(gx_s.at[t], s_rl.at[t])
    sc(None)


def emit(fin, loss, gqi, gqo, gvi, gvo, loss_o):
    for t, (gi, go) in enumerate(((gqi, gqo), (gvi, gvo))):
        full = fin[t].reshape(768, 128)
        gi[:, 0:128] = full[0:256]
        gi[:, 128:256] = full[256:512]
        go[...] = full[512:768]
    loss_o[...] = loss[...]


def build(NZ, NY, NX):
    def step(query_feat, item_feat, log_q, w_query_in, w_query_out, w_item_in, w_item_out):
        NXY = NY * NX
        NQ, NI, CH = NZ * R, 2 * NXY * R, 384 // NXY
        V, S = pltpu.VMEM, pltpu.SemaphoreType.DMA
        vm, hbm = pl.BlockSpec(memory_space=pltpu.VMEM), pl.BlockSpec(memory_space=pl.ANY)
        sd = jax.ShapeDtypeStruct
        tower = [V((R, 128), f32), V((R, 128), f32), V((R, 256), bf16), V((R, 256), f32)]
        fin, loss = pl.pallas_call(
            functools.partial(kernel, NZ, NY, NX),
            name="two_tower",
            out_shape=[pltpu.VMEM((2, 2, NXY, CH, 128), f32), pltpu.VMEM((1, 128), f32)],
            in_specs=[hbm] * 7,
            out_specs=[vm] * 2,
            scratch_shapes=[
                V((R, 256), bf16), V((R, 256), bf16), V((1, 128), f32),
                V((256, 256), bf16), V((256, 128), bf16), V((256, 256), bf16), V((256, 128), bf16), S((7,)),
                V((NQ, 128), bf16), V((NI, 128), bf16), V((128, NI), bf16), V((2 * NXY, 1, 128), f32), V((2 * NXY, 1, 128), f32), V((2 * NXY, 1, 128), f32), V((65, 1, 128), f32),
                V((NI, 128), f32), V((2, GR, 2 * R), f32), V((NI, NQ), f32), V((NI, NQ), bf16), V((2 * NXY, 8, NQ), f32),
                V((NZ, 1, NQ + 256), f32), V((1, NQ), f32), V((1, NQ), f32),
                *tower, *tower,
                V((NZ, 128, 128), f32), V((NZ, 128, 128), f32), V((NZ, 128, 128), f32),
                V((NXY, 128, 128), f32), V((NXY, 128, 128), f32), V((NXY, 128, 128), f32),
                V((NY, NX - 1, H, 128), f32), V((NX, NY - 1, H, 128), f32), V((NY, H, 128), f32), V((NX, H, 128), f32),
                V((NY - 1, H, 128), f32), V((NX - 1, H, 128), f32), V((NY + NX - 2, H, 128), f32),
                V((2, 768, 128), f32), V((2, 384, 128), f32), V((2, NXY, CH, 128), f32), V((2, NXY, CH, 128), f32),
                V((2, NZ, CH, 128), f32), V((2, 1, 128), f32), V((NXY, 1, 128), f32),
                S, S((NZ,)), S, S((2 * NXY,)), S, S, S, S, S((NXY,)), S, S, S((NY,)), S((NX,)), S, S, S, S, S((NZ,)),
                S((2,)), S((2,)), S((2,)), S((2,)), S((2,)), S((2,)), S((2,)), S((2, NXY)), S((2,)), S((2, NXY)),
                S, S, S, S, S,
            ],
            compiler_params=pltpu.CompilerParams(collective_id=0, has_side_effects=True, vmem_limit_bytes=60 * 2**20),
        )(query_feat, item_feat, log_q.reshape(1, 128), w_query_in, w_query_out, w_item_in, w_item_out)
        gqi, gqo, gvi, gvo, out = pl.pallas_call(
            emit,
            name="emit",
            out_shape=[sd((256, 256), f32), sd((256, 128), f32), sd((256, 256), f32), sd((256, 128), f32), sd((1, 128), f32)],
            in_specs=[vm] * 2,
            out_specs=[vm] * 5,
        )(pltpu.with_memory_space_constraint(fin, pltpu.VMEM), pltpu.with_memory_space_constraint(loss, pltpu.VMEM))
        return out[0, 0:1], gqi, gqo, gvi, gvo
    return step


def solution(mesh):
    n = mesh.shape["dp"]
    dims = (8, 4, 4) if n == 256 else (4, 2, 2)
    return jax.shard_map(build(*dims), mesh=mesh,
                         in_specs=(P("dp", None), P("dp", None), P("dp"), P(), P(), P(), P()),
                         out_specs=(P(), P(), P(), P(), P()), check_vma=False)
```

```python
import functools

import jax
import jax.numpy as jnp
from jax import lax
from jax.experimental import pallas as pl
from jax.experimental.pallas import tpu as pltpu
from jax.sharding import PartitionSpec as P

f32, bf16 = jnp.float32, jnp.bfloat16
MESH = pl.DeviceIdType.MESH
TEMP = 0.05
EPS = 1e-6
LOG2E = 1.4426950408889634
LN2 = 0.6931471805599453
NT = (((1,), (1,)), ((), ()))
TN = (((0,), (0,)), ((), ()))
NN = (((1,), (0,)), ((), ()))
R = 128
GR = 256
H = R // 2


class Scope:
    def __init__(self):
        self.cur = None

    def __call__(self, name):
        if self.cur is not None:
            self.cur.__exit__(None, None, None)
        self.cur = None
        if name:
            self.cur = jax.named_scope(name)
            self.cur.__enter__()


def dot(a, b, dims=NN):
    return lax.dot_general(a, b, dims, preferred_element_type=f32)


def arrange(near, level):
    rest = near[level:]
    return near[:level] + rest[level:][::-1] + rest[:level]


def ring(n):
    return sorted(range(n), key=lambda k: (min(k, n - k), k))


def torus(ny, nx):
    def dist(o):
        return min(o[0], ny - o[0]) + min(o[1], nx - o[1])
    return sorted(((a, b) for a in range(ny) for b in range(nx)), key=lambda o: (dist(o), o[0] * o[1] != 0, o))


def kernel(NZ, NY, NX, qf_h, vf_h, lq_h, wqi_h, wqo_h, wvi_h, wvo_h, fin, loss_o,
           qf, vf, lq, wqi, wqo, wvi, wvo, s_in,
           u4, v_all, vt, lq_all, mslot, wslot, cnt, bcol, sbuf, e_all, g_all, csum, stats, invl, invt,
           up, ui, uh, ua, vp, vi, vh, va,
           su, ru, hop_in, sv, rv, v2, b2, w2, e2, g2, il4, gl, gpair, gx_s, gx_r, gz_r, loss_p, loss_x,
           s_u, r_u, s_v, r_v, s_lq, s_st, r_st, s_sv, r_sv, s_u2, r_u2, s_il, r_il, s_su, r_su, r_hop,
           s_gp, r_gp, s_gx, r_gx, s_gz, r_gz, s_ag, r_ag, s_rl, r_rl, s_lp, r_lp, s_lx, r_lx, s_vr):
    sc = Scope()
    NXY = NY * NX
    NQ = NZ * R
    NI = 2 * NXY * R
    B = NZ * NI
    CH = 384 // NXY
    LV = NZ // 2
    SL = NXY // LV
    QC = 2 * R
    IR = 2 * SL * R
    NG = IR // GR
    zoff, xoff = arrange(ring(NZ), 2), arrange(torus(NY, NX), SL)
    zfar = [zoff.index(o) for o in ring(NZ)[:0:-1]]
    xfar = [xoff.index(o) for o in torus(NY, NX)[:0:-1]]
    me = lax.axis_index("dp")
    c = lax.rem(me, 2)
    j = lax.rem(lax.div(me, 2), NXY)
    y, x = lax.div(j, NX), lax.rem(j, NX)
    z = lax.div(me, 2 * NXY)
    oc = 1 - c

    def dev(zz, jj, cc):
        return ((zz * NXY + jj) * 2 + cc,)

    def zs(k, sign):
        o = zoff[k]
        return lax.rem(z + (o if sign > 0 else NZ - o), NZ)

    def xs(k, sign):
        a, b = xoff[k]
        yy = lax.rem(y + (a if sign > 0 else NY - a), NY)
        xx = lax.rem(x + (b if sign > 0 else NX - b), NX)
        return yy * NX + xx

    def ax(a, o):
        return lax.rem(y + o * (1 - a), NY) * NX + lax.rem(x + o * a, NX)

    def slot(k, core):
        return (k // SL) * 2 * SL + core * SL + k % SL

    def send(src, dst, ss, rs, to):
        pltpu.make_async_remote_copy(src_ref=src, dst_ref=dst, send_sem=ss, recv_sem=rs,
                                     device_id=to, device_id_type=MESH).start()

    def wait(ref, sem):
        pltpu.make_async_copy(ref, ref, sem).wait()

    def vrows(s):
        return v_all.at[pl.ds(s * R, R), :]

    sc("barsig")
    bar = pltpu.get_barrier_semaphore()
    peers = [dev(zs(k, 1), j, c) for k in range(1, NZ)]
    peers += [dev(z, xs(k, 1), c) for k in range(1, NXY)]
    peers += [dev(z, j, oc)]
    peers += [dev(z, ax(a, o), oc) for a in (0, 1) for o in range(1, NX)]
    for p in peers:
        pl.semaphore_signal(bar, inc=1, device_id=p, device_id_type=MESH)
    loads = [pltpu.make_async_copy(a, b, s_in.at[i]) for i, (a, b) in enumerate(
        ((vf_h, vf), (wvi_h, wvi), (wvo_h, wvo), (lq_h, lq), (qf_h, qf), (wqi_h, wqi), (wqo_h, wqo)))]
    for cp in loads:
        cp.start()

    def tower(xr, wi, wo, unit, inv, hid, act, cps):
        cps[0].wait()
        cps[1].wait()
        a = dot(xr[...], wi[...])
        h = jnp.maximum(a, 0.0).astype(bf16)
        cps[2].wait()
        e = dot(h, wo[...])
        r = lax.rsqrt(jnp.sum(e * e, axis=-1, keepdims=True) + EPS)
        u = e * r
        unit[...] = u
        inv[...] = jnp.broadcast_to(r, (R, 128))
        hid[...] = h
        act[...] = a
        return u.astype(bf16)

    def send_item(s, s2, ss, to):
        send(lq_all.at[s], lq_all.at[s2], s_lq, r_v.at[s2], to)
        send(vrows(s), vrows(s2), ss, r_v.at[s2], to)

    sc("tower_v")
    v_bf = tower(vf, wvi, wvo, vp, vi, vh, va, loads[0:3])
    v_all[0:R, :] = v_bf
    loads[3].wait()
    lq_all[0] = lq[...]
    sc("barwait")
    pl.semaphore_wait(bar, len(peers))
    sc("sends_v")
    for k in range(1, NXY):
        send_item(0, slot(k, 0), s_v, dev(z, xs(k, 1), c))
    send_item(0, slot(0, 1), s_vr, dev(z, j, oc))
    sc("tower_q")
    u_bf = tower(qf, wqi, wqo, up, ui, uh, ua, loads[4:7])
    u4[0:R, :] = u_bf
    for k in range(1, NZ):
        send(u4.at[pl.ds(0, R), :], u4.at[pl.ds(k * R, R), :], s_u, r_u.at[k], dev(zs(k, 1), j, c))
    pos = jnp.sum(u_bf.astype(f32) * v_bf.astype(f32), axis=0, keepdims=True) * (1.0 / TEMP) - lq[...]
    stats[z, :, pl.ds(NQ + 128, 128)] = pos

    def grp(g):
        return slice(g * GR, (g + 1) * GR)

    def dyn(g):
        return pl.ds(pl.multiple_of(g * GR, GR), GR)

    def qcols(l):
        return slice(l * QC, (l + 1) * QC)

    def loop(lo, n, f):
        lax.fori_loop(0, n, lambda i, u: (f(lo + i), u)[1], 0)

    def bias(s0):
        q = lq_all[s0:s0 + SL].reshape(SL, 128)
        big = jnp.max(-q, axis=1, keepdims=True)
        b = (big + q) * LOG2E
        bt = jnp.transpose(jnp.concatenate([b] * (8 // SL), axis=0))
        for i in range(SL):
            mslot[s0 + i] = jnp.broadcast_to(big[i:i + 1, :], (1, 128))
            bcol[(s0 + i) * R:(s0 + i + 1) * R, :] = jnp.broadcast_to(bt[:, i:i + 1], (R, 128))

    def expo(n, g, l):
        rows, cols = grp(g), qcols(l)
        bb = bcol[rows, :]
        e = jnp.exp2(sbuf[n % 2] * (LOG2E / TEMP) - jnp.concatenate([bb, bb], axis=1))
        e_all[rows, cols] = e
        csum[2 * g:2 * g + 2, :, cols] = jnp.sum(e.reshape(2, R // 8, 8, QC), axis=1)

    def groups(l, core):
        return [l * NG + core * (NG // 2) + t for t in range(NG // 2)]

    done = []
    for l in range(LV + 1):
        sc(f"wait{l}")
        fresh = []
        if l < LV:
            for k in range(l * SL, (l + 1) * SL):
                if k:
                    wait(cnt, r_v.at[slot(k, 0)])
                    send_item(slot(k, 0), slot(k, 1), s_vr, dev(z, j, oc))
            for k in (2 * l, 2 * l + 1):
                if k:
                    wait(u4.at[pl.ds(k * R, R), :], r_u.at[k])
            if l >= LV - 2:
                r0, nr = (0, (LV - 1) * QC) if l == LV - 2 else ((LV - 1) * QC, QC)
                for b in ring(NX)[1:]:
                    send(u4.at[pl.ds(r0, nr), :], u4.at[pl.ds(b * NQ + r0, nr), :], s_u2, r_u2.at[b], dev(z, ax(1 - c, b), c))
            fresh += groups(l, 0)
        if l:
            for k in range((l - 1) * SL, l * SL):
                wait(cnt, r_v.at[slot(k, 1)])
            fresh += groups(l - 1, 1)
        sc(f"pass1_{l}")
        if l < LV:
            bias(slot(l * SL, 0))
        if l:
            bias(slot((l - 1) * SL, 1))
        tasks = [(g, l2) for g in fresh for l2 in range(min(l, LV - 1) + 1)]
        if l < LV:
            old = [g for g in range(LV * NG) if g in done]
            tasks = [(g, l) for g in old] + tasks
        done += fresh
        for n, (g, l2) in enumerate(tasks):
            sbuf[n % 2] = dot(v_all[grp(g), :], u4[qcols(l2), :], NT)
            if n:
                expo(n - 1, *tasks[n - 1])
        expo(len(tasks) - 1, *tasks[-1])

    sc("stats_send")
    big = jnp.max(mslot[...], axis=0)
    stats[z, :, pl.ds(NQ, 128)] = big
    wslot[...] = jnp.exp2((mslot[...] - big) * LOG2E)
    for k in range(NZ):
        acc = csum[0, :, k * R:(k + 1) * R] * wslot[0]
        for s in range(1, 2 * NXY):
            acc = acc + csum[s, :, k * R:(k + 1) * R] * wslot[s]
        stats[z, :, pl.ds(pl.multiple_of(zs(k, -1) * R, R), R)] = jnp.sum(acc, axis=0, keepdims=True)
    for k in zfar:
        send(stats.at[z], stats.at[z], s_st, r_st, dev(zs(k, 1), j, c))
    sc("transpose")
    for g in range(LV * NG):
        vt[:, grp(g)] = jnp.transpose(v_all[grp(g), :].astype(f32)).astype(bf16)
    line = [(a, core) for a in ring(NX)[::-1] for core in (0, 1)]
    at = []
    for i, (a, core) in enumerate(line):
        s0, s1 = (slot(xoff.index(o), core) for o in ((a, 0), (0, a)))
        s = s0 + c * (s1 - s0)
        at.append(s)
        v2[i * R:(i + 1) * R, :] = v_all[pl.ds(s * R, R), :]
        b2[i * R:(i + 1) * R, :] = bcol[pl.ds(s * R, R), :]
        w2[i] = wslot[s]

    def line_exp(bs):
        sc(f"line{bs[0]}")
        for b in bs:
            wait(u4.at[pl.ds(b * NQ, NQ), :], r_u2.at[b])
        tasks = [(g, b, l) for b in bs for g in range(len(line) // 2) for l in range(LV)]

        def fin_exp(n, g, b, l):
            bb = b2[grp(g), :]
            e2[grp(g), (b - 1) * NQ + l * QC:(b - 1) * NQ + (l + 1) * QC] = jnp.exp2(
                sbuf[n % 2] * (LOG2E / TEMP) - jnp.concatenate([bb, bb], axis=1))

        for n, (g, b, l) in enumerate(tasks):
            sbuf[n % 2] = dot(v2[grp(g), :], u4[b * NQ + l * QC:b * NQ + (l + 1) * QC, :], NT)
            if n:
                fin_exp(n - 1, *tasks[n - 1])
        fin_exp(len(tasks) - 1, *tasks[-1])

    near = ring(NX)[1:]
    sc("stats_wait")
    wait(stats.at[pl.ds(0, NZ - 1)], r_st)
    sc("stats_comp")
    ms = [stats[k, :, NQ:NQ + 128] for k in range(NZ)]
    mx = functools.reduce(jnp.maximum, ms)
    tot = jnp.zeros((1, NQ), f32)
    for k in range(NZ):
        tot = tot + stats[k, :, 0:NQ] * jnp.concatenate([jnp.exp2((ms[k] - mx) * LOG2E)] * NZ, axis=1)
    invt[...] = jnp.concatenate([jnp.exp2((big - mx) * LOG2E)] * NZ, axis=1) / tot
    for k in range(NZ):
        invl[:, k * R:(k + 1) * R] = invt[:, pl.ds(pl.multiple_of(zs(k, -1) * R, R), R)]
    il4[0] = invl[...]
    for b in ring(NX)[1:]:
        send(il4.at[0], il4.at[b], s_il, r_il.at[b], dev(z, ax(1 - c, b), c))
    lse = jnp.log2(tot) * LN2 + jnp.concatenate([mx] * NZ, axis=1)
    lrow = jnp.zeros((1, 128), f32)
    for k in range(NZ):
        lrow = lrow + (lse[:, k * R:(k + 1) * R] - stats[k, :, NQ + 128:NQ + 256])
    loss_p[c] = lrow
    send(loss_p.at[c], loss_p.at[c], s_lp, r_lp, dev(z, j, oc))

    def norm(g, c0, c1):
        cols = slice(c0 * QC, c1 * QC)
        out = []
        for i in range(2):
            rows = slice(g * GR + i * R, g * GR + (i + 1) * R)
            p = e_all[rows, cols] * (invl[:, cols] * jnp.concatenate([wslot[2 * g + i]] * (2 * (c1 - c0)), axis=1))
            if g == 0 and i == 0 and c0 == 0:
                col = lax.broadcasted_iota(jnp.int32, p.shape, 1)
                p = jnp.where(lax.broadcasted_iota(jnp.int32, p.shape, 0) == col, p - 1.0, p)
            p = p.astype(bf16)
            g_all[rows, cols] = p
            out.append(p)
        return jnp.concatenate(out, axis=0)

    normed = set()

    def ready(g, l):
        if (g, l) not in normed:
            normed.add((g, l))
            norm(g, l, l + 1)

    def line_norm(g, bs):
        for i in (2 * g, 2 * g + 1):
            for b in bs:
                for l in range(LV):
                    cols = slice(l * QC, (l + 1) * QC)
                    f = il4[b, :, cols] * jnp.concatenate([w2[i], w2[i]], axis=1)
                    if b:
                        p = e2[i * R:(i + 1) * R, (b - 1) * NQ + l * QC:(b - 1) * NQ + (l + 1) * QC] * f
                    else:
                        p = e_all[pl.ds(pl.multiple_of(at[i] * R, R), R), cols] * f
                    if line[i] == (0, 0) and b == 0 and l == 0:
                        col = lax.broadcasted_iota(jnp.int32, p.shape, 1)
                        p = jnp.where(lax.broadcasted_iota(jnp.int32, p.shape, 0) == col, p - 1.0, p)
                    g2[i * R:(i + 1) * R, b * NQ + l * QC:b * NQ + (l + 1) * QC] = p.astype(bf16)

    def line_dots(gs, k0, k1):
        if len(gs) > 1:
            ds = [dot(g2[grp(g), k0:k1], u4[k0:k1, :]) for g in gs]
            ds = [d[i * R:(i + 1) * R] for d in ds for i in range(2)]
        else:
            ds = [dot(g2[i * R:(i + 1) * R, k0:k1], u4[k0:k1, :]) for i in (2 * gs[0], 2 * gs[0] + 1)]
        return [i for g in gs for i in (2 * g, 2 * g + 1)], ds

    def line_own():
        sc("ldv_own")
        gs = list(range(len(line) // 2))
        for g in gs:
            line_norm(g, [0])
        for i, d in zip(*line_dots(gs, 0, NQ)):
            sv[i] = d

    def line_dv(gs):
        sc(f"ldv{gs[0]}")
        for g in gs:
            line_norm(g, range(1, NX))
        idx, ds = line_dots(gs, NQ, NX * NQ)
        for i, d in zip(idx, ds):
            a, core = line[i]
            d = sv[i] + d
            if a or core:
                sv[i] = d
            else:
                rv[c * NX] = d
        for i in idx:
            a, core = line[i]
            if a or core:
                send(sv.at[i], rv.at[c * NX + a], s_sv, r_sv, dev(z, ax(c, NX - a), oc if core else c))

    def du_levels(ls):
        sc(f"du{ls[0]}")
        for l in ls:
            parts = []
            for lk in range(LV):
                for g in range(lk * NG, (lk + 1) * NG):
                    ready(g, l)
                rows = slice(lk * IR, (lk + 1) * IR)
                parts.append(dot(vt[:, rows], g_all[rows, qcols(l)]))
            d = functools.reduce(jnp.add, parts)
            for i in range(2):
                su[2 * l + i] = d[:, i * R:(i + 1) * R]
        ks = [k for l in ls for k in (2 * l, 2 * l + 1)]
        for k in ks:
            if k in hop:
                send(su.at[k], hop_in.at[k], s_su, r_hop.at[k], dev(lax.rem(z + NZ - hop[k], NZ), j, c))
        for k in ks:
            if k and k not in hop and k not in late:
                send(su.at[k], ru.at[k], s_su, r_su, dev(zs(k, -1), j, c))

    hop, late = {}, {}
    if NZ >= 8:
        for o, via in ((3, 2), (NZ - 3, NZ - 2)):
            hop[zoff.index(o)] = (o - via) % NZ
            late[zoff.index(via)] = zoff.index(o)

    def send_late():
        sc("late")
        for k, k2 in late.items():
            wait(hop_in.at[k2], r_hop.at[k2])
            su[k] = su[k] + hop_in[k2]
            send(su.at[k], ru.at[k], s_su, r_su, dev(zs(k, -1), j, c))

    if LV == 4:
        du_levels([1, 2])
        line_own()
        line_exp(near[:2])
        line_exp(near[2:])
        sc("il_wait")
        for b in near:
            wait(il4.at[b], r_il.at[b])
        line_dv([0])
        du_levels([3, 0])
        line_dv([1, 2])
        line_dv([3])
        send_late()
    else:
        du_levels([1, 0])
        line_exp(near)
        line_own()
        for b in near:
            wait(il4.at[b], r_il.at[b])
        line_dv([0])
        line_dv([1])

    sc("loss")
    wait(loss_p.at[oc], r_lp)
    loss_x[j] = loss_p[0] + loss_p[1]
    for k in range(1, NXY):
        send(loss_x.at[j], loss_x.at[j], s_lx, r_lx, dev(z, xs(k, 1), c))

    def backward(du, xr, wo, unit, inv, hid, act, t):
        u, r = unit[...], inv[...]
        de = (r * (du - u * jnp.sum(u * du, axis=-1, keepdims=True))).astype(bf16)
        go = dot(hid[...], de, TN)
        dh = dot(de, wo[...], NT)
        da = jnp.where(act[...] > 0, dh, 0.0).astype(bf16)
        gi = dot(xr[...], da, TN)
        gl[t, 0:256, :] = gi[:, 0:128]
        gl[t, 256:512, :] = gi[:, 128:256]
        gl[t, 512:768, :] = go
        send(gl.at[t, pl.ds(pl.multiple_of(oc * 384, 8), 384), :], gpair.at[t], s_gp.at[t], r_gp.at[t], dev(z, j, oc))

    def pair_sum(t):
        sc(f"gp_wait{t}")
        wait(gpair.at[t], r_gp.at[t])
        gx_s[t] = (gl[t, pl.ds(pl.multiple_of(c * 384, 8), 384), :] + gpair[t]).reshape(NXY, CH, 128)
        for k in xfar:
            to = xs(k, 1)
            send(gx_s.at[t, to], gx_r.at[t, j], s_gx.at[t], r_gx.at[t], dev(z, to, c))
        gx_r[t, j] = gx_s[t, j]

    def plane_sum(t):
        sc(f"gx_wait{t}")
        wait(gx_r.at[t, pl.ds(0, NXY - 1)], r_gx.at[t])
        acc = gx_r[t, 0]
        for k in range(1, NXY):
            acc = acc + gx_r[t, k]
        gz_r[t, z] = acc
        for k in zfar:
            send(gz_r.at[t, z], gz_r.at[t, z], s_gz.at[t], r_gz.at[t], dev(zs(k, 1), j, c))

    def ring_sum(t):
        sc(f"gz_wait{t}")
        wait(gz_r.at[t, pl.ds(0, NZ - 1)], r_gz.at[t])
        acc = gz_r[t, 0]
        for k in range(1, NZ):
            acc = acc + gz_r[t, k]
        fin[t, c, j] = acc
        for k in xfar:
            send(fin.at[t, c, j], fin.at[t, c, j], s_ag.at[t], r_ag.at[t, k], dev(z, xs(k, 1), c))
        send(fin.at[t, c, j], fin.at[t, c, j], s_rl.at[t], r_rl.at[t, 0], dev(z, j, oc))

    def relay(t):
        sc(f"ag_wait{t}")
        for k in xfar:
            ref = fin.at[t, c, xs(k, -1)]
            wait(ref, r_ag.at[t, k])
            send(ref, ref, s_rl.at[t], r_rl.at[t, k], dev(z, j, oc))

    scale = 1.0 / (TEMP * B)
    sc("rv_wait")
    wait(rv.at[pl.ds(0, 2 * NX - 1)], r_sv)
    sc("bwd_v")
    acc = rv[0]
    for i in range(1, 2 * NX):
        acc = acc + rv[i]
    backward(acc * scale, vf, wvo, vp, vi, vh, va, 1)
    pair_sum(1)
    sc("ru_wait")
    wait(ru.at[pl.ds(0, NZ - 1 - len(hop))], r_su)
    sc("bwd_q")
    acc = su[0]
    for k in range(1, NZ):
        if k not in hop:
            acc = acc + ru[k]
    backward(jnp.transpose(acc) * scale, qf, wqo, up, ui, uh, ua, 0)
    pair_sum(0)
    plane_sum(1)
    plane_sum(0)
    ring_sum(1)
    ring_sum(0)
    relay(1)
    relay(0)
    sc("loss2")
    wait(loss_x.at[pl.ds(0, NXY - 1)], r_lx)
    ls = loss_x[0]
    for k in range(1, NXY):
        ls = ls + loss_x[k]
    loss_o[...] = jnp.broadcast_to(jnp.sum(ls, axis=-1, keepdims=True) * (1.0 / B), (1, 128))
    sc("rl_wait")
    for t in range(2):
        for k in range(NXY):
            wait(fin.at[t, oc, xs(k, -1)], r_rl.at[t, k])

    sc("sendwait")
    wait(lq_all.at[pl.ds(0, 2 * NXY - 1)], s_lq)
    wait(u4.at[pl.ds(0, (NZ - 1) * R), :], s_u)
    wait(v_all.at[pl.ds(0, (NXY - 1) * R), :], s_v)
    wait(v_all.at[pl.ds(0, NXY * R), :], s_vr)
    wait(stats.at[pl.ds(0, NZ - 1)], s_st)
    wait(loss_p.at[0], s_lp)
    wait(sv.at[pl.ds(0, 2 * NX - 1)], s_sv)
    wait(u4.at[pl.ds(NQ, (NX - 1) * NQ), :], s_u2)
    wait(il4.at[pl.ds(1, NX - 1)], s_il)
    wait(su.at[pl.ds(0, NZ - 1)], s_su)
    wait(loss_x.at[pl.ds(0, NXY - 1)], s_lx)
    for t in range(2):
        wait(gpair.at[t], s_gp.at[t])
        wait(gx_s.at[t, pl.ds(0, NXY - 1)], s_gx.at[t])
        wait(gz_r.at[t, pl.ds(0, NZ - 1)], s_gz.at[t])
        wait(gx_s.at[t, pl.ds(0, NXY - 1)], s_ag.at[t])
        wait(gx_s.at[t], s_rl.at[t])
    sc(None)


def emit(fin, loss, gqi, gqo, gvi, gvo, loss_o):
    for t, (gi, go) in enumerate(((gqi, gqo), (gvi, gvo))):
        full = fin[t].reshape(768, 128)
        gi[:, 0:128] = full[0:256]
        gi[:, 128:256] = full[256:512]
        go[...] = full[512:768]
    loss_o[...] = loss[...]


def build(NZ, NY, NX):
    def step(query_feat, item_feat, log_q, w_query_in, w_query_out, w_item_in, w_item_out):
        NXY = NY * NX
        NQ, NI, CH = NZ * R, 2 * NXY * R, 384 // NXY
        V, S = pltpu.VMEM, pltpu.SemaphoreType.DMA
        vm, hbm = pl.BlockSpec(memory_space=pltpu.VMEM), pl.BlockSpec(memory_space=pl.ANY)
        sd = jax.ShapeDtypeStruct
        tower = [V((R, 128), f32), V((R, 128), f32), V((R, 256), bf16), V((R, 256), f32)]
        fin, loss = pl.pallas_call(
            functools.partial(kernel, NZ, NY, NX),
            name="two_tower",
            out_shape=[pltpu.VMEM((2, 2, NXY, CH, 128), f32), pltpu.VMEM((1, 128), f32)],
            in_specs=[hbm] * 7,
            out_specs=[vm] * 2,
            scratch_shapes=[
                V((R, 256), bf16), V((R, 256), bf16), V((1, 128), f32),
                V((256, 256), bf16), V((256, 128), bf16), V((256, 256), bf16), V((256, 128), bf16), S((7,)),
                V((NX * NQ, 128), bf16), V((NI, 128), bf16), V((128, NI), bf16), V((2 * NXY, 1, 128), f32), V((2 * NXY, 1, 128), f32), V((2 * NXY, 1, 128), f32), V((65, 1, 128), f32),
                V((NI, 128), f32), V((2, GR, 2 * R), f32), V((NI, NQ), f32), V((NI, NQ), bf16), V((2 * NXY, 8, NQ), f32),
                V((NZ, 1, NQ + 256), f32), V((1, NQ), f32), V((1, NQ), f32),
                *tower, *tower,
                V((NZ, 128, 128), f32), V((NZ, 128, 128), f32), V((NZ, 128, 128), f32),
                V((2 * NX, 128, 128), f32), V((2 * NX, 128, 128), f32),
                V((2 * NX * R, 128), bf16), V((2 * NX * R, 128), f32), V((2 * NX, 1, 128), f32),
                V((2 * NX * R, (NX - 1) * NQ), f32), V((2 * NX * R, NX * NQ), bf16), V((NX, 1, NQ), f32),
                V((2, 768, 128), f32), V((2, 384, 128), f32), V((2, NXY, CH, 128), f32), V((2, NXY, CH, 128), f32),
                V((2, NZ, CH, 128), f32), V((2, 1, 128), f32), V((NXY, 1, 128), f32),
                S, S((NZ,)), S, S((2 * NXY,)), S, S, S, S, S, S, S((NX,)), S, S((NX,)), S, S, S((NZ,)),
                S((2,)), S((2,)), S((2,)), S((2,)), S((2,)), S((2,)), S((2,)), S((2, NXY)), S((2,)), S((2, NXY)),
                S, S, S, S, S,
            ],
            compiler_params=pltpu.CompilerParams(collective_id=0, has_side_effects=True, vmem_limit_bytes=60 * 2**20),
        )(query_feat, item_feat, log_q.reshape(1, 128), w_query_in, w_query_out, w_item_in, w_item_out)
        gqi, gqo, gvi, gvo, out = pl.pallas_call(
            emit,
            name="emit",
            out_shape=[sd((256, 256), f32), sd((256, 128), f32), sd((256, 256), f32), sd((256, 128), f32), sd((1, 128), f32)],
            in_specs=[vm] * 2,
            out_specs=[vm] * 5,
        )(pltpu.with_memory_space_constraint(fin, pltpu.VMEM), pltpu.with_memory_space_constraint(loss, pltpu.VMEM))
        return out[0, 0:1], gqi, gqo, gvi, gvo
    return step


def solution(mesh):
    n = mesh.shape["dp"]
    dims = (8, 4, 4) if n == 256 else (4, 2, 2)
    return jax.shard_map(build(*dims), mesh=mesh,
                         in_specs=(P("dp", None), P("dp", None), P("dp"), P(), P(), P(), P()),
                         out_specs=(P(), P(), P(), P(), P()), check_vma=False)
```

```python
import functools

import jax
import jax.numpy as jnp
from jax import lax
from jax.experimental import pallas as pl
from jax.experimental.pallas import tpu as pltpu
from jax.sharding import PartitionSpec as P

f32, bf16 = jnp.float32, jnp.bfloat16
MESH = pl.DeviceIdType.MESH
TEMP = 0.05
EPS = 1e-6
LOG2E = 1.4426950408889634
LN2 = 0.6931471805599453
NT = (((1,), (1,)), ((), ()))
TN = (((0,), (0,)), ((), ()))
NN = (((1,), (0,)), ((), ()))
R = 128
GR = 256
ROWS = (256, 512), (384, 384)


class Scope:
    def __init__(self):
        self.cur = None

    def __call__(self, name):
        if self.cur is not None:
            self.cur.__exit__(None, None, None)
        self.cur = None
        if name:
            self.cur = jax.named_scope(name)
            self.cur.__enter__()


def dot(a, b, dims=NN):
    return lax.dot_general(a, b, dims, preferred_element_type=f32)


def arrange(near, level):
    rest = near[level:]
    return near[:level] + rest[level:][::-1] + rest[:level]


def ring(n):
    return sorted(range(n), key=lambda k: (min(k, n - k), k))


def torus(ny, nx):
    def dist(o):
        return min(o[0], ny - o[0]) + min(o[1], nx - o[1])
    return sorted(((a, b) for a in range(ny) for b in range(nx)), key=lambda o: (dist(o), o[0] * o[1] != 0, o))


def kernel(NZ, NY, NX, qf_h, vf_h, lq_h, wqi_h, wqo_h, wvi_h, wvo_h, fin, loss_o,
           qf, vf, lq, wqi, wqo, wvi, wvo, s_in,
           u4, v_all, vt, lq_all, mslot, wslot, cnt, bcol, sbuf, e_all, g_all, csum, stats, invl, invt,
           up, ui, uh, ua, vp, vi, vh, va,
           su, ru, hop_in, sv, rv, v2, b2, w2, e2, g2, il4, gl, gpair, gx_s, gx_r, gz_r, loss_p, loss_x,
           s_u, r_u, s_v, r_v, s_lq, s_st, r_st, s_sv, r_sv, s_u2, r_u2, s_il, r_il, s_su, r_su, r_hop,
           s_gp, r_gp, s_gx, r_gx, s_gz, r_gz, s_ag, r_ag, s_rl, r_rl, s_lp, r_lp, s_lx, r_lx, s_vr):
    sc = Scope()
    NXY = NY * NX
    NQ = NZ * R
    NI = 2 * NXY * R
    B = NZ * NI
    LV = NZ // 2
    SL = NXY // LV
    QC = 2 * R
    IR = 2 * SL * R
    NG = IR // GR
    zoff, xoff = arrange(ring(NZ), 2), arrange(torus(NY, NX), SL)
    zfar = [zoff.index(o) for o in ring(NZ)[:0:-1]]
    xfar = [xoff.index(o) for o in torus(NY, NX)[:0:-1]]
    me = lax.axis_index("dp")
    c = lax.rem(me, 2)
    j = lax.rem(lax.div(me, 2), NXY)
    y, x = lax.div(j, NX), lax.rem(j, NX)
    z = lax.div(me, 2 * NXY)
    oc = 1 - c

    def dev(zz, jj, cc):
        return ((zz * NXY + jj) * 2 + cc,)

    def zs(k, sign):
        o = zoff[k]
        return lax.rem(z + (o if sign > 0 else NZ - o), NZ)

    def xs(k, sign):
        a, b = xoff[k]
        yy = lax.rem(y + (a if sign > 0 else NY - a), NY)
        xx = lax.rem(x + (b if sign > 0 else NX - b), NX)
        return yy * NX + xx

    def ax(a, o):
        return lax.rem(y + o * (1 - a), NY) * NX + lax.rem(x + o * a, NX)

    def slot(k, core):
        return (k // SL) * 2 * SL + core * SL + k % SL

    def send(src, dst, ss, rs, to):
        pltpu.make_async_remote_copy(src_ref=src, dst_ref=dst, send_sem=ss, recv_sem=rs,
                                     device_id=to, device_id_type=MESH).start()

    def wait(ref, sem):
        pltpu.make_async_copy(ref, ref, sem).wait()

    def vrows(s):
        return v_all.at[pl.ds(s * R, R), :]

    sc("barsig")
    bar = pltpu.get_barrier_semaphore()
    peers = [dev(zs(k, 1), j, c) for k in range(1, NZ)]
    peers += [dev(z, xs(k, 1), c) for k in range(1, NXY)]
    peers += [dev(z, j, oc)]
    peers += [dev(z, ax(a, o), oc) for a in (0, 1) for o in range(1, NX)]
    for p in peers:
        pl.semaphore_signal(bar, inc=1, device_id=p, device_id_type=MESH)
    loads = [pltpu.make_async_copy(a, b, s_in.at[i]) for i, (a, b) in enumerate(
        ((vf_h, vf), (wvi_h, wvi), (wvo_h, wvo), (lq_h, lq), (qf_h, qf), (wqi_h, wqi), (wqo_h, wqo)))]
    for cp in loads:
        cp.start()

    def tower(xr, wi, wo, unit, inv, hid, act, cps):
        cps[0].wait()
        cps[1].wait()
        a = dot(xr[...], wi[...])
        h = jnp.maximum(a, 0.0).astype(bf16)
        cps[2].wait()
        e = dot(h, wo[...])
        r = lax.rsqrt(jnp.sum(e * e, axis=-1, keepdims=True) + EPS)
        u = e * r
        unit[...] = u
        inv[...] = jnp.broadcast_to(r, (R, 128))
        hid[...] = h
        act[...] = a
        return u.astype(bf16)

    def send_item(s, s2, ss, to):
        send(lq_all.at[s], lq_all.at[s2], s_lq, r_v.at[s2], to)
        send(vrows(s), vrows(s2), ss, r_v.at[s2], to)

    sc("tower_v")
    v_bf = tower(vf, wvi, wvo, vp, vi, vh, va, loads[0:3])
    v_all[0:R, :] = v_bf
    loads[3].wait()
    lq_all[0] = lq[...]
    sc("barwait")
    pl.semaphore_wait(bar, len(peers))
    sc("sends_v")
    for k in range(1, NXY):
        send_item(0, slot(k, 0), s_v, dev(z, xs(k, 1), c))
    send_item(0, slot(0, 1), s_vr, dev(z, j, oc))
    sc("tower_q")
    u_bf = tower(qf, wqi, wqo, up, ui, uh, ua, loads[4:7])
    u4[0:R, :] = u_bf
    for k in range(1, NZ):
        send(u4.at[pl.ds(0, R), :], u4.at[pl.ds(k * R, R), :], s_u, r_u.at[k], dev(zs(k, 1), j, c))
    pos = jnp.sum(u_bf.astype(f32) * v_bf.astype(f32), axis=0, keepdims=True) * (1.0 / TEMP) - lq[...]
    stats[z, :, pl.ds(NQ + 128, 128)] = pos

    def grp(g):
        return slice(g * GR, (g + 1) * GR)

    def dyn(g):
        return pl.ds(pl.multiple_of(g * GR, GR), GR)

    def qcols(l):
        return slice(l * QC, (l + 1) * QC)

    def loop(lo, n, f):
        lax.fori_loop(0, n, lambda i, u: (f(lo + i), u)[1], 0)

    def bias(s0):
        q = lq_all[s0:s0 + SL].reshape(SL, 128)
        big = jnp.max(-q, axis=1, keepdims=True)
        b = (big + q) * LOG2E
        bt = jnp.transpose(jnp.concatenate([b] * (8 // SL), axis=0))
        for i in range(SL):
            mslot[s0 + i] = jnp.broadcast_to(big[i:i + 1, :], (1, 128))
            bcol[(s0 + i) * R:(s0 + i + 1) * R, :] = jnp.broadcast_to(bt[:, i:i + 1], (R, 128))

    def expo(n, g, l):
        rows, cols = grp(g), qcols(l)
        bb = bcol[rows, :]
        e = jnp.exp2(sbuf[n % 2] * (LOG2E / TEMP) - jnp.concatenate([bb, bb], axis=1))
        e_all[rows, cols] = e
        csum[2 * g:2 * g + 2, :, cols] = jnp.sum(e.reshape(2, R // 8, 8, QC), axis=1)

    def groups(l, core):
        return [l * NG + core * (NG // 2) + t for t in range(NG // 2)]

    done = []
    for l in range(LV + 1):
        sc(f"wait{l}")
        fresh = []
        if l < LV:
            for k in range(l * SL, (l + 1) * SL):
                if k:
                    wait(cnt, r_v.at[slot(k, 0)])
                    send_item(slot(k, 0), slot(k, 1), s_vr, dev(z, j, oc))
            for k in (2 * l, 2 * l + 1):
                if k:
                    wait(u4.at[pl.ds(k * R, R), :], r_u.at[k])
            if l >= LV - 2:
                r0, nr = (0, (LV - 1) * QC) if l == LV - 2 else ((LV - 1) * QC, QC)
                for b in ring(NX)[1:]:
                    send(u4.at[pl.ds(r0, nr), :], u4.at[pl.ds(b * NQ + r0, nr), :], s_u2, r_u2.at[b], dev(z, ax(1 - c, b), c))
            fresh += groups(l, 0)
        if l:
            for k in range((l - 1) * SL, l * SL):
                wait(cnt, r_v.at[slot(k, 1)])
            fresh += groups(l - 1, 1)
        sc(f"pass1_{l}")
        if l < LV:
            bias(slot(l * SL, 0))
        if l:
            bias(slot((l - 1) * SL, 1))
        tasks = [(g, l2) for g in fresh for l2 in range(min(l, LV - 1) + 1)]
        if l < LV:
            old = [g for g in range(LV * NG) if g in done]
            tasks = [(g, l) for g in old] + tasks
        done += fresh
        for n, (g, l2) in enumerate(tasks):
            sbuf[n % 2] = dot(v_all[grp(g), :], u4[qcols(l2), :], NT)
            if n:
                expo(n - 1, *tasks[n - 1])
        expo(len(tasks) - 1, *tasks[-1])

    sc("stats_send")
    big = jnp.max(mslot[...], axis=0)
    stats[z, :, pl.ds(NQ, 128)] = big
    wslot[...] = jnp.exp2((mslot[...] - big) * LOG2E)
    for k in range(NZ):
        acc = csum[0, :, k * R:(k + 1) * R] * wslot[0]
        for s in range(1, 2 * NXY):
            acc = acc + csum[s, :, k * R:(k + 1) * R] * wslot[s]
        stats[z, :, pl.ds(pl.multiple_of(zs(k, -1) * R, R), R)] = jnp.sum(acc, axis=0, keepdims=True)
    for k in zfar:
        send(stats.at[z], stats.at[z], s_st, r_st, dev(zs(k, 1), j, c))
    sc("transpose")
    for g in range(LV * NG):
        vt[:, grp(g)] = jnp.transpose(v_all[grp(g), :].astype(f32)).astype(bf16)
    line = [(a, core) for a in ring(NX)[::-1] for core in (0, 1)]
    at = []
    for i, (a, core) in enumerate(line):
        s0, s1 = (slot(xoff.index(o), core) for o in ((a, 0), (0, a)))
        s = s0 + c * (s1 - s0)
        at.append(s)
        v2[i * R:(i + 1) * R, :] = v_all[pl.ds(s * R, R), :]
        b2[i * R:(i + 1) * R, :] = bcol[pl.ds(s * R, R), :]
        w2[i] = wslot[s]

    def line_exp(bs):
        sc(f"line{bs[0]}")
        for b in bs:
            wait(u4.at[pl.ds(b * NQ, NQ), :], r_u2.at[b])
        tasks = [(g, b, l) for b in bs for g in range(len(line) // 2) for l in range(LV)]

        def fin_exp(n, g, b, l):
            bb = b2[grp(g), :]
            e2[grp(g), (b - 1) * NQ + l * QC:(b - 1) * NQ + (l + 1) * QC] = jnp.exp2(
                sbuf[n % 2] * (LOG2E / TEMP) - jnp.concatenate([bb, bb], axis=1))

        for n, (g, b, l) in enumerate(tasks):
            sbuf[n % 2] = dot(v2[grp(g), :], u4[b * NQ + l * QC:b * NQ + (l + 1) * QC, :], NT)
            if n:
                fin_exp(n - 1, *tasks[n - 1])
        fin_exp(len(tasks) - 1, *tasks[-1])

    near = ring(NX)[1:]
    sc("stats_wait")
    wait(stats.at[pl.ds(0, NZ - 1)], r_st)
    sc("stats_comp")
    ms = [stats[k, :, NQ:NQ + 128] for k in range(NZ)]
    mx = functools.reduce(jnp.maximum, ms)
    tot = jnp.zeros((1, NQ), f32)
    for k in range(NZ):
        tot = tot + stats[k, :, 0:NQ] * jnp.concatenate([jnp.exp2((ms[k] - mx) * LOG2E)] * NZ, axis=1)
    invt[...] = jnp.concatenate([jnp.exp2((big - mx) * LOG2E)] * NZ, axis=1) / tot
    for k in range(NZ):
        invl[:, k * R:(k + 1) * R] = invt[:, pl.ds(pl.multiple_of(zs(k, -1) * R, R), R)]
    il4[0] = invl[...]
    for b in ring(NX)[1:]:
        send(il4.at[0], il4.at[b], s_il, r_il.at[b], dev(z, ax(1 - c, b), c))
    lse = jnp.log2(tot) * LN2 + jnp.concatenate([mx] * NZ, axis=1)
    lrow = jnp.zeros((1, 128), f32)
    for k in range(NZ):
        lrow = lrow + (lse[:, k * R:(k + 1) * R] - stats[k, :, NQ + 128:NQ + 256])
    loss_p[c] = lrow
    send(loss_p.at[c], loss_p.at[c], s_lp, r_lp, dev(z, j, oc))

    def norm(g, c0, c1):
        cols = slice(c0 * QC, c1 * QC)
        out = []
        for i in range(2):
            rows = slice(g * GR + i * R, g * GR + (i + 1) * R)
            p = e_all[rows, cols] * (invl[:, cols] * jnp.concatenate([wslot[2 * g + i]] * (2 * (c1 - c0)), axis=1))
            if g == 0 and i == 0 and c0 == 0:
                col = lax.broadcasted_iota(jnp.int32, p.shape, 1)
                p = jnp.where(lax.broadcasted_iota(jnp.int32, p.shape, 0) == col, p - 1.0, p)
            p = p.astype(bf16)
            g_all[rows, cols] = p
            out.append(p)
        return jnp.concatenate(out, axis=0)

    normed = set()

    def ready(g, l):
        if (g, l) not in normed:
            normed.add((g, l))
            norm(g, l, l + 1)

    def line_norm(g, bs):
        for i in (2 * g, 2 * g + 1):
            for b in bs:
                for l in range(LV):
                    cols = slice(l * QC, (l + 1) * QC)
                    f = il4[b, :, cols] * jnp.concatenate([w2[i], w2[i]], axis=1)
                    if b:
                        p = e2[i * R:(i + 1) * R, (b - 1) * NQ + l * QC:(b - 1) * NQ + (l + 1) * QC] * f
                    else:
                        p = e_all[pl.ds(pl.multiple_of(at[i] * R, R), R), cols] * f
                    if line[i] == (0, 0) and b == 0 and l == 0:
                        col = lax.broadcasted_iota(jnp.int32, p.shape, 1)
                        p = jnp.where(lax.broadcasted_iota(jnp.int32, p.shape, 0) == col, p - 1.0, p)
                    g2[i * R:(i + 1) * R, b * NQ + l * QC:b * NQ + (l + 1) * QC] = p.astype(bf16)

    def line_dots(gs, k0, k1):
        if len(gs) > 1:
            ds = [dot(g2[grp(g), k0:k1], u4[k0:k1, :]) for g in gs]
            ds = [d[i * R:(i + 1) * R] for d in ds for i in range(2)]
        else:
            ds = [dot(g2[i * R:(i + 1) * R, k0:k1], u4[k0:k1, :]) for i in (2 * gs[0], 2 * gs[0] + 1)]
        return [i for g in gs for i in (2 * g, 2 * g + 1)], ds

    def line_own():
        sc("ldv_own")
        gs = list(range(len(line) // 2))
        for g in gs:
            line_norm(g, [0])
        for i, d in zip(*line_dots(gs, 0, NQ)):
            sv[i] = d

    def line_dv(gs):
        sc(f"ldv{gs[0]}")
        for g in gs:
            line_norm(g, range(1, NX))
        idx, ds = line_dots(gs, NQ, NX * NQ)
        for i, d in zip(idx, ds):
            a, core = line[i]
            d = sv[i] + d
            if a or core:
                sv[i] = d
            else:
                rv[c * NX] = d
        for i in idx:
            a, core = line[i]
            if a or core:
                send(sv.at[i], rv.at[c * NX + a], s_sv, r_sv, dev(z, ax(c, NX - a), oc if core else c))

    def du_levels(ls):
        sc(f"du{ls[0]}")
        for l in ls:
            parts = []
            for lk in range(LV):
                for g in range(lk * NG, (lk + 1) * NG):
                    ready(g, l)
                rows = slice(lk * IR, (lk + 1) * IR)
                parts.append(dot(vt[:, rows], g_all[rows, qcols(l)]))
            d = functools.reduce(jnp.add, parts)
            for i in range(2):
                su[2 * l + i] = d[:, i * R:(i + 1) * R]
        ks = [k for l in ls for k in (2 * l, 2 * l + 1)]
        for k in ks:
            if k in hop:
                send(su.at[k], hop_in.at[k], s_su, r_hop.at[k], dev(lax.rem(z + NZ - hop[k], NZ), j, c))
        for k in ks:
            if k and k not in hop and k not in late:
                send(su.at[k], ru.at[k], s_su, r_su, dev(zs(k, -1), j, c))

    hop, late = {}, {}
    if NZ >= 8:
        for o, via in ((3, 2), (NZ - 3, NZ - 2)):
            hop[zoff.index(o)] = (o - via) % NZ
            late[zoff.index(via)] = zoff.index(o)

    def send_late(ks):
        sc("late")
        for k in ks:
            k2 = late[k]
            wait(hop_in.at[k2], r_hop.at[k2])
            su[k] = su[k] + hop_in[k2]
            send(su.at[k], ru.at[k], s_su, r_su, dev(zs(k, -1), j, c))

    if LV == 4:
        du_levels([1, 2])
        line_own()
        line_exp(near[:2])
        line_exp(near[2:])
        sc("il_wait")
        for b in near:
            wait(il4.at[b], r_il.at[b])
        line_dv([0])
        line_dv([1, 2])
        du_levels([3, 0])
        send_late([k for k in late if k // 2 == 2])
        line_dv([3])
        send_late([k for k in late if k // 2 != 2])
    else:
        du_levels([1, 0])
        line_exp(near)
        line_own()
        for b in near:
            wait(il4.at[b], r_il.at[b])
        line_dv([0])
        line_dv([1])

    sc("loss")
    wait(loss_p.at[oc], r_lp)
    loss_x[j] = loss_p[0] + loss_p[1]
    for k in range(1, NXY):
        send(loss_x.at[j], loss_x.at[j], s_lx, r_lx, dev(z, xs(k, 1), c))

    def per_core(f):
        for core in (0, 1):
            @pl.when(c == core)
            def _():
                f(core)

    def chunk(t, core):
        return ROWS[t][core] // NXY

    def rows_of(t, core, k):
        return pl.ds(pl.multiple_of(k * chunk(t, core), 8), chunk(t, core))

    def backward(du, xr, wo, unit, inv, hid, act, t):
        u, r = unit[...], inv[...]
        de = (r * (du - u * jnp.sum(u * du, axis=-1, keepdims=True))).astype(bf16)
        go = dot(hid[...], de, TN)
        dh = dot(de, wo[...], NT)
        da = jnp.where(act[...] > 0, dh, 0.0).astype(bf16)
        gi = dot(xr[...], da, TN)
        gl[t, 0:256, :] = gi[:, 0:128]
        gl[t, 256:512, :] = gi[:, 128:256]
        gl[t, 512:768, :] = go

        @per_core
        def _(core):
            o = 1 - core
            send(gl.at[t, pl.ds(o * ROWS[t][0], ROWS[t][o]), :], gpair.at[t, pl.ds(0, ROWS[t][o]), :], s_gp.at[t], r_gp.at[t], dev(z, j, oc))

    def pair_sum(t):
        sc(f"gp_wait{t}")

        @per_core
        def _(core):
            wait(gpair.at[t, pl.ds(0, ROWS[t][core]), :], r_gp.at[t])
            gx_s[t, 0:ROWS[t][core], :] = gl[t, core * ROWS[t][0]:core * ROWS[t][0] + ROWS[t][core], :] + gpair[t, 0:ROWS[t][core], :]
            for k in xfar:
                to = xs(k, 1)
                send(gx_s.at[t, rows_of(t, core, to), :], gx_r.at[t, rows_of(t, core, j), :], s_gx.at[t], r_gx.at[t], dev(z, to, c))
            gx_r[t, rows_of(t, core, j), :] = gx_s[t, rows_of(t, core, j), :]

    def plane_sum(t):
        sc(f"gx_wait{t}")

        @per_core
        def _(core):
            n = chunk(t, core)
            wait(gx_r.at[t, pl.ds(0, (NXY - 1) * n), :], r_gx.at[t])
            acc = gx_r[t, 0:n, :]
            for k in range(1, NXY):
                acc = acc + gx_r[t, k * n:(k + 1) * n, :]
            gz_r[t, rows_of(t, core, z), :] = acc
            for k in zfar:
                send(gz_r.at[t, rows_of(t, core, z), :], gz_r.at[t, rows_of(t, core, z), :], s_gz.at[t], r_gz.at[t], dev(zs(k, 1), j, c))

    def part(t, core, jj):
        return fin.at[t, pl.ds(pl.multiple_of(core * ROWS[t][0] + jj * chunk(t, core), 8), chunk(t, core)), :]

    def ring_sum(t):
        sc(f"gz_wait{t}")

        @per_core
        def _(core):
            n = chunk(t, core)
            wait(gz_r.at[t, pl.ds(0, (NZ - 1) * n), :], r_gz.at[t])
            acc = gz_r[t, 0:n, :]
            for k in range(1, NZ):
                acc = acc + gz_r[t, k * n:(k + 1) * n, :]
            mine = part(t, core, j)
            mine[...] = acc
            for k in xfar:
                send(mine, mine, s_ag.at[t], r_ag.at[t, k], dev(z, xs(k, 1), c))
            send(mine, mine, s_rl.at[t], r_rl.at[t, 0], dev(z, j, oc))

    def relay(t):
        sc(f"ag_wait{t}")

        @per_core
        def _(core):
            for k in xfar:
                ref = part(t, core, xs(k, -1))
                wait(ref, r_ag.at[t, k])
                send(ref, ref, s_rl.at[t], r_rl.at[t, k], dev(z, j, oc))

    scale = 1.0 / (TEMP * B)
    sc("rv_wait")
    wait(rv.at[pl.ds(0, 2 * NX - 1)], r_sv)
    sc("bwd_v")
    acc = rv[0]
    for i in range(1, 2 * NX):
        acc = acc + rv[i]
    backward(acc * scale, vf, wvo, vp, vi, vh, va, 1)
    pair_sum(1)
    sc("ru_wait")
    wait(ru.at[pl.ds(0, NZ - 1 - len(hop))], r_su)
    sc("bwd_q")
    acc = su[0]
    for k in range(1, NZ):
        if k not in hop:
            acc = acc + ru[k]
    backward(jnp.transpose(acc) * scale, qf, wqo, up, ui, uh, ua, 0)
    pair_sum(0)
    sc("loss2")
    wait(loss_x.at[pl.ds(0, NXY - 1)], r_lx)
    ls = loss_x[0]
    for k in range(1, NXY):
        ls = ls + loss_x[k]
    loss_o[...] = jnp.broadcast_to(jnp.sum(ls, axis=-1, keepdims=True) * (1.0 / B), (1, 128))
    plane_sum(1)
    plane_sum(0)
    ring_sum(1)
    ring_sum(0)
    relay(1)
    relay(0)
    sc("rl_wait")

    @per_core
    def _(core):
        for t in range(2):
            for k in range(NXY):
                wait(part(t, 1 - core, xs(k, -1)), r_rl.at[t, k])

    sc("sendwait")
    wait(lq_all.at[pl.ds(0, 2 * NXY - 1)], s_lq)
    wait(u4.at[pl.ds(0, (NZ - 1) * R), :], s_u)
    wait(v_all.at[pl.ds(0, (NXY - 1) * R), :], s_v)
    wait(v_all.at[pl.ds(0, NXY * R), :], s_vr)
    wait(stats.at[pl.ds(0, NZ - 1)], s_st)
    wait(loss_p.at[0], s_lp)
    wait(sv.at[pl.ds(0, 2 * NX - 1)], s_sv)
    wait(u4.at[pl.ds(NQ, (NX - 1) * NQ), :], s_u2)
    wait(il4.at[pl.ds(1, NX - 1)], s_il)
    wait(su.at[pl.ds(0, NZ - 1)], s_su)
    wait(loss_x.at[pl.ds(0, NXY - 1)], s_lx)

    @per_core
    def _(core):
        for t in range(2):
            n = chunk(t, core)
            wait(gpair.at[t, pl.ds(0, ROWS[t][1 - core]), :], s_gp.at[t])
            wait(gx_s.at[t, pl.ds(0, (NXY - 1) * n), :], s_gx.at[t])
            wait(gz_r.at[t, pl.ds(0, (NZ - 1) * n), :], s_gz.at[t])
            wait(gx_s.at[t, pl.ds(0, (NXY - 1) * n), :], s_ag.at[t])
            wait(gx_s.at[t, pl.ds(0, NXY * n), :], s_rl.at[t])

    sc(None)


def emit(fin, loss, gqi, gqo, gvi, gvo, loss_o, sem):
    copies = [(loss, loss_o)]
    for t, (gi, go) in enumerate(((gqi, gqo), (gvi, gvo))):
        copies += [(fin.at[t, 0:256, :], gi.at[:, 0:128]), (fin.at[t, 256:512, :], gi.at[:, 128:256]), (fin.at[t, 512:768, :], go)]
    copies = [pltpu.make_async_copy(a, b, sem.at[i]) for i, (a, b) in enumerate(copies)]
    for cp in copies:
        cp.start()
    for cp in copies:
        cp.wait()


def build(NZ, NY, NX):
    def step(query_feat, item_feat, log_q, w_query_in, w_query_out, w_item_in, w_item_out):
        NXY = NY * NX
        NQ, NI = NZ * R, 2 * NXY * R
        V, S = pltpu.VMEM, pltpu.SemaphoreType.DMA
        vm, hbm = pl.BlockSpec(memory_space=pltpu.VMEM), pl.BlockSpec(memory_space=pl.ANY)
        sd = jax.ShapeDtypeStruct
        tower = [V((R, 128), f32), V((R, 128), f32), V((R, 256), bf16), V((R, 256), f32)]
        fin, loss = pl.pallas_call(
            functools.partial(kernel, NZ, NY, NX),
            name="two_tower",
            out_shape=[pltpu.VMEM((2, 768, 128), f32), pltpu.VMEM((1, 128), f32)],
            in_specs=[hbm] * 7,
            out_specs=[vm] * 2,
            scratch_shapes=[
                V((R, 256), bf16), V((R, 256), bf16), V((1, 128), f32),
                V((256, 256), bf16), V((256, 128), bf16), V((256, 256), bf16), V((256, 128), bf16), S((7,)),
                V((NX * NQ, 128), bf16), V((NI, 128), bf16), V((128, NI), bf16), V((2 * NXY, 1, 128), f32), V((2 * NXY, 1, 128), f32), V((2 * NXY, 1, 128), f32), V((65, 1, 128), f32),
                V((NI, 128), f32), V((2, GR, 2 * R), f32), V((NI, NQ), f32), V((NI, NQ), bf16), V((2 * NXY, 8, NQ), f32),
                V((NZ, 1, NQ + 256), f32), V((1, NQ), f32), V((1, NQ), f32),
                *tower, *tower,
                V((NZ, 128, 128), f32), V((NZ, 128, 128), f32), V((NZ, 128, 128), f32),
                V((2 * NX, 128, 128), f32), V((2 * NX, 128, 128), f32),
                V((2 * NX * R, 128), bf16), V((2 * NX * R, 128), f32), V((2 * NX, 1, 128), f32),
                V((2 * NX * R, (NX - 1) * NQ), f32), V((2 * NX * R, NX * NQ), bf16), V((NX, 1, NQ), f32),
                V((2, 768, 128), f32), V((2, max(map(max, ROWS)), 128), f32), V((2, max(map(max, ROWS)), 128), f32), V((2, max(map(max, ROWS)), 128), f32),
                V((2, NZ * max(map(max, ROWS)) // NXY, 128), f32), V((2, 1, 128), f32), V((NXY, 1, 128), f32),
                S, S((NZ,)), S, S((2 * NXY,)), S, S, S, S, S, S, S((NX,)), S, S((NX,)), S, S, S((NZ,)),
                S((2,)), S((2,)), S((2,)), S((2,)), S((2,)), S((2,)), S((2,)), S((2, NXY)), S((2,)), S((2, NXY)),
                S, S, S, S, S,
            ],
            compiler_params=pltpu.CompilerParams(collective_id=0, has_side_effects=True, vmem_limit_bytes=60 * 2**20),
        )(query_feat, item_feat, log_q.reshape(1, 128), w_query_in, w_query_out, w_item_in, w_item_out)
        gqi, gqo, gvi, gvo, out = pl.pallas_call(
            emit,
            name="emit",
            out_shape=[sd((256, 256), f32), sd((256, 128), f32), sd((256, 256), f32), sd((256, 128), f32), sd((1, 128), f32)],
            in_specs=[vm] * 2,
            out_specs=[hbm] * 5,
            scratch_shapes=[S((7,))],
        )(pltpu.with_memory_space_constraint(fin, pltpu.VMEM), pltpu.with_memory_space_constraint(loss, pltpu.VMEM))
        return out[0, 0:1], gqi, gqo, gvi, gvo
    return step


def solution(mesh):
    n = mesh.shape["dp"]
    dims = (8, 4, 4) if n == 256 else (4, 2, 2)
    return jax.shard_map(build(*dims), mesh=mesh,
                         in_specs=(P("dp", None), P("dp", None), P("dp"), P(), P(), P(), P()),
                         out_specs=(P(), P(), P(), P(), P()), check_vma=False)
```

```python
import functools

import jax
import jax.numpy as jnp
from jax import lax
from jax.experimental import pallas as pl
from jax.experimental.pallas import tpu as pltpu
from jax.sharding import PartitionSpec as P

f32, bf16 = jnp.float32, jnp.bfloat16
MESH = pl.DeviceIdType.MESH
TEMP = 0.05
EPS = 1e-6
LOG2E = 1.4426950408889634
LN2 = 0.6931471805599453
NT = (((1,), (1,)), ((), ()))
TN = (((0,), (0,)), ((), ()))
NN = (((1,), (0,)), ((), ()))
R = 128
W = 256
GR = 2 * R
ROWS = (256, 512), (384, 384)


class Scope:
    def __init__(self):
        self.cur = None

    def __call__(self, name):
        if self.cur is not None:
            self.cur.__exit__(None, None, None)
        self.cur = None
        if name:
            self.cur = jax.named_scope(name)
            self.cur.__enter__()


def dot(a, b, dims=NN):
    return lax.dot_general(a, b, dims, preferred_element_type=f32)


def arrange(near, level):
    rest = near[level:]
    return near[:level] + rest[level:][::-1] + rest[:level]


def ring(n):
    return sorted(range(n), key=lambda k: (min(k, n - k), k))


def torus(ny, nx):
    def dist(o):
        return min(o[0], ny - o[0]) + min(o[1], nx - o[1])
    return sorted(((a, b) for a in range(ny) for b in range(nx)), key=lambda o: (dist(o), o[0] * o[1] != 0, o))


def kernel(NZ, NY, NX, qf_h, vf_h, lq_h, wqi_h, wqo_h, wvi_h, wvo_h, fin, loss_o,
           qf, vf, lq, wqi, wqo, wvi, wvo, s_in,
           u4, v_all, vt, lq_all, mslot, wslot, cnt, bcol, sbuf, e_all, g_all, csum, stats, invl, invt,
           up, ui, uh, ua, vp, vi, vh, va,
           su, ru, hop_in, sv, rv, v2, b2, w2, e2, g2, il4, gl, gpair, gx_s, gx_r, gz_r, loss_p, loss_x,
           s_u, r_u, s_v, r_v, s_lq, s_st, r_st, s_sv, r_sv, s_u2, r_u2, s_il, r_il, s_su, r_su, r_hop,
           s_gp, r_gp, s_gx, r_gx, s_gz, r_gz, s_ag, r_ag, s_rl, r_rl, s_lp, r_lp, s_lx, r_lx, s_vr):
    sc = Scope()
    NXY = NY * NX
    NQ = NZ * R
    NI = 2 * NXY * R
    B = NZ * NI
    LV = NZ // 2
    SL = NXY // LV
    QC = 2 * R
    IR = 2 * SL * R
    NG = IR // GR
    zoff, xoff = arrange(ring(NZ), 2), arrange(torus(NY, NX), SL)
    zfar = [zoff.index(o) for o in ring(NZ)[:0:-1]]
    xfar = [xoff.index(o) for o in torus(NY, NX)[:0:-1]]
    me = lax.axis_index("dp")
    c = lax.rem(me, 2)
    j = lax.rem(lax.div(me, 2), NXY)
    y, x = lax.div(j, NX), lax.rem(j, NX)
    z = lax.div(me, 2 * NXY)
    oc = 1 - c

    def dev(zz, jj, cc):
        return ((zz * NXY + jj) * 2 + cc,)

    def zs(k, sign):
        o = zoff[k]
        return lax.rem(z + (o if sign > 0 else NZ - o), NZ)

    def xs(k, sign):
        a, b = xoff[k]
        yy = lax.rem(y + (a if sign > 0 else NY - a), NY)
        xx = lax.rem(x + (b if sign > 0 else NX - b), NX)
        return yy * NX + xx

    def ax(a, o):
        return lax.rem(y + o * (1 - a), NY) * NX + lax.rem(x + o * a, NX)

    def slot(k, core):
        return (k // SL) * 2 * SL + core * SL + k % SL

    def send(src, dst, ss, rs, to):
        pltpu.make_async_remote_copy(src_ref=src, dst_ref=dst, send_sem=ss, recv_sem=rs,
                                     device_id=to, device_id_type=MESH).start()

    def wait(ref, sem):
        pltpu.make_async_copy(ref, ref, sem).wait()

    def vrows(s):
        return v_all.at[pl.ds(s * R, R), :]

    sc("barsig")
    bar = pltpu.get_barrier_semaphore()
    peers = [dev(zs(k, 1), j, c) for k in range(1, NZ)]
    peers += [dev(z, xs(k, 1), c) for k in range(1, NXY)]
    peers += [dev(z, j, oc)]
    peers += [dev(z, ax(a, o), oc) for a in (0, 1) for o in range(1, NX)]
    for p in peers:
        pl.semaphore_signal(bar, inc=1, device_id=p, device_id_type=MESH)
    loads = [pltpu.make_async_copy(a, b, s_in.at[i]) for i, (a, b) in enumerate(
        ((vf_h, vf), (wvi_h, wvi), (wvo_h, wvo), (lq_h, lq), (qf_h, qf), (wqi_h, wqi), (wqo_h, wqo)))]
    for cp in loads:
        cp.start()

    def tower(xr, wi, wo, unit, inv, hid, act, cps):
        cps[0].wait()
        cps[1].wait()
        a = dot(xr[...], wi[...])
        h = jnp.maximum(a, 0.0).astype(bf16)
        cps[2].wait()
        e = dot(h, wo[...])
        r = lax.rsqrt(jnp.sum(e * e, axis=-1, keepdims=True) + EPS)
        u = e * r
        unit[...] = u
        inv[...] = jnp.broadcast_to(r, (R, R))
        hid[...] = h
        act[...] = a
        return u.astype(bf16)

    def send_item(s, s2, ss, to):
        send(lq_all.at[s], lq_all.at[s2], s_lq, r_v.at[s2], to)
        send(vrows(s), vrows(s2), ss, r_v.at[s2], to)

    sc("tower_v")
    v_bf = tower(vf, wvi, wvo, vp, vi, vh, va, loads[0:3])
    v_all[0:R, :] = v_bf
    loads[3].wait()
    lq_all[0] = lq[...]
    sc("barwait")
    pl.semaphore_wait(bar, len(peers))
    sc("sends_v")
    for k in range(1, NXY):
        send_item(0, slot(k, 0), s_v, dev(z, xs(k, 1), c))
    send_item(0, slot(0, 1), s_vr, dev(z, j, oc))
    sc("tower_q")
    u_bf = tower(qf, wqi, wqo, up, ui, uh, ua, loads[4:7])
    u4[0:R, :] = u_bf
    for k in range(1, NZ):
        send(u4.at[pl.ds(0, R), :], u4.at[pl.ds(k * R, R), :], s_u, r_u.at[k], dev(zs(k, 1), j, c))
    pos = jnp.sum(u_bf.astype(f32) * v_bf.astype(f32), axis=0, keepdims=True) * (1.0 / TEMP) - lq[...]
    stats[z, :, pl.ds(NQ + R, R)] = pos

    def grp(g):
        return slice(g * GR, (g + 1) * GR)

    def qcols(l):
        return slice(l * QC, (l + 1) * QC)

    def bias(s0):
        q = lq_all[s0:s0 + SL].reshape(SL, R)
        big = jnp.max(-q, axis=1, keepdims=True)
        b = (big + q) * LOG2E
        bt = jnp.transpose(jnp.concatenate([b] * (8 // SL), axis=0))
        for i in range(SL):
            mslot[s0 + i] = jnp.broadcast_to(big[i:i + 1, :], (1, R))
            bcol[(s0 + i) * R:(s0 + i + 1) * R, :] = jnp.broadcast_to(bt[:, i:i + 1], (R, R))

    def expo(n, g, l):
        rows, cols = grp(g), qcols(l)
        bb = bcol[rows, :]
        e = jnp.exp2(sbuf[n % 2] * (LOG2E / TEMP) - jnp.concatenate([bb, bb], axis=1))
        e_all[rows, cols] = e
        csum[2 * g:2 * g + 2, :, cols] = jnp.sum(e.reshape(2, R // 8, 8, QC), axis=1)

    def groups(l, core):
        return [l * NG + core * (NG // 2) + t for t in range(NG // 2)]

    done = []
    for l in range(LV + 1):
        sc(f"wait{l}")
        fresh = []
        if l < LV:
            for k in range(l * SL, (l + 1) * SL):
                if k:
                    wait(cnt, r_v.at[slot(k, 0)])
                    send_item(slot(k, 0), slot(k, 1), s_vr, dev(z, j, oc))
            for k in (2 * l, 2 * l + 1):
                if k:
                    wait(u4.at[pl.ds(k * R, R), :], r_u.at[k])
            if l >= LV - 2:
                r0, nr = (0, (LV - 1) * QC) if l == LV - 2 else ((LV - 1) * QC, QC)
                for b in ring(NX)[1:]:
                    send(u4.at[pl.ds(r0, nr), :], u4.at[pl.ds(b * NQ + r0, nr), :], s_u2, r_u2.at[b], dev(z, ax(1 - c, b), c))
            fresh += groups(l, 0)
        if l:
            for k in range((l - 1) * SL, l * SL):
                wait(cnt, r_v.at[slot(k, 1)])
            fresh += groups(l - 1, 1)
        sc(f"pass1_{l}")
        if l < LV:
            bias(slot(l * SL, 0))
        if l:
            bias(slot((l - 1) * SL, 1))
        tasks = [(g, l2) for g in fresh for l2 in range(min(l, LV - 1) + 1)]
        if l < LV:
            old = [g for g in range(LV * NG) if g in done]
            tasks = [(g, l) for g in old] + tasks
        done += fresh
        for n, (g, l2) in enumerate(tasks):
            sbuf[n % 2] = dot(v_all[grp(g), :], u4[qcols(l2), :], NT)
            if n:
                expo(n - 1, *tasks[n - 1])
        expo(len(tasks) - 1, *tasks[-1])

    sc("stats_send")
    big = jnp.max(mslot[...], axis=0)
    stats[z, :, pl.ds(NQ, R)] = big
    wslot[...] = jnp.exp2((mslot[...] - big) * LOG2E)
    for k in range(NZ):
        acc = csum[0, :, k * R:(k + 1) * R] * wslot[0]
        for s in range(1, 2 * NXY):
            acc = acc + csum[s, :, k * R:(k + 1) * R] * wslot[s]
        stats[z, :, pl.ds(pl.multiple_of(zs(k, -1) * R, R), R)] = jnp.sum(acc, axis=0, keepdims=True)
    for k in zfar:
        send(stats.at[z], stats.at[z], s_st, r_st, dev(zs(k, 1), j, c))
    sc("transpose")
    for g in range(LV * NG):
        vt[:, grp(g)] = jnp.transpose(v_all[grp(g), :].astype(f32)).astype(bf16)
    line = [(a, core) for a in ring(NX)[::-1] for core in (0, 1)]
    at = []
    for i, (a, core) in enumerate(line):
        s0, s1 = (slot(xoff.index(o), core) for o in ((a, 0), (0, a)))
        s = s0 + c * (s1 - s0)
        at.append(s)
        v2[i * R:(i + 1) * R, :] = v_all[pl.ds(s * R, R), :]
        b2[i * R:(i + 1) * R, :] = bcol[pl.ds(s * R, R), :]
        w2[i] = wslot[s]

    def line_exp(bs):
        sc(f"line{bs[0]}")
        for b in bs:
            wait(u4.at[pl.ds(b * NQ, NQ), :], r_u2.at[b])
        tasks = [(g, b, l) for b in bs for g in range(len(line) // 2) for l in range(LV)]

        def fin_exp(n, g, b, l):
            bb = b2[grp(g), :]
            e2[grp(g), (b - 1) * NQ + l * QC:(b - 1) * NQ + (l + 1) * QC] = jnp.exp2(
                sbuf[n % 2] * (LOG2E / TEMP) - jnp.concatenate([bb, bb], axis=1))

        for n, (g, b, l) in enumerate(tasks):
            sbuf[n % 2] = dot(v2[grp(g), :], u4[b * NQ + l * QC:b * NQ + (l + 1) * QC, :], NT)
            if n:
                fin_exp(n - 1, *tasks[n - 1])
        fin_exp(len(tasks) - 1, *tasks[-1])

    near = ring(NX)[1:]
    sc("stats_wait")
    wait(stats.at[pl.ds(0, NZ - 1)], r_st)
    sc("stats_comp")
    ms = [stats[k, :, NQ:NQ + R] for k in range(NZ)]
    mx = functools.reduce(jnp.maximum, ms)
    tot = jnp.zeros((1, NQ), f32)
    for k in range(NZ):
        tot = tot + stats[k, :, 0:NQ] * jnp.concatenate([jnp.exp2((ms[k] - mx) * LOG2E)] * NZ, axis=1)
    invt[...] = jnp.concatenate([jnp.exp2((big - mx) * LOG2E)] * NZ, axis=1) / tot
    for k in range(NZ):
        invl[:, k * R:(k + 1) * R] = invt[:, pl.ds(pl.multiple_of(zs(k, -1) * R, R), R)]
    il4[0] = invl[...]
    for b in ring(NX)[1:]:
        send(il4.at[0], il4.at[b], s_il, r_il.at[b], dev(z, ax(1 - c, b), c))
    lse = jnp.log2(tot) * LN2 + jnp.concatenate([mx] * NZ, axis=1)
    lrow = jnp.zeros((1, R), f32)
    for k in range(NZ):
        lrow = lrow + (lse[:, k * R:(k + 1) * R] - stats[k, :, NQ + R:NQ + W])
    loss_p[c] = lrow
    send(loss_p.at[c], loss_p.at[c], s_lp, r_lp, dev(z, j, oc))

    def norm(g, c0, c1):
        cols = slice(c0 * QC, c1 * QC)
        out = []
        for i in range(2):
            rows = slice(g * GR + i * R, g * GR + (i + 1) * R)
            p = e_all[rows, cols] * (invl[:, cols] * jnp.concatenate([wslot[2 * g + i]] * (2 * (c1 - c0)), axis=1))
            if g == 0 and i == 0 and c0 == 0:
                col = lax.broadcasted_iota(jnp.int32, p.shape, 1)
                p = jnp.where(lax.broadcasted_iota(jnp.int32, p.shape, 0) == col, p - 1.0, p)
            p = p.astype(bf16)
            g_all[rows, cols] = p
            out.append(p)
        return jnp.concatenate(out, axis=0)

    normed = set()

    def ready(g, l):
        if (g, l) not in normed:
            normed.add((g, l))
            norm(g, l, l + 1)

    def line_norm(g, bs):
        for i in (2 * g, 2 * g + 1):
            for b in bs:
                for l in range(LV):
                    cols = slice(l * QC, (l + 1) * QC)
                    f = il4[b, :, cols] * jnp.concatenate([w2[i], w2[i]], axis=1)
                    if b:
                        p = e2[i * R:(i + 1) * R, (b - 1) * NQ + l * QC:(b - 1) * NQ + (l + 1) * QC] * f
                    else:
                        p = e_all[pl.ds(pl.multiple_of(at[i] * R, R), R), cols] * f
                    if line[i] == (0, 0) and b == 0 and l == 0:
                        col = lax.broadcasted_iota(jnp.int32, p.shape, 1)
                        p = jnp.where(lax.broadcasted_iota(jnp.int32, p.shape, 0) == col, p - 1.0, p)
                    g2[i * R:(i + 1) * R, b * NQ + l * QC:b * NQ + (l + 1) * QC] = p.astype(bf16)

    def line_dots(gs, k0, k1):
        if len(gs) > 1:
            ds = [dot(g2[grp(g), k0:k1], u4[k0:k1, :]) for g in gs]
            ds = [d[i * R:(i + 1) * R] for d in ds for i in range(2)]
        else:
            ds = [dot(g2[i * R:(i + 1) * R, k0:k1], u4[k0:k1, :]) for i in (2 * gs[0], 2 * gs[0] + 1)]
        return [i for g in gs for i in (2 * g, 2 * g + 1)], ds

    def line_own():
        sc("ldv_own")
        gs = list(range(len(line) // 2))
        for g in gs:
            line_norm(g, [0])
        for i, d in zip(*line_dots(gs, 0, NQ)):
            sv[i] = d

    def line_dv(gs):
        sc(f"ldv{gs[0]}")
        for g in gs:
            line_norm(g, range(1, NX))
        idx, ds = line_dots(gs, NQ, NX * NQ)
        for i, d in zip(idx, ds):
            a, core = line[i]
            d = sv[i] + d
            if a or core:
                sv[i] = d
            else:
                rv[c * NX] = d
        for i in idx:
            a, core = line[i]
            if a or core:
                send(sv.at[i], rv.at[c * NX + a], s_sv, r_sv, dev(z, ax(c, NX - a), oc if core else c))

    def du_levels(ls):
        sc(f"du{ls[0]}")
        for l in ls:
            parts = []
            for lk in range(LV):
                for g in range(lk * NG, (lk + 1) * NG):
                    ready(g, l)
                rows = slice(lk * IR, (lk + 1) * IR)
                parts.append(dot(vt[:, rows], g_all[rows, qcols(l)]))
            d = functools.reduce(jnp.add, parts)
            for i in range(2):
                su[2 * l + i] = d[:, i * R:(i + 1) * R]
        ks = [k for l in ls for k in (2 * l, 2 * l + 1)]
        for k in ks:
            if k in hop:
                send(su.at[k], hop_in.at[k], s_su, r_hop.at[k], dev(lax.rem(z + NZ - hop[k], NZ), j, c))
        for k in ks:
            if k and k not in hop and k not in late:
                send(su.at[k], ru.at[k], s_su, r_su, dev(zs(k, -1), j, c))

    hop, late = {}, {}
    if NZ >= 8:
        for o, via in ((3, 2), (NZ - 3, NZ - 2)):
            hop[zoff.index(o)] = (o - via) % NZ
            late[zoff.index(via)] = zoff.index(o)

    def send_late(ks):
        sc("late")
        for k in ks:
            k2 = late[k]
            wait(hop_in.at[k2], r_hop.at[k2])
            su[k] = su[k] + hop_in[k2]
            send(su.at[k], ru.at[k], s_su, r_su, dev(zs(k, -1), j, c))

    du_levels([1, 2])
    line_own()
    line_exp(near[:2])
    line_exp(near[2:])
    sc("il_wait")
    for b in near:
        wait(il4.at[b], r_il.at[b])
    line_dv([0])
    line_dv([1, 2])
    du_levels([3, 0])
    send_late([k for k in late if k // 2 == 2])
    line_dv([3])
    send_late([k for k in late if k // 2 != 2])

    sc("loss")
    wait(loss_p.at[oc], r_lp)
    loss_x[j] = loss_p[0] + loss_p[1]
    for k in range(1, NXY):
        send(loss_x.at[j], loss_x.at[j], s_lx, r_lx, dev(z, xs(k, 1), c))

    def per_core(f):
        for core in (0, 1):
            @pl.when(c == core)
            def _():
                f(core)

    def chunk(t, core):
        return ROWS[t][core] // NXY

    def rows_of(t, core, k):
        return pl.ds(pl.multiple_of(k * chunk(t, core), 8), chunk(t, core))

    def backward(du, xr, wo, unit, inv, hid, act, t):
        u, r = unit[...], inv[...]
        de = (r * (du - u * jnp.sum(u * du, axis=-1, keepdims=True))).astype(bf16)
        go = dot(hid[...], de, TN)
        dh = dot(de, wo[...], NT)
        da = jnp.where(act[...] > 0, dh, 0.0).astype(bf16)
        gi = dot(xr[...], da, TN)
        gl[t, 0:W, :] = gi[:, 0:R]
        gl[t, W:512, :] = gi[:, R:W]
        gl[t, 512:768, :] = go

        @per_core
        def _(core):
            o = 1 - core
            send(gl.at[t, pl.ds(o * ROWS[t][0], ROWS[t][o]), :], gpair.at[t, pl.ds(0, ROWS[t][o]), :], s_gp.at[t], r_gp.at[t], dev(z, j, oc))

    def pair_sum(t):
        sc(f"gp_wait{t}")

        @per_core
        def _(core):
            wait(gpair.at[t, pl.ds(0, ROWS[t][core]), :], r_gp.at[t])
            gx_s[t, 0:ROWS[t][core], :] = gl[t, core * ROWS[t][0]:core * ROWS[t][0] + ROWS[t][core], :] + gpair[t, 0:ROWS[t][core], :]
            for k in xfar:
                to = xs(k, 1)
                send(gx_s.at[t, rows_of(t, core, to), :], gx_r.at[t, rows_of(t, core, j), :], s_gx.at[t], r_gx.at[t], dev(z, to, c))
            gx_r[t, rows_of(t, core, j), :] = gx_s[t, rows_of(t, core, j), :]

    def plane_sum(t):
        sc(f"gx_wait{t}")

        @per_core
        def _(core):
            n = chunk(t, core)
            wait(gx_r.at[t, pl.ds(0, (NXY - 1) * n), :], r_gx.at[t])
            acc = gx_r[t, 0:n, :]
            for k in range(1, NXY):
                acc = acc + gx_r[t, k * n:(k + 1) * n, :]
            gz_r[t, rows_of(t, core, z), :] = acc
            for k in zfar:
                send(gz_r.at[t, rows_of(t, core, z), :], gz_r.at[t, rows_of(t, core, z), :], s_gz.at[t], r_gz.at[t], dev(zs(k, 1), j, c))

    def part(t, core, jj):
        return fin.at[t, pl.ds(pl.multiple_of(core * ROWS[t][0] + jj * chunk(t, core), 8), chunk(t, core)), :]

    def ring_sum(t):
        sc(f"gz_wait{t}")

        @per_core
        def _(core):
            n = chunk(t, core)
            wait(gz_r.at[t, pl.ds(0, (NZ - 1) * n), :], r_gz.at[t])
            acc = gz_r[t, 0:n, :]
            for k in range(1, NZ):
                acc = acc + gz_r[t, k * n:(k + 1) * n, :]
            mine = part(t, core, j)
            mine[...] = acc
            for k in xfar:
                send(mine, mine, s_ag.at[t], r_ag.at[t, k], dev(z, xs(k, 1), c))
            send(mine, mine, s_rl.at[t], r_rl.at[t, 0], dev(z, j, oc))

    def relay(t):
        sc(f"ag_wait{t}")

        @per_core
        def _(core):
            for k in xfar:
                ref = part(t, core, xs(k, -1))
                wait(ref, r_ag.at[t, k])
                send(ref, ref, s_rl.at[t], r_rl.at[t, k], dev(z, j, oc))

    scale = 1.0 / (TEMP * B)
    sc("rv_wait")
    wait(rv.at[pl.ds(0, 2 * NX - 1)], r_sv)
    sc("bwd_v")
    acc = rv[0]
    for i in range(1, 2 * NX):
        acc = acc + rv[i]
    backward(acc * scale, vf, wvo, vp, vi, vh, va, 1)
    pair_sum(1)
    sc("ru_wait")
    wait(ru.at[pl.ds(0, NZ - 1 - len(hop))], r_su)
    sc("bwd_q")
    acc = su[0]
    for k in range(1, NZ):
        if k not in hop:
            acc = acc + ru[k]
    backward(jnp.transpose(acc) * scale, qf, wqo, up, ui, uh, ua, 0)
    pair_sum(0)
    sc("loss2")
    wait(loss_x.at[pl.ds(0, NXY - 1)], r_lx)
    ls = loss_x[0]
    for k in range(1, NXY):
        ls = ls + loss_x[k]
    loss_o[...] = jnp.broadcast_to(jnp.sum(ls, axis=-1, keepdims=True) * (1.0 / B), (1, R))
    plane_sum(1)
    plane_sum(0)
    ring_sum(1)
    ring_sum(0)
    relay(1)
    relay(0)
    sc("rl_wait")

    @per_core
    def _(core):
        for t in range(2):
            for k in range(NXY):
                wait(part(t, 1 - core, xs(k, -1)), r_rl.at[t, k])

    sc("sendwait")
    wait(lq_all.at[pl.ds(0, 2 * NXY - 1)], s_lq)
    wait(u4.at[pl.ds(0, (NZ - 1) * R), :], s_u)
    wait(v_all.at[pl.ds(0, (NXY - 1) * R), :], s_v)
    wait(v_all.at[pl.ds(0, NXY * R), :], s_vr)
    wait(stats.at[pl.ds(0, NZ - 1)], s_st)
    wait(loss_p.at[0], s_lp)
    wait(sv.at[pl.ds(0, 2 * NX - 1)], s_sv)
    wait(u4.at[pl.ds(NQ, (NX - 1) * NQ), :], s_u2)
    wait(il4.at[pl.ds(1, NX - 1)], s_il)
    wait(su.at[pl.ds(0, NZ - 1)], s_su)
    wait(loss_x.at[pl.ds(0, NXY - 1)], s_lx)

    @per_core
    def _(core):
        for t in range(2):
            n = chunk(t, core)
            wait(gpair.at[t, pl.ds(0, ROWS[t][1 - core]), :], s_gp.at[t])
            wait(gx_s.at[t, pl.ds(0, (NXY - 1) * n), :], s_gx.at[t])
            wait(gz_r.at[t, pl.ds(0, (NZ - 1) * n), :], s_gz.at[t])
            wait(gx_s.at[t, pl.ds(0, (NXY - 1) * n), :], s_ag.at[t])
            wait(gx_s.at[t, pl.ds(0, NXY * n), :], s_rl.at[t])

    sc(None)


def emit(fin, loss, gqi, gqo, gvi, gvo, loss_o, sem):
    copies = [(loss, loss_o)]
    for t, (gi, go) in enumerate(((gqi, gqo), (gvi, gvo))):
        copies += [(fin.at[t, 0:W, :], gi.at[:, 0:R]), (fin.at[t, W:512, :], gi.at[:, R:W]), (fin.at[t, 512:768, :], go)]
    copies = [pltpu.make_async_copy(a, b, sem.at[i]) for i, (a, b) in enumerate(copies)]
    for cp in copies:
        cp.start()
    for cp in copies:
        cp.wait()


def build(NZ, NY, NX):
    def step(query_feat, item_feat, log_q, w_query_in, w_query_out, w_item_in, w_item_out):
        NXY = NY * NX
        NQ, NI = NZ * R, 2 * NXY * R
        V, S = pltpu.VMEM, pltpu.SemaphoreType.DMA
        vm, hbm = pl.BlockSpec(memory_space=pltpu.VMEM), pl.BlockSpec(memory_space=pl.ANY)
        sd = jax.ShapeDtypeStruct
        tower = [V((R, R), f32), V((R, R), f32), V((R, W), bf16), V((R, W), f32)]
        fin, loss = pl.pallas_call(
            functools.partial(kernel, NZ, NY, NX),
            name="two_tower",
            out_shape=[pltpu.VMEM((2, 768, R), f32), pltpu.VMEM((1, R), f32)],
            in_specs=[hbm] * 7,
            out_specs=[vm] * 2,
            scratch_shapes=[
                V((R, W), bf16), V((R, W), bf16), V((1, R), f32),
                V((W, W), bf16), V((W, R), bf16), V((W, W), bf16), V((W, R), bf16), S((7,)),
                V((NX * NQ, R), bf16), V((NI, R), bf16), V((R, NI), bf16), V((2 * NXY, 1, R), f32), V((2 * NXY, 1, R), f32), V((2 * NXY, 1, R), f32), V((65, 1, R), f32),
                V((NI, R), f32), V((2, GR, 2 * R), f32), V((NI, NQ), f32), V((NI, NQ), bf16), V((2 * NXY, 8, NQ), f32),
                V((NZ, 1, NQ + W), f32), V((1, NQ), f32), V((1, NQ), f32),
                *tower, *tower,
                V((NZ, R, R), f32), V((NZ, R, R), f32), V((NZ, R, R), f32),
                V((2 * NX, R, R), f32), V((2 * NX, R, R), f32),
                V((2 * NX * R, R), bf16), V((2 * NX * R, R), f32), V((2 * NX, 1, R), f32),
                V((2 * NX * R, (NX - 1) * NQ), f32), V((2 * NX * R, NX * NQ), bf16), V((NX, 1, NQ), f32),
                V((2, 768, R), f32), V((2, max(map(max, ROWS)), R), f32), V((2, max(map(max, ROWS)), R), f32), V((2, max(map(max, ROWS)), R), f32),
                V((2, NZ * max(map(max, ROWS)) // NXY, R), f32), V((2, 1, R), f32), V((NXY, 1, R), f32),
                S, S((NZ,)), S, S((2 * NXY,)), S, S, S, S, S, S, S((NX,)), S, S((NX,)), S, S, S((NZ,)),
                S((2,)), S((2,)), S((2,)), S((2,)), S((2,)), S((2,)), S((2,)), S((2, NXY)), S((2,)), S((2, NXY)),
                S, S, S, S, S,
            ],
            compiler_params=pltpu.CompilerParams(collective_id=0, has_side_effects=True, vmem_limit_bytes=60 * 2**20),
        )(query_feat, item_feat, log_q.reshape(1, R), w_query_in, w_query_out, w_item_in, w_item_out)
        gqi, gqo, gvi, gvo, out = pl.pallas_call(
            emit,
            name="emit",
            out_shape=[sd((W, W), f32), sd((W, R), f32), sd((W, W), f32), sd((W, R), f32), sd((1, R), f32)],
            in_specs=[vm] * 2,
            out_specs=[hbm] * 5,
            scratch_shapes=[S((7,))],
        )(pltpu.with_memory_space_constraint(fin, pltpu.VMEM), pltpu.with_memory_space_constraint(loss, pltpu.VMEM))
        return out[0, 0:1], gqi, gqo, gvi, gvo
    return step


def solution(mesh):
    return jax.shard_map(build(8, 4, 4), mesh=mesh,
                         in_specs=(P("dp", None), P("dp", None), P("dp"), P(), P(), P(), P()),
                         out_specs=(P(), P(), P(), P(), P()), check_vma=False)
```

```python
import functools

import jax
import jax.numpy as jnp
from jax import lax
from jax.experimental import pallas as pl
from jax.experimental.pallas import tpu as pltpu
from jax.sharding import PartitionSpec as P

f32, bf16 = jnp.float32, jnp.bfloat16
MESH = pl.DeviceIdType.MESH
TEMP = 0.05
EPS = 1e-6
LOG2E = 1.4426950408889634
LN2 = 0.6931471805599453
NT = (((1,), (1,)), ((), ()))
TN = (((0,), (0,)), ((), ()))
NN = (((1,), (0,)), ((), ()))
R = 128
W = 256
GR = 2 * R
ROWS = (256, 512), (384, 384)


class Scope:
    def __init__(self):
        self.cur = None

    def __call__(self, name):
        if self.cur is not None:
            self.cur.__exit__(None, None, None)
        self.cur = None
        if name:
            self.cur = jax.named_scope(name)
            self.cur.__enter__()


def dot(a, b, dims=NN):
    return lax.dot_general(a, b, dims, preferred_element_type=f32)


def arrange(near, level):
    rest = near[level:]
    return near[:level] + rest[level:][::-1] + rest[:level]


def ring(n):
    return sorted(range(n), key=lambda k: (min(k, n - k), k))


def torus(ny, nx):
    def dist(o):
        return min(o[0], ny - o[0]) + min(o[1], nx - o[1])
    return sorted(((a, b) for a in range(ny) for b in range(nx)), key=lambda o: (dist(o), o[0] * o[1] != 0, o))


def kernel(NZ, NY, NX, qf_h, vf_h, lq_h, wqi_h, wqo_h, wvi_h, wvo_h, fin, loss_o,
           qf, vf, lq, wqi, wqo, wvi, wvo, s_in,
           u4, v_all, vt, lq_all, mslot, wslot, cnt, bcol, sbuf, e_all, g_all, csum, stats, invl, invt,
           up, ui, uh, ua, vp, vi, vh, va,
           su, ru, hop_in, sv, rv, v2, b2, w2, e2, g2, il4, gl, gpair, gx_s, gx_r, gz_r, loss_p, loss_x,
           s_u, r_u, s_v, r_v, s_lq, s_st, r_st, s_sv, r_sv, s_u2, r_u2, s_il, r_il, s_su, r_su, r_hop,
           s_gp, r_gp, s_gx, r_gx, s_gz, r_gz, s_ag, r_ag, s_rl, r_rl, s_lp, r_lp, s_lx, r_lx, s_vr, order):
    sc = Scope()
    NXY = NY * NX
    NQ = NZ * R
    NI = 2 * NXY * R
    B = NZ * NI
    LV = NZ // 2
    SL = NXY // LV
    QC = 2 * R
    IR = 2 * SL * R
    NG = IR // GR
    zoff, xoff = arrange(ring(NZ), 2), arrange(torus(NY, NX), SL)
    zfar = [zoff.index(o) for o in ring(NZ)[:0:-1]]
    xfar = [xoff.index(o) for o in torus(NY, NX)[:0:-1]]
    me = lax.axis_index("dp")
    c = lax.rem(me, 2)
    j = lax.rem(lax.div(me, 2), NXY)
    y, x = lax.div(j, NX), lax.rem(j, NX)
    z = lax.div(me, 2 * NXY)
    oc = 1 - c

    def dev(zz, jj, cc):
        return ((zz * NXY + jj) * 2 + cc,)

    def zs(k, sign):
        o = zoff[k]
        return lax.rem(z + (o if sign > 0 else NZ - o), NZ)

    def xs(k, sign):
        a, b = xoff[k]
        yy = lax.rem(y + (a if sign > 0 else NY - a), NY)
        xx = lax.rem(x + (b if sign > 0 else NX - b), NX)
        return yy * NX + xx

    def ax(a, o):
        return lax.rem(y + o * (1 - a), NY) * NX + lax.rem(x + o * a, NX)

    def slot(k, core):
        return (k // SL) * 2 * SL + core * SL + k % SL

    def send(src, dst, ss, rs, to):
        pltpu.make_async_remote_copy(src_ref=src, dst_ref=dst, send_sem=ss, recv_sem=rs,
                                     device_id=to, device_id_type=MESH).start()

    def wait(ref, sem):
        pltpu.make_async_copy(ref, ref, sem).wait()

    def fence():
        pl.semaphore_signal(order, inc=1)
        pl.semaphore_wait(order, 1)

    def vrows(s):
        return v_all.at[pl.ds(s * R, R), :]

    sc("barsig")
    bar = pltpu.get_barrier_semaphore()
    peers = [dev(zs(k, 1), j, c) for k in range(1, NZ)]
    peers += [dev(z, xs(k, 1), c) for k in range(1, NXY)]
    peers += [dev(z, j, oc)]
    peers += [dev(z, ax(a, o), oc) for a in (0, 1) for o in range(1, NX)]
    for p in peers:
        pl.semaphore_signal(bar, inc=1, device_id=p, device_id_type=MESH)
    loads = [pltpu.make_async_copy(a, b, s_in.at[i]) for i, (a, b) in enumerate(
        ((vf_h, vf), (wvi_h, wvi), (wvo_h, wvo), (lq_h, lq), (qf_h, qf), (wqi_h, wqi), (wqo_h, wqo)))]
    for cp in loads:
        cp.start()

    def tower(xr, wi, wo, unit, inv, hid, act, cps):
        cps[0].wait()
        cps[1].wait()
        a = dot(xr[...], wi[...])
        h = jnp.maximum(a, 0.0).astype(bf16)
        cps[2].wait()
        e = dot(h, wo[...])
        r = lax.rsqrt(jnp.sum(e * e, axis=-1, keepdims=True) + EPS)
        u = e * r
        unit[...] = u
        inv[...] = jnp.broadcast_to(r, (R, R))
        hid[...] = h
        act[...] = a
        return u.astype(bf16)

    def send_item(s, s2, ss, to):
        send(lq_all.at[s], lq_all.at[s2], s_lq, r_v.at[s2], to)
        send(vrows(s), vrows(s2), ss, r_v.at[s2], to)

    sc("tower_v")
    v_bf = tower(vf, wvi, wvo, vp, vi, vh, va, loads[0:3])
    v_all[0:R, :] = v_bf
    loads[3].wait()
    lq_all[0] = lq[...]
    sc("barwait")
    pl.semaphore_wait(bar, len(peers))
    sc("sends_v")
    for k in range(1, NXY):
        send_item(0, slot(k, 0), s_v, dev(z, xs(k, 1), c))
    send_item(0, slot(0, 1), s_vr, dev(z, j, oc))
    sc("tower_q")
    u_bf = tower(qf, wqi, wqo, up, ui, uh, ua, loads[4:7])
    u4[0:R, :] = u_bf
    for k in range(1, NZ):
        send(u4.at[pl.ds(0, R), :], u4.at[pl.ds(k * R, R), :], s_u, r_u.at[k], dev(zs(k, 1), j, c))
    pos = jnp.sum(u_bf.astype(f32) * v_bf.astype(f32), axis=0, keepdims=True) * (1.0 / TEMP) - lq[...]
    stats[z, :, pl.ds(NQ + R, R)] = pos

    def grp(g):
        return slice(g * GR, (g + 1) * GR)

    def qcols(l):
        return slice(l * QC, (l + 1) * QC)

    def bias(s0):
        q = lq_all[s0:s0 + SL].reshape(SL, R)
        big = jnp.max(-q, axis=1, keepdims=True)
        b = (big + q) * LOG2E
        bt = jnp.transpose(jnp.concatenate([b] * (8 // SL), axis=0))
        for i in range(SL):
            mslot[s0 + i] = jnp.broadcast_to(big[i:i + 1, :], (1, R))
            bcol[(s0 + i) * R:(s0 + i + 1) * R, :] = jnp.broadcast_to(bt[:, i:i + 1], (R, R))

    def expo(n, g, l):
        rows, cols = grp(g), qcols(l)
        bb = bcol[rows, :]
        e = jnp.exp2(sbuf[n % 2] * (LOG2E / TEMP) - jnp.concatenate([bb, bb], axis=1))
        e_all[rows, cols] = e
        csum[2 * g:2 * g + 2, :, cols] = jnp.sum(e.reshape(2, R // 8, 8, QC), axis=1)

    def groups(l, core):
        return [l * NG + core * (NG // 2) + t for t in range(NG // 2)]

    done = []
    for l in range(LV + 1):
        sc(f"wait{l}")
        fresh = []
        if l < LV:
            for k in range(l * SL, (l + 1) * SL):
                if k:
                    wait(cnt, r_v.at[slot(k, 0)])
                    send_item(slot(k, 0), slot(k, 1), s_vr, dev(z, j, oc))
            for k in (2 * l, 2 * l + 1):
                if k:
                    wait(u4.at[pl.ds(k * R, R), :], r_u.at[k])
            if l >= LV - 2:
                r0, nr = (0, (LV - 1) * QC) if l == LV - 2 else ((LV - 1) * QC, QC)
                for b in ring(NX)[1:]:
                    send(u4.at[pl.ds(r0, nr), :], u4.at[pl.ds(b * NQ + r0, nr), :], s_u2, r_u2.at[b], dev(z, ax(1 - c, b), c))
            fresh += groups(l, 0)
        if l:
            for k in range((l - 1) * SL, l * SL):
                wait(cnt, r_v.at[slot(k, 1)])
            fresh += groups(l - 1, 1)
        sc(f"pass1_{l}")
        if l < LV:
            bias(slot(l * SL, 0))
        if l:
            bias(slot((l - 1) * SL, 1))
        tasks = [(g, l2) for g in fresh for l2 in range(min(l, LV - 1) + 1)]
        if l < LV:
            old = [g for g in range(LV * NG) if g in done]
            tasks = [(g, l) for g in old] + tasks
        done += fresh
        for n, (g, l2) in enumerate(tasks):
            sbuf[n % 2] = dot(v_all[grp(g), :], u4[qcols(l2), :], NT)
            if n:
                expo(n - 1, *tasks[n - 1])
        expo(len(tasks) - 1, *tasks[-1])

    sc("stats_send")
    big = jnp.max(mslot[...], axis=0)
    stats[z, :, pl.ds(NQ, R)] = big
    wslot[...] = jnp.exp2((mslot[...] - big) * LOG2E)
    for k in range(NZ):
        acc = csum[0, :, k * R:(k + 1) * R] * wslot[0]
        for s in range(1, 2 * NXY):
            acc = acc + csum[s, :, k * R:(k + 1) * R] * wslot[s]
        stats[z, :, pl.ds(pl.multiple_of(zs(k, -1) * R, R), R)] = jnp.sum(acc, axis=0, keepdims=True)
    for k in zfar:
        send(stats.at[z], stats.at[z], s_st, r_st, dev(zs(k, 1), j, c))
    fence()
    sc("transpose")
    for g in range(LV * NG):
        vt[:, grp(g)] = jnp.transpose(v_all[grp(g), :].astype(f32)).astype(bf16)
    line = [(a, core) for a in ring(NX)[::-1] for core in (0, 1)]
    at = []
    for i, (a, core) in enumerate(line):
        s0, s1 = (slot(xoff.index(o), core) for o in ((a, 0), (0, a)))
        s = s0 + c * (s1 - s0)
        at.append(s)
        v2[i * R:(i + 1) * R, :] = v_all[pl.ds(s * R, R), :]
        b2[i * R:(i + 1) * R, :] = bcol[pl.ds(s * R, R), :]
        w2[i] = wslot[s]

    def line_exp(bs):
        sc(f"line{bs[0]}")
        for b in bs:
            wait(u4.at[pl.ds(b * NQ, NQ), :], r_u2.at[b])
        tasks = [(g, b, l) for b in bs for g in range(len(line) // 2) for l in range(LV)]

        def fin_exp(n, g, b, l):
            bb = b2[grp(g), :]
            e2[grp(g), (b - 1) * NQ + l * QC:(b - 1) * NQ + (l + 1) * QC] = jnp.exp2(
                sbuf[n % 2] * (LOG2E / TEMP) - jnp.concatenate([bb, bb], axis=1))

        for n, (g, b, l) in enumerate(tasks):
            sbuf[n % 2] = dot(v2[grp(g), :], u4[b * NQ + l * QC:b * NQ + (l + 1) * QC, :], NT)
            if n:
                fin_exp(n - 1, *tasks[n - 1])
        fin_exp(len(tasks) - 1, *tasks[-1])

    near = ring(NX)[1:]
    sc("stats_wait")
    wait(stats.at[pl.ds(0, NZ - 1)], r_st)
    sc("stats_comp")
    ms = [stats[k, :, NQ:NQ + R] for k in range(NZ)]
    mx = functools.reduce(jnp.maximum, ms)
    tot = jnp.zeros((1, NQ), f32)
    for k in range(NZ):
        tot = tot + stats[k, :, 0:NQ] * jnp.concatenate([jnp.exp2((ms[k] - mx) * LOG2E)] * NZ, axis=1)
    invt[...] = jnp.concatenate([jnp.exp2((big - mx) * LOG2E)] * NZ, axis=1) / tot
    for k in range(NZ):
        invl[:, k * R:(k + 1) * R] = invt[:, pl.ds(pl.multiple_of(zs(k, -1) * R, R), R)]
    il4[0] = invl[...]
    for b in ring(NX)[1:]:
        send(il4.at[0], il4.at[b], s_il, r_il.at[b], dev(z, ax(1 - c, b), c))
    fence()
    lse = jnp.log2(tot) * LN2 + jnp.concatenate([mx] * NZ, axis=1)
    lrow = jnp.zeros((1, R), f32)
    for k in range(NZ):
        lrow = lrow + (lse[:, k * R:(k + 1) * R] - stats[k, :, NQ + R:NQ + W])
    loss_p[c] = lrow
    send(loss_p.at[c], loss_p.at[c], s_lp, r_lp, dev(z, j, oc))

    def norm(g, c0, c1):
        cols = slice(c0 * QC, c1 * QC)
        out = []
        for i in range(2):
            rows = slice(g * GR + i * R, g * GR + (i + 1) * R)
            p = e_all[rows, cols] * (invl[:, cols] * jnp.concatenate([wslot[2 * g + i]] * (2 * (c1 - c0)), axis=1))
            if g == 0 and i == 0 and c0 == 0:
                col = lax.broadcasted_iota(jnp.int32, p.shape, 1)
                p = jnp.where(lax.broadcasted_iota(jnp.int32, p.shape, 0) == col, p - 1.0, p)
            p = p.astype(bf16)
            g_all[rows, cols] = p
            out.append(p)
        return jnp.concatenate(out, axis=0)

    normed = set()

    def ready(g, l):
        if (g, l) not in normed:
            normed.add((g, l))
            norm(g, l, l + 1)

    def line_norm(g, bs):
        for i in (2 * g, 2 * g + 1):
            for b in bs:
                for l in range(LV):
                    cols = slice(l * QC, (l + 1) * QC)
                    f = il4[b, :, cols] * jnp.concatenate([w2[i], w2[i]], axis=1)
                    if b:
                        p = e2[i * R:(i + 1) * R, (b - 1) * NQ + l * QC:(b - 1) * NQ + (l + 1) * QC] * f
                    else:
                        p = e_all[pl.ds(pl.multiple_of(at[i] * R, R), R), cols] * f
                    if line[i] == (0, 0) and b == 0 and l == 0:
                        col = lax.broadcasted_iota(jnp.int32, p.shape, 1)
                        p = jnp.where(lax.broadcasted_iota(jnp.int32, p.shape, 0) == col, p - 1.0, p)
                    g2[i * R:(i + 1) * R, b * NQ + l * QC:b * NQ + (l + 1) * QC] = p.astype(bf16)

    def line_dots(gs, k0, k1):
        if len(gs) > 1:
            ds = [dot(g2[grp(g), k0:k1], u4[k0:k1, :]) for g in gs]
            ds = [d[i * R:(i + 1) * R] for d in ds for i in range(2)]
        else:
            ds = [dot(g2[i * R:(i + 1) * R, k0:k1], u4[k0:k1, :]) for i in (2 * gs[0], 2 * gs[0] + 1)]
        return [i for g in gs for i in (2 * g, 2 * g + 1)], ds

    def line_own():
        sc("ldv_own")
        gs = list(range(len(line) // 2))
        for g in gs:
            line_norm(g, [0])
        for i, d in zip(*line_dots(gs, 0, NQ)):
            sv[i] = d

    def line_dv(gs):
        sc(f"ldv{gs[0]}")
        for g in gs:
            line_norm(g, range(1, NX))
        idx, ds = line_dots(gs, NQ, NX * NQ)
        for i, d in zip(idx, ds):
            a, core = line[i]
            d = sv[i] + d
            if a or core:
                sv[i] = d
            else:
                rv[c * NX] = d
        for i in idx:
            a, core = line[i]
            if a or core:
                send(sv.at[i], rv.at[c * NX + a], s_sv, r_sv, dev(z, ax(c, NX - a), oc if core else c))

    def du_levels(ls):
        sc(f"du{ls[0]}")
        for l in ls:
            parts = []
            for lk in range(LV):
                for g in range(lk * NG, (lk + 1) * NG):
                    ready(g, l)
                rows = slice(lk * IR, (lk + 1) * IR)
                parts.append(dot(vt[:, rows], g_all[rows, qcols(l)]))
            d = functools.reduce(jnp.add, parts)
            for i in range(2):
                su[2 * l + i] = d[:, i * R:(i + 1) * R]
        ks = [k for l in ls for k in (2 * l, 2 * l + 1)]
        for k in ks:
            if k in hop:
                send(su.at[k], hop_in.at[k], s_su, r_hop.at[k], dev(lax.rem(z + NZ - hop[k], NZ), j, c))
        for k in ks:
            if k and k not in hop and k not in late:
                send(su.at[k], ru.at[k], s_su, r_su, dev(zs(k, -1), j, c))

    hop, late = {}, {}
    if NZ >= 8:
        for o, via in ((3, 2), (NZ - 3, NZ - 2)):
            hop[zoff.index(o)] = (o - via) % NZ
            late[zoff.index(via)] = zoff.index(o)

    def send_late(ks):
        sc("late")
        for k in ks:
            k2 = late[k]
            wait(hop_in.at[k2], r_hop.at[k2])
            su[k] = su[k] + hop_in[k2]
            send(su.at[k], ru.at[k], s_su, r_su, dev(zs(k, -1), j, c))

    du_levels([1, 2])
    fence()
    line_own()
    fence()
    line_exp(near[:2])
    fence()
    line_exp(near[2:])
    fence()
    sc("il_wait")
    for b in near:
        wait(il4.at[b], r_il.at[b])
    line_dv([0])
    fence()
    line_dv([1, 2])
    fence()
    du_levels([3, 0])
    fence()
    send_late([k for k in late if k // 2 == 2])
    line_dv([3])
    fence()
    send_late([k for k in late if k // 2 != 2])

    sc("loss")
    wait(loss_p.at[oc], r_lp)
    loss_x[j] = loss_p[0] + loss_p[1]
    for k in range(1, NXY):
        send(loss_x.at[j], loss_x.at[j], s_lx, r_lx, dev(z, xs(k, 1), c))

    def per_core(f):
        for core in (0, 1):
            @pl.when(c == core)
            def _():
                f(core)

    def chunk(t, core):
        return ROWS[t][core] // NXY

    def rows_of(t, core, k):
        return pl.ds(pl.multiple_of(k * chunk(t, core), 8), chunk(t, core))

    def backward(du, xr, wo, unit, inv, hid, act, t):
        u, r = unit[...], inv[...]
        de = (r * (du - u * jnp.sum(u * du, axis=-1, keepdims=True))).astype(bf16)
        go = dot(hid[...], de, TN)
        dh = dot(de, wo[...], NT)
        da = jnp.where(act[...] > 0, dh, 0.0).astype(bf16)
        gi = dot(xr[...], da, TN)
        gl[t, 0:W, :] = gi[:, 0:R]
        gl[t, W:512, :] = gi[:, R:W]
        gl[t, 512:768, :] = go

        @per_core
        def _(core):
            o = 1 - core
            send(gl.at[t, pl.ds(o * ROWS[t][0], ROWS[t][o]), :], gpair.at[t, pl.ds(0, ROWS[t][o]), :], s_gp.at[t], r_gp.at[t], dev(z, j, oc))

    def pair_sum(t):
        sc(f"gp_wait{t}")

        @per_core
        def _(core):
            wait(gpair.at[t, pl.ds(0, ROWS[t][core]), :], r_gp.at[t])
            gx_s[t, 0:ROWS[t][core], :] = gl[t, core * ROWS[t][0]:core * ROWS[t][0] + ROWS[t][core], :] + gpair[t, 0:ROWS[t][core], :]
            for k in xfar:
                to = xs(k, 1)
                send(gx_s.at[t, rows_of(t, core, to), :], gx_r.at[t, rows_of(t, core, j), :], s_gx.at[t], r_gx.at[t], dev(z, to, c))
            gx_r[t, rows_of(t, core, j), :] = gx_s[t, rows_of(t, core, j), :]

    def plane_sum(t):
        sc(f"gx_wait{t}")

        @per_core
        def _(core):
            n = chunk(t, core)
            wait(gx_r.at[t, pl.ds(0, (NXY - 1) * n), :], r_gx.at[t])
            acc = gx_r[t, 0:n, :]
            for k in range(1, NXY):
                acc = acc + gx_r[t, k * n:(k + 1) * n, :]
            gz_r[t, rows_of(t, core, z), :] = acc
            for k in zfar:
                send(gz_r.at[t, rows_of(t, core, z), :], gz_r.at[t, rows_of(t, core, z), :], s_gz.at[t], r_gz.at[t], dev(zs(k, 1), j, c))

    def part(t, core, jj):
        return fin.at[t, pl.ds(pl.multiple_of(core * ROWS[t][0] + jj * chunk(t, core), 8), chunk(t, core)), :]

    def ring_sum(t):
        sc(f"gz_wait{t}")

        @per_core
        def _(core):
            n = chunk(t, core)
            wait(gz_r.at[t, pl.ds(0, (NZ - 1) * n), :], r_gz.at[t])
            acc = gz_r[t, 0:n, :]
            for k in range(1, NZ):
                acc = acc + gz_r[t, k * n:(k + 1) * n, :]
            mine = part(t, core, j)
            mine[...] = acc
            for k in xfar:
                send(mine, mine, s_ag.at[t], r_ag.at[t, k], dev(z, xs(k, 1), c))
            send(mine, mine, s_rl.at[t], r_rl.at[t, 0], dev(z, j, oc))

    def relay(t):
        sc(f"ag_wait{t}")

        @per_core
        def _(core):
            for k in xfar:
                ref = part(t, core, xs(k, -1))
                wait(ref, r_ag.at[t, k])
                send(ref, ref, s_rl.at[t], r_rl.at[t, k], dev(z, j, oc))

    scale = 1.0 / (TEMP * B)
    sc("rv_wait")
    wait(rv.at[pl.ds(0, 2 * NX - 1)], r_sv)
    sc("bwd_v")
    acc = rv[0]
    for i in range(1, 2 * NX):
        acc = acc + rv[i]
    backward(acc * scale, vf, wvo, vp, vi, vh, va, 1)
    pair_sum(1)
    sc("ru_wait")
    wait(ru.at[pl.ds(0, NZ - 1 - len(hop))], r_su)
    sc("bwd_q")
    acc = su[0]
    for k in range(1, NZ):
        if k not in hop:
            acc = acc + ru[k]
    backward(jnp.transpose(acc) * scale, qf, wqo, up, ui, uh, ua, 0)
    pair_sum(0)
    sc("loss2")
    wait(loss_x.at[pl.ds(0, NXY - 1)], r_lx)
    ls = loss_x[0]
    for k in range(1, NXY):
        ls = ls + loss_x[k]
    loss_o[...] = jnp.broadcast_to(jnp.sum(ls, axis=-1, keepdims=True) * (1.0 / B), (1, R))
    plane_sum(1)
    plane_sum(0)
    ring_sum(1)
    ring_sum(0)
    relay(1)
    relay(0)
    sc("rl_wait")

    @per_core
    def _(core):
        for t in range(2):
            for k in range(NXY):
                wait(part(t, 1 - core, xs(k, -1)), r_rl.at[t, k])

    sc("sendwait")
    wait(lq_all.at[pl.ds(0, 2 * NXY - 1)], s_lq)
    wait(u4.at[pl.ds(0, (NZ - 1) * R), :], s_u)
    wait(v_all.at[pl.ds(0, (NXY - 1) * R), :], s_v)
    wait(v_all.at[pl.ds(0, NXY * R), :], s_vr)
    wait(stats.at[pl.ds(0, NZ - 1)], s_st)
    wait(loss_p.at[0], s_lp)
    wait(sv.at[pl.ds(0, 2 * NX - 1)], s_sv)
    wait(u4.at[pl.ds(NQ, (NX - 1) * NQ), :], s_u2)
    wait(il4.at[pl.ds(1, NX - 1)], s_il)
    wait(su.at[pl.ds(0, NZ - 1)], s_su)
    wait(loss_x.at[pl.ds(0, NXY - 1)], s_lx)

    @per_core
    def _(core):
        for t in range(2):
            n = chunk(t, core)
            wait(gpair.at[t, pl.ds(0, ROWS[t][1 - core]), :], s_gp.at[t])
            wait(gx_s.at[t, pl.ds(0, (NXY - 1) * n), :], s_gx.at[t])
            wait(gz_r.at[t, pl.ds(0, (NZ - 1) * n), :], s_gz.at[t])
            wait(gx_s.at[t, pl.ds(0, (NXY - 1) * n), :], s_ag.at[t])
            wait(gx_s.at[t, pl.ds(0, NXY * n), :], s_rl.at[t])

    sc(None)


def emit(fin, loss, gqi, gqo, gvi, gvo, loss_o, sem):
    copies = [(loss, loss_o)]
    for t, (gi, go) in enumerate(((gqi, gqo), (gvi, gvo))):
        copies += [(fin.at[t, 0:W, :], gi.at[:, 0:R]), (fin.at[t, W:512, :], gi.at[:, R:W]), (fin.at[t, 512:768, :], go)]
    copies = [pltpu.make_async_copy(a, b, sem.at[i]) for i, (a, b) in enumerate(copies)]
    for cp in copies:
        cp.start()
    for cp in copies:
        cp.wait()


def build(NZ, NY, NX):
    def step(query_feat, item_feat, log_q, w_query_in, w_query_out, w_item_in, w_item_out):
        NXY = NY * NX
        NQ, NI = NZ * R, 2 * NXY * R
        V, S = pltpu.VMEM, pltpu.SemaphoreType.DMA
        vm, hbm = pl.BlockSpec(memory_space=pltpu.VMEM), pl.BlockSpec(memory_space=pl.ANY)
        sd = jax.ShapeDtypeStruct
        tower = [V((R, R), f32), V((R, R), f32), V((R, W), bf16), V((R, W), f32)]
        fin, loss = pl.pallas_call(
            functools.partial(kernel, NZ, NY, NX),
            name="two_tower",
            out_shape=[pltpu.VMEM((2, 768, R), f32), pltpu.VMEM((1, R), f32)],
            in_specs=[hbm] * 7,
            out_specs=[vm] * 2,
            scratch_shapes=[
                V((R, W), bf16), V((R, W), bf16), V((1, R), f32),
                V((W, W), bf16), V((W, R), bf16), V((W, W), bf16), V((W, R), bf16), S((7,)),
                V((NX * NQ, R), bf16), V((NI, R), bf16), V((R, NI), bf16), V((2 * NXY, 1, R), f32), V((2 * NXY, 1, R), f32), V((2 * NXY, 1, R), f32), V((65, 1, R), f32),
                V((NI, R), f32), V((2, GR, 2 * R), f32), V((NI, NQ), f32), V((NI, NQ), bf16), V((2 * NXY, 8, NQ), f32),
                V((NZ, 1, NQ + W), f32), V((1, NQ), f32), V((1, NQ), f32),
                *tower, *tower,
                V((NZ, R, R), f32), V((NZ, R, R), f32), V((NZ, R, R), f32),
                V((2 * NX, R, R), f32), V((2 * NX, R, R), f32),
                V((2 * NX * R, R), bf16), V((2 * NX * R, R), f32), V((2 * NX, 1, R), f32),
                V((2 * NX * R, (NX - 1) * NQ), f32), V((2 * NX * R, NX * NQ), bf16), V((NX, 1, NQ), f32),
                V((2, 768, R), f32), V((2, max(map(max, ROWS)), R), f32), V((2, max(map(max, ROWS)), R), f32), V((2, max(map(max, ROWS)), R), f32),
                V((2, NZ * max(map(max, ROWS)) // NXY, R), f32), V((2, 1, R), f32), V((NXY, 1, R), f32),
                S, S((NZ,)), S, S((2 * NXY,)), S, S, S, S, S, S, S((NX,)), S, S((NX,)), S, S, S((NZ,)),
                S((2,)), S((2,)), S((2,)), S((2,)), S((2,)), S((2,)), S((2,)), S((2, NXY)), S((2,)), S((2, NXY)),
                S, S, S, S, S, pltpu.SemaphoreType.REGULAR,
            ],
            compiler_params=pltpu.CompilerParams(collective_id=0, has_side_effects=True, vmem_limit_bytes=60 * 2**20),
        )(query_feat, item_feat, log_q.reshape(1, R), w_query_in, w_query_out, w_item_in, w_item_out)
        gqi, gqo, gvi, gvo, out = pl.pallas_call(
            emit,
            name="emit",
            out_shape=[sd((W, W), f32), sd((W, R), f32), sd((W, W), f32), sd((W, R), f32), sd((1, R), f32)],
            in_specs=[vm] * 2,
            out_specs=[hbm] * 5,
            scratch_shapes=[S((7,))],
        )(pltpu.with_memory_space_constraint(fin, pltpu.VMEM), pltpu.with_memory_space_constraint(loss, pltpu.VMEM))
        return out[0, 0:1], gqi, gqo, gvi, gvo
    return step


def solution(mesh):
    return jax.shard_map(build(8, 4, 4), mesh=mesh,
                         in_specs=(P("dp", None), P("dp", None), P("dp"), P(), P(), P(), P()),
                         out_specs=(P(), P(), P(), P(), P()), check_vma=False)
```
